32 devices in a mesh: dp: 8 (over z, x), mp: 4 (over y, core).
Axes of the slice: x: 2, y: 2, z: 4, core: 2. Of those that a mesh axis runs over, the one named last changes fastest.
Arguments:
- tokens: bfloat16 [16384, 1024], P('dp'), may hold values from -6 to 6
- segment_ids: int32 [8, 2048], P('dp'), may hold values from 0 to 127, never falling along the last dimension, each value on 1 to 512 neighbouring positions
- w_query: bfloat16 [1024, 1024], P(None, 'mp'), may hold values from -0.1875 to 0.1875
- w_key: bfloat16 [1024, 1024], P(None, 'mp'), may hold values from -0.1875 to 0.1875
- w_value: bfloat16 [1024, 1024], P(None, 'mp'), may hold values from -0.1875 to 0.1875
- w_gate: bfloat16 [1024, 1024], P(None, 'mp'), may hold values from -0.1875 to 0.1875
- w_out: bfloat16 [1024, 1024], P('mp'), may hold values from -0.25 to 0.25
- w_left: bfloat16 [1024, 2816], P(None, 'mp'), may hold values from -0.1875 to 0.1875
- w_right: bfloat16 [1024, 2816], P(None, 'mp'), may hold values from -0.1875 to 0.1875
- w_down: bfloat16 [2816, 1024], P('mp'), may hold values from -0.109375 to 0.109375
- cotangent: bfloat16 [16384, 1024], P('dp'), may hold values from -6 to 6
Outputs:
- output: bfloat16 [16384, 1024], P('dp')
- grad_tokens: bfloat16 [16384, 1024], P('dp')
- grad_w_query: float32 [1024, 1024], P('dp', 'mp')
- grad_w_key: float32 [1024, 1024], P('dp', 'mp')
- grad_w_value: float32 [1024, 1024], P('dp', 'mp')
- grad_w_gate: float32 [1024, 1024], P('dp', 'mp')
- grad_w_out: float32 [1024, 1024], P('mp', 'dp')
- grad_w_left: float32 [1024, 2816], P('dp', 'mp')
- grad_w_right: float32 [1024, 2816], P('dp', 'mp')
- grad_w_down: float32 [2816, 1024], P('mp', 'dp')
The draws below stay inside these ranges and needn't reach their ends.
Inputs may be any that keep to these rules, and one draw needn't show every extreme that they name: `segment_ids`: in each row of 2048 positions the ids never fall; a document spans 1 to 512 positions, and one of them exactly that many.
All inputs are finite; a program needn't handle non-finite values.
Results may differ from the reference program's by a relative error of at most 0.02.
Values may be sent and summed in bfloat16 or wider, within the bound.
A program may use at most 192 MiB of HBM per device.

```python
import math
import jax
import jax.numpy as jnp
import numpy as np
from jax import lax

D = 1024
H = 16
HD = 64
FF = 2816
BLOCK = 64
SEQ = 2048
SEQS = 8
TOKENS = 16384
N_MP = 4


def strengthened(drawn, own_key, source, target, parts, factor):
    owner, partner = [(jnp.arange(drawn.shape[dim]) // (drawn.shape[dim] // parts)).reshape([-1 if axis == dim else 1 for axis in range(drawn.ndim)]) for dim in (source, target)]
    chosen = jax.random.permutation(own_key, parts)[partner]
    strong = (owner == chosen) | (owner == (partner + parts // 2) % parts)
    return jnp.where(strong, factor * drawn, drawn)


def block_levels(stream_key, dims, pieces, least, largest):
    def one(dim, shards_of):
        heights = jax.random.uniform(jax.random.fold_in(jax.random.fold_in(stream_key, 6), dim), (shards_of,), jnp.float32, least / len(pieces), largest / len(pieces))
        return jnp.repeat(jnp.exp(heights), dims[dim] // shards_of).reshape((-1,) + (1,) * (len(dims) - dim - 1))

    factor_of = one(*pieces[0])
    for cut in pieces[1:]:
        factor_of = factor_of * one(*cut)
    return factor_of


def profile(amount, total, reach, lean):
    loads = [(1 << 20) // math.isqrt(grade ** lean) + 1 for grade in range(2, amount + 1)]
    spare, holding = total - reach - (amount - 1), [1] * (amount - 1)
    while spare > 0:
        free = [i for i in range(amount - 1) if holding[i] < reach]
        whole, remaining = sum([loads[i] for i in free]), spare
        for i in free:
            extra = min(reach - holding[i], max(1, remaining * loads[i] // whole), spare)
            holding[i] = holding[i] + extra
            spare = spare - extra
    return np.array([reach] + holding)


def uneven(stream_key, number_of, total, most, skew):
    if number_of == 2:
        one = jax.random.randint(stream_key, (), max(1, total - most), min(most, total - 1) + 1)
        return jnp.stack([one, total - one])
    sizes = jnp.asarray(profile(number_of, total, most, skew), jnp.int32)
    twos = (number_of - 1) // 2
    source_of, taker = sizes[1:1 + 2 * twos:2], sizes[2:2 + 2 * twos:2]
    margin = jnp.minimum(source_of - 1, most - taker)
    moved = jax.random.randint(jax.random.fold_in(stream_key, 1), (twos,), 0, 1 << 20) % (margin + 1)
    sizes = sizes.at[1:1 + 2 * twos:2].set(source_of - moved).at[2:2 + 2 * twos:2].set(taker + moved)
    return sizes[jax.random.permutation(jax.random.fold_in(stream_key, 2), number_of)]


def noise(own_key, extent, spread, reach, cuts=(), kind=jnp.bfloat16):
    values = jax.random.normal(own_key, extent, jnp.float32) * spread
    if len(cuts) > 0:
        values = block_levels(own_key, extent, cuts, -0.22, 0.18) * values
    return jnp.clip(values, min=-reach, max=reach).astype(kind)


def bell_draw_with(stream_key, dims, scale, bound, split, heavy, kind=jnp.bfloat16):
    drawn = scale * jax.random.normal(stream_key, dims, jnp.float32)
    if split:
        drawn = drawn * block_levels(stream_key, dims, split, -0.22, 0.18)
    return jnp.clip(strengthened(drawn, jax.random.fold_in(stream_key, 3), *heavy), -bound, bound).astype(kind)


def setup_inputs(seed: int = 0) -> dict:
    streams_of = jax.random.split(jax.random.key(seed), 12)
    return {
        "tokens": bell_draw_with(streams_of[0], (TOKENS, D), 1.0, 6.0, ((0, 8),), (0, 1, 8, 2.0)),
        "segment_ids": jax.vmap(lambda own: jnp.searchsorted(jnp.cumsum(uneven(own, SEQ // 16, SEQ, SEQ // 4, 1)), jnp.arange(SEQ), side="right"))(jax.random.split(streams_of[1], SEQS)).reshape((SEQS, SEQ)).astype(jnp.int32),
        "w_query": noise(streams_of[2], (D, H * HD), D ** -0.5, 0.1875, ((1, 4),)),
        "w_key": noise(streams_of[3], (D, H * HD), D ** -0.5, 0.1875, ((1, 4),)),
        "w_value": noise(streams_of[4], (D, H * HD), D ** -0.5, 0.1875, ((1, 4),)),
        "w_gate": noise(streams_of[5], (D, H * HD), D ** -0.5, 0.1875, ((1, 4),)),
        "w_out": noise(streams_of[6], (H * HD, D), (H * HD // 2) ** -0.5, 0.25, ((0, 4),)),
        "w_left": noise(streams_of[7], (D, FF), D ** -0.5, 0.1875, ((1, 4),)),
        "w_right": noise(streams_of[8], (D, FF), D ** -0.5, 0.1875, ((1, 4),)),
        "w_down": noise(streams_of[9], (FF, D), FF ** -0.5, 0.109375, ((0, 4),)),
        "cotangent": bell_draw_with(streams_of[10], (TOKENS, D), 1.0, 6.0, ((0, 8),), (0, 1, 8, 2.0)),
    }


@jax.custom_vjp
def low(v):
    return lax.optimization_barrier(v.astype(jnp.bfloat16)).astype(jnp.float32)

@jax.custom_vjp
def low_back(v):
    return v

def low_keep(v):
    return (low(v), None)

def low_pass(kept, grad):
    return (grad,)

def back_keep(v):
    return (v, None)

def back_low(kept, grad):
    return (low(grad),)
low.defvjp(low_keep, low_pass)
low_back.defvjp(back_keep, back_low)

def multiply(left_arr, right_arr):
    return jnp.dot(left_arr, right_arr, precision=lax.Precision.HIGHEST, preferred_element_type=jnp.float32)

def rms_normal(values):
    return values * lax.rsqrt(lax.optimization_barrier(jnp.mean(values * values, axis=-1, keepdims=True)) + 1e-06)

def layer(source, weights, segments):
    w_query, w_key, w_value, w_gate, w_out, w_left, w_right, w_down = weights
    width_c = H * HD // N_MP
    width_f = FF // N_MP
    normed_low = low(rms_normal(source))
    query_parts, key_parts, value_parts, gate_parts = ([], [], [], [])
    for group in range(N_MP):
        group_in = low_back(normed_low)
        cols = slice(group * width_c, (group + 1) * width_c)
        query_parts.append(multiply(group_in, w_query[:, cols]))
        key_parts.append(multiply(group_in, w_key[:, cols]))
        value_parts.append(multiply(group_in, w_value[:, cols]))
        gate_parts.append(multiply(group_in, w_gate[:, cols]))
    queries = low_back(low(jnp.concatenate(query_parts, axis=1)))
    keys_all = low_back(low(jnp.concatenate(key_parts, axis=1)))
    values_all = low_back(low(jnp.concatenate(value_parts, axis=1)))
    gate_pre = low_back(jnp.concatenate(gate_parts, axis=1))
    blocks = SEQ // BLOCK
    query_blocks = queries.reshape(blocks, BLOCK, H, HD)
    key_blocks = keys_all.reshape(blocks, BLOCK, H, HD)
    value_blocks = values_all.reshape(blocks, BLOCK, H, HD)
    raw_scores = jnp.einsum('bqhd,bkhd->bhqk', query_blocks, key_blocks, precision=lax.Precision.HIGHEST) * HD ** (-0.5)
    scores = low_back(raw_scores)
    seg_blocks = segments.reshape(blocks, BLOCK)
    lower = jnp.arange(BLOCK)[:, None] >= jnp.arange(BLOCK)[None, :]
    allowed = (seg_blocks[:, :, None] == seg_blocks[:, None, :]) & lower[None]
    masked = jnp.where(allowed[:, None], scores, jnp.float32(-1e+30))
    top = lax.optimization_barrier(jnp.max(masked, axis=-1, keepdims=True))
    expd = jnp.exp(masked - top)
    probs = expd / lax.optimization_barrier(jnp.sum(expd, axis=-1, keepdims=True))
    attended = jnp.einsum('bhqk,bkhd->bqhd', low(probs), value_blocks, precision=lax.Precision.HIGHEST)
    attended = low_back(attended).reshape(SEQ, H, HD)
    head_normed = attended * lax.rsqrt(lax.optimization_barrier(jnp.mean(attended * attended, axis=-1, keepdims=True)) + 1e-06)
    gated = low((head_normed * jax.nn.sigmoid(gate_pre.reshape(SEQ, H, HD))).reshape(SEQ, H * HD))
    attn_sum = jnp.zeros((SEQ, D), jnp.float32)
    for group in range(N_MP):
        rows = slice(group * width_c, (group + 1) * width_c)
        attn_sum = attn_sum + low(multiply(gated[:, rows], w_out[rows]))
    hidden = source + low_back(attn_sum)
    normed_two = low(rms_normal(hidden))
    glu_sum = jnp.zeros((SEQ, D), jnp.float32)
    for group in range(N_MP):
        group_in = low_back(normed_two)
        cols = slice(group * width_f, (group + 1) * width_f)
        left = low_back(multiply(group_in, w_left[:, cols]))
        right = low_back(multiply(group_in, w_right[:, cols]))
        mixed = low(left * right)
        glu_sum = glu_sum + low(multiply(mixed, w_down[cols]))
    return hidden + low_back(glu_sum)

def reference(tokens, segment_ids, w_query, w_key, w_value, w_gate, w_out, w_left, w_right, w_down, cotangent):
    weights = tuple((w.astype(jnp.float32) for w in (w_query, w_key, w_value, w_gate, w_out, w_left, w_right, w_down)))
    sources = tokens.astype(jnp.float32).reshape(SEQS, SEQ, D)
    grads_in = cotangent.astype(jnp.float32).reshape(SEQS, SEQ, D)

    def one_sequence(carry, item):
        source, grad_out, segments = item
        result, pull = jax.vjp(lambda xv, *ws: layer(xv, ws, segments), source, *weights)
        grads = pull(grad_out)
        carry = tuple((c + g for c, g in zip(carry, grads[1:])))
        return (carry, (result, grads[0]))
    start = tuple((jnp.zeros(w.shape, jnp.float32) for w in weights))
    totals, (results, grad_src) = lax.scan(one_sequence, start, (sources, grads_in, segment_ids))
    output = results.reshape(TOKENS, D).astype(jnp.bfloat16)
    grad_tokens = grad_src.reshape(TOKENS, D).astype(jnp.bfloat16)
    return (output, grad_tokens, totals[0], totals[1], totals[2], totals[3], totals[4], totals[5], totals[6], totals[7])
```

```python
import jax
import jax.numpy as jnp
from jax import lax
from jax.sharding import PartitionSpec as P

HD = 64
BLOCK = 64


def head_total(partial_value):
    return lax.psum(partial_value.astype(jnp.bfloat16), "mp").astype(jnp.float32)


def scatter_sum(grads):
    joined = jnp.concatenate([g.astype(jnp.bfloat16) for g in grads], axis=1)
    summed = lax.psum_scatter(joined, "dp", scatter_dimension=0, tiled=True).astype(jnp.float32)
    cuts = []
    at = 0
    for g in grads:
        cuts.append(summed[:, at : at + g.shape[1]])
        at += g.shape[1]
    return cuts


def rms_factor(values):
    return lax.rsqrt(jnp.mean(values * values, axis=-1, keepdims=True) + 1e-06)


def norm_back(grad, normed, factor):
    return factor * (grad - normed * jnp.mean(grad * normed, axis=-1, keepdims=True))


def block_scores(query_blocks, key_blocks, allowed):
    scores = jnp.einsum(
        "bqhd,bkhd->bhqk", query_blocks, key_blocks, preferred_element_type=jnp.float32
    ) * HD ** (-0.5)
    return jnp.where(allowed[:, None], scores, jnp.float32(-1e30))


def body(
    tokens, segment_ids, w_query, w_key, w_value, w_gate, w_out, w_left, w_right, w_down, cotangent
):
    rows_all = tokens.shape[0]
    width_c = w_query.shape[1]
    heads_here = width_c // HD
    blocks = rows_all // BLOCK
    source = tokens.astype(jnp.float32)
    recip_one = rms_factor(source)
    normed_one = source * recip_one
    normed_low = normed_one.astype(jnp.bfloat16)
    queries = jnp.dot(normed_low, w_query, preferred_element_type=jnp.float32).astype(jnp.bfloat16)
    keys_all = jnp.dot(normed_low, w_key, preferred_element_type=jnp.float32).astype(jnp.bfloat16)
    values_all = jnp.dot(normed_low, w_value, preferred_element_type=jnp.float32).astype(
        jnp.bfloat16
    )
    gate_pre = jnp.dot(normed_low, w_gate, preferred_element_type=jnp.float32).reshape(
        rows_all, heads_here, HD
    )
    query_blocks = queries.reshape(blocks, BLOCK, heads_here, HD)
    key_blocks = keys_all.reshape(blocks, BLOCK, heads_here, HD)
    value_blocks = values_all.reshape(blocks, BLOCK, heads_here, HD)
    seg_blocks = segment_ids.reshape(blocks, BLOCK)
    lower = jnp.arange(BLOCK)[:, None] >= jnp.arange(BLOCK)[None, :]
    allowed = (seg_blocks[:, :, None] == seg_blocks[:, None, :]) & lower[None]
    masked = block_scores(query_blocks, key_blocks, allowed)
    top = jnp.max(masked, axis=-1, keepdims=True)
    expd = jnp.exp(masked - top)
    total = jnp.sum(expd, axis=-1, keepdims=True)
    log_total = top + jnp.log(total)
    probs_low = (expd / total).astype(jnp.bfloat16)
    attended = jnp.einsum(
        "bhqk,bkhd->bqhd", probs_low, value_blocks, preferred_element_type=jnp.float32
    )
    attended = attended.reshape(rows_all, heads_here, HD)
    head_factor = rms_factor(attended)
    head_normed = attended * head_factor
    sigma = jax.nn.sigmoid(gate_pre)
    gated = (head_normed * sigma).reshape(rows_all, width_c).astype(jnp.bfloat16)
    attn_sum = head_total(jnp.dot(gated, w_out, preferred_element_type=jnp.float32))
    hidden = source + attn_sum
    recip_two = rms_factor(hidden)
    normed_two = hidden * recip_two
    normed_two_low = normed_two.astype(jnp.bfloat16)
    left = jnp.dot(normed_two_low, w_left, preferred_element_type=jnp.float32)
    right = jnp.dot(normed_two_low, w_right, preferred_element_type=jnp.float32)
    mixed = (left * right).astype(jnp.bfloat16)
    glu_sum = head_total(jnp.dot(mixed, w_down, preferred_element_type=jnp.float32))
    output = (hidden + glu_sum).astype(jnp.bfloat16)
    grad_down = jnp.einsum("tc,tf->cf", cotangent, mixed, preferred_element_type=jnp.float32)
    d_mixed = jnp.einsum("tc,fc->tf", cotangent, w_down, preferred_element_type=jnp.float32)
    d_left = (d_mixed * right).astype(jnp.bfloat16)
    d_right = (d_mixed * left).astype(jnp.bfloat16)
    grad_left = jnp.einsum("td,tf->df", normed_two_low, d_left, preferred_element_type=jnp.float32)
    grad_right = jnp.einsum(
        "td,tf->df", normed_two_low, d_right, preferred_element_type=jnp.float32
    )
    glu_grads = scatter_sum((grad_left, grad_right, grad_down))
    d_partial_two = jnp.einsum("tf,df->td", d_left, w_left, preferred_element_type=jnp.float32)
    d_partial_two = d_partial_two + jnp.einsum(
        "tf,df->td", d_right, w_right, preferred_element_type=jnp.float32
    )
    d_norm_two = head_total(d_partial_two)
    d_hidden = cotangent.astype(jnp.float32) + norm_back(d_norm_two, normed_two, recip_two)
    d_out_low = d_hidden.astype(jnp.bfloat16)
    grad_out = jnp.einsum("td,tc->dc", d_out_low, gated, preferred_element_type=jnp.float32)
    d_gated = jnp.einsum("td,cd->tc", d_out_low, w_out, preferred_element_type=jnp.float32)
    d_gated = d_gated.reshape(rows_all, heads_here, HD)
    d_head = d_gated * sigma
    d_gate = (
        (d_gated * head_normed * sigma * (1.0 - sigma))
        .reshape(rows_all, width_c)
        .astype(jnp.bfloat16)
    )
    d_attended = norm_back(d_head, head_normed, head_factor).astype(jnp.bfloat16)
    d_attended = d_attended.reshape(blocks, BLOCK, heads_here, HD)
    probs = jnp.exp(block_scores(query_blocks, key_blocks, allowed) - log_total)
    probs_back = probs.astype(jnp.bfloat16)
    d_probs = jnp.einsum(
        "bqhd,bkhd->bhqk", d_attended, value_blocks, preferred_element_type=jnp.float32
    )
    d_values = jnp.einsum(
        "bhqk,bqhd->bkhd", probs_back, d_attended, preferred_element_type=jnp.float32
    )
    delta_rows = jnp.sum(probs * d_probs, axis=-1, keepdims=True)
    d_scores = (probs * (d_probs - delta_rows)).astype(jnp.bfloat16)
    d_queries = jnp.einsum(
        "bhqk,bkhd->bqhd", d_scores, key_blocks, preferred_element_type=jnp.float32
    ) * HD ** (-0.5)
    d_keys = jnp.einsum(
        "bhqk,bqhd->bkhd", d_scores, query_blocks, preferred_element_type=jnp.float32
    ) * HD ** (-0.5)
    d_queries = d_queries.reshape(rows_all, width_c).astype(jnp.bfloat16)
    d_keys = d_keys.reshape(rows_all, width_c).astype(jnp.bfloat16)
    d_values = d_values.reshape(rows_all, width_c).astype(jnp.bfloat16)
    grad_query = jnp.einsum("td,tc->dc", normed_low, d_queries, preferred_element_type=jnp.float32)
    grad_key = jnp.einsum("td,tc->dc", normed_low, d_keys, preferred_element_type=jnp.float32)
    grad_value = jnp.einsum("td,tc->dc", normed_low, d_values, preferred_element_type=jnp.float32)
    grad_gate = jnp.einsum("td,tc->dc", normed_low, d_gate, preferred_element_type=jnp.float32)
    attn_grads = scatter_sum((grad_query, grad_key, grad_value, grad_gate, grad_out))
    d_partial_one = jnp.einsum("tc,dc->td", d_queries, w_query, preferred_element_type=jnp.float32)
    d_partial_one = d_partial_one + jnp.einsum(
        "tc,dc->td", d_keys, w_key, preferred_element_type=jnp.float32
    )
    d_partial_one = d_partial_one + jnp.einsum(
        "tc,dc->td", d_values, w_value, preferred_element_type=jnp.float32
    )
    d_partial_one = d_partial_one + jnp.einsum(
        "tc,dc->td", d_gate, w_gate, preferred_element_type=jnp.float32
    )
    d_norm_one = head_total(d_partial_one)
    d_source = d_hidden + norm_back(d_norm_one, normed_one, recip_one)
    grad_tokens = d_source.astype(jnp.bfloat16)
    return (
        output,
        grad_tokens,
        attn_grads[0],
        attn_grads[1],
        attn_grads[2],
        attn_grads[3],
        attn_grads[4].T,
        glu_grads[0],
        glu_grads[1],
        glu_grads[2].T,
    )


def solution(mesh):
    in_specs = (
        P("dp", None),
        P("dp", None),
        P(None, "mp"),
        P(None, "mp"),
        P(None, "mp"),
        P(None, "mp"),
        P("mp", None),
        P(None, "mp"),
        P(None, "mp"),
        P("mp", None),
        P("dp", None),
    )
    out_specs = (
        P("dp", None),
        P("dp", None),
        P("dp", "mp"),
        P("dp", "mp"),
        P("dp", "mp"),
        P("dp", "mp"),
        P("mp", "dp"),
        P("dp", "mp"),
        P("dp", "mp"),
        P("mp", "dp"),
    )
    return jax.shard_map(body, mesh=mesh, in_specs=in_specs, out_specs=out_specs, check_vma=False)
```

```python
import functools

import jax
import jax.numpy as jnp
from jax import lax
from jax.experimental import pallas as pl
from jax.experimental.pallas import tpu as pltpu
from jax.sharding import PartitionSpec as P

HD = 64
BLOCK = 64
CHUNK = 256
TILE = 128
RING = 4
EPS = 1e-06
F32 = jnp.float32
BF16 = jnp.bfloat16
MESH = pl.DeviceIdType.MESH


def dot_nn(a, b):
    return lax.dot_general(a, b, (((1,), (0,)), ((), ())), preferred_element_type=F32)


def dot_nt(a, b):
    return lax.dot_general(a, b, (((1,), (1,)), ((), ())), preferred_element_type=F32)


def dot_tn(a, b):
    return lax.dot_general(a, b, (((0,), (0,)), ((), ())), preferred_element_type=F32)


def rms_factor(v):
    return lax.rsqrt(jnp.mean(v * v, axis=-1, keepdims=True) + EPS)


def norm_back(grad, normed, factor):
    return factor * (grad - normed * jnp.mean(grad * normed, axis=-1, keepdims=True))


def mult(v, n):
    return pl.multiple_of(v, n)


class Refs:
    pass


def kernel(names, ndp, *refs):
    r = Refs()
    for name, ref in zip(names, refs):
        setattr(r, name, ref)
    tokens, width = r.n1.shape
    chunks = tokens // CHUNK
    half, quarter = CHUNK // 2, CHUNK // 4
    wc = r.wo.shape[0]
    fp = r.wl.shape[1]
    ff = r.wl_h.shape[1]
    block_rows = width // ndp
    pairs = ndp // 2
    groups = width // 256
    per_group = pairs // groups
    half_chunks = chunks // 2
    wide = 5 * wc // 2

    dp = lax.axis_index("dp")
    mp = lax.axis_index("mp")
    core = mp % 2
    side = mp // 2
    partner = (dp, mp + 1 - 2 * core)
    across = (dp, mp + 2 - 4 * side)
    parity = dp % 2
    line = dp // 2
    beside = (dp + 1 - 2 * parity, mp)

    def remote(src, dst, send, recv, device):
        return pltpu.make_async_remote_copy(
            src_ref=src,
            dst_ref=dst,
            send_sem=send,
            recv_sem=recv,
            device_id=device,
            device_id_type=MESH,
        )

    barrier = pltpu.get_barrier_semaphore()
    for device in (partner, across, beside):
        pl.semaphore_signal(barrier, inc=1, device_id=device, device_id_type=MESH)

    def greet(j, carry):
        @pl.when(j != line)
        def _():
            pl.semaphore_signal(
                barrier, inc=1, device_id=(2 * j + parity, mp), device_id_type=MESH
            )

        return carry

    lax.fori_loop(0, pairs, greet, 0)

    def load_tokens(c):
        rows = pl.ds(mult(c * CHUNK, CHUNK), CHUNK)
        return pltpu.make_async_copy(r.tok_h.at[rows], r.n1.at[rows], r.sem_tok.at[c])

    def load_stage(i):
        src = r.wl_h if i < 2 else r.wr_h
        return pltpu.make_async_copy(
            src.at[pl.ds((i % 2) * (width // 2), width // 2)], r.stage, r.sem_w.at[7]
        )

    load_tokens(0).start()
    w_loads = [
        pltpu.make_async_copy(h, r.w.at[:, pl.ds(i * wc, wc)], r.sem_w.at[i])
        for i, h in enumerate((r.wq_h, r.wk_h, r.wv_h, r.wg_h))
    ]
    for copy in w_loads:
        copy.start()
    wo_load = pltpu.make_async_copy(r.wo_h, r.wo, r.sem_w.at[4])
    wo_load.start()
    for c in range(1, chunks):
        load_tokens(c).start()
    load_stage(0).start()
    wd_load = pltpu.make_async_copy(r.wd_h, r.wd.at[pl.ds(0, ff)], r.sem_w.at[5])
    wd_load.start()
    cot_load = pltpu.make_async_copy(r.cot_h, r.cot, r.sem_w.at[6])
    cot_load.start()

    pl.semaphore_wait(barrier, 3 + pairs - 1)

    def base(c):
        return mult(c * CHUNK, CHUNK)

    def own_rows(c):
        return pl.ds(mult(c * CHUNK + core * half + side * quarter, quarter), quarter)

    def other_rows(c):
        return pl.ds(mult(c * CHUNK + core * half + (1 - side) * quarter, quarter), quarter)

    def partner_own_rows(c):
        return pl.ds(mult(c * CHUNK + (1 - core) * half + side * quarter, quarter), quarter)

    def partner_other_rows(c):
        return pl.ds(mult(c * CHUNK + (1 - core) * half + (1 - side) * quarter, quarter), quarter)

    def kept(c):
        return pl.ds(mult(c * quarter, quarter), quarter)

    def part_of(s):
        return r.part_g if s == 1 else r.part

    def pair_of(s):
        return r.pair_g if s == 1 else r.pair

    def sent_of(s):
        return r.sent_g if s == 1 else r.sent

    def got_of(s):
        return r.got_g if s == 1 else r.got

    def full_of(s):
        return (r.n2, r.out_h, r.do, r.gt_h)[s]

    def at(s, c):
        return s * chunks + c

    def pair_copy(s, c):
        slot = c % RING
        return remote(
            part_of(s).at[c % 2, pl.ds(mult((1 - core) * half, half), half)],
            pair_of(s).at[slot],
            r.sem_as.at[at(s, c)],
            r.sem_ar.at[at(s, c)],
            partner,
        )

    def across_copy(s, c):
        return remote(
            sent_of(s).at[kept(c)],
            got_of(s).at[kept(c)],
            r.sem_bs.at[at(s, c)],
            r.sem_br.at[at(s, c)],
            across,
        )

    def result_src(s, c):
        if s in (0, 2):
            return full_of(s).at[own_rows(c)]
        return sent_of(s).at[kept(c)]

    def result_across(s, c):
        return remote(
            result_src(s, c),
            full_of(s).at[own_rows(c)],
            r.sem_cs.at[at(s, c)],
            r.sem_cr.at[at(s, c)],
            across,
        )

    def result_partner(s, c):
        return remote(
            result_src(s, c),
            full_of(s).at[own_rows(c)],
            r.sem_ps.at[at(s, c)],
            r.sem_pr.at[at(s, c)],
            partner,
        )

    def result_own(s, c):
        return pltpu.make_async_copy(
            sent_of(s).at[kept(c)], full_of(s).at[own_rows(c)], r.sem_o.at[at(s // 2, c)]
        )

    def forward(s, c):
        return remote(
            full_of(s).at[other_rows(c)],
            full_of(s).at[other_rows(c)],
            r.sem_ds.at[at(s, c)],
            r.sem_dr.at[at(s, c)],
            partner,
        )

    def step_b(s, c, send=True):
        copy = pair_copy(s, c)
        copy.wait_recv()
        copy.wait_send()
        part, pair = part_of(s), pair_of(s)
        slot, ring = c % 2, c % RING

        def piece(i, carry):
            rows = mult(i * 32, 32)
            away = pl.ds(mult(core * half + (1 - side) * quarter + rows, 32), 32)
            away_pair = pl.ds(mult((1 - side) * quarter + rows, 32), 32)
            total = part[slot, away, :].astype(F32) + pair[ring, away_pair, :].astype(F32)
            sent_of(s)[pl.ds(mult(c * quarter + rows, 32), 32), :] = total.astype(BF16)
            mine = pl.ds(mult(core * half + side * quarter + rows, 32), 32)
            mine_pair = pl.ds(mult(side * quarter + rows, 32), 32)
            total = part[slot, mine, :].astype(F32) + pair[ring, mine_pair, :].astype(F32)
            if s == 1:
                r.own_g[pl.ds(mult(c * quarter + rows, 32), 32), :] = total.astype(BF16)
            else:
                r.own[slot, pl.ds(rows, 32), :] = total
            return carry

        lax.fori_loop(0, quarter // 32, piece, 0)
        if send:
            across_copy(s, c).start()

    def step_c(s, c):
        copy = across_copy(s, c)
        copy.wait_recv()
        copy.wait_send()
        slot = c % 2

        def piece(i, carry):
            rows = mult(i * 32, 32)
            mine = pl.ds(mult(c * quarter + rows, 32), 32)
            full = pl.ds(mult(c * CHUNK + core * half + side * quarter + rows, 32), 32)
            arrived = got_of(s)[mine, :].astype(F32)
            if s == 1:
                total = r.own_g[mine, :].astype(F32) + arrived
            else:
                total = r.own[slot, pl.ds(rows, 32), :] + arrived
            if s == 0:
                hidden = r.tok_own[mine, :].astype(F32) + total
                r.hidden[mine, :] = hidden
                r.n2[full, :] = (hidden * rms_factor(hidden)).astype(BF16)
            elif s == 1:
                r.sent_g[mine, :] = (r.hidden[mine, :] + total).astype(BF16)
            elif s == 2:
                hidden = r.hidden[mine, :]
                factor = rms_factor(hidden)
                d_hidden = r.cot[full, :].astype(F32) + norm_back(total, hidden * factor, factor)
                r.d_hidden[mine, :] = d_hidden
                r.do[full, :] = d_hidden.astype(BF16)
            else:
                source = r.tok_own[mine, :].astype(F32)
                factor = rms_factor(source)
                d_source = r.d_hidden[mine, :] + norm_back(total, source * factor, factor)
                r.sent[mine, :] = d_source.astype(BF16)
            return carry

        lax.fori_loop(0, quarter // 32, piece, 0)
        result_across(s, c).start()
        result_partner(s, c).start()
        if s in (1, 3):
            result_own(s, c).start()

    def step_d(s, c):
        result_across(s, c).wait_recv()
        forward(s, c).start()

    def step_e(s, c):
        remote(
            result_src(s, c),
            full_of(s).at[partner_own_rows(c)],
            r.sem_ps.at[at(s, c)],
            r.sem_pr.at[at(s, c)],
            partner,
        ).wait_recv()
        remote(
            full_of(s).at[other_rows(c)],
            full_of(s).at[partner_other_rows(c)],
            r.sem_ds.at[at(s, c)],
            r.sem_dr.at[at(s, c)],
            partner,
        ).wait_recv()
        result_across(s, c).wait_send()
        result_partner(s, c).wait_send()
        forward(s, c).wait_send()
        if s in (1, 3):
            result_own(s, c).wait()

    def tick(s, c):
        @pl.when(c >= 1)
        def _():
            step_b(s, c - 1)

        @pl.when(c >= 2)
        def _():
            step_c(s, c - 2)

        @pl.when(c >= 3)
        def _():
            step_d(s, c - 3)

    def late_tick(s, n):
        if n == 0:
            step_b(s, chunks - 1)
        if n <= 1:
            step_c(s, chunks - 2 + n)
        step_d(s, chunks - 3 + n)

    lane = lax.broadcasted_iota(jnp.int32, (TILE, TILE), 1)
    row = lax.broadcasted_iota(jnp.int32, (TILE, TILE), 0)
    first = lane < HD

    def stacked(v):
        zero = jnp.zeros_like(v)
        return jnp.concatenate([jnp.where(first, v, zero), jnp.where(first, zero, v)], axis=0)

    def unstacked(v):
        return jnp.where(first, v[:TILE], v[TILE:])

    def head_mean(v):
        zero = jnp.zeros_like(v)
        low = jnp.sum(jnp.where(first, v, zero), axis=-1, keepdims=True)
        high = jnp.sum(jnp.where(first, zero, v), axis=-1, keepdims=True)
        return jnp.where(first, low, high) * (1.0 / HD)

    def probs_of(tile, rows, lanes):
        ids = r.seg[pl.ds(tile, 1), :].astype(F32)
        across_ids = jnp.broadcast_to(ids, (TILE, TILE))
        allowed = (
            (across_ids == across_ids.T) & (lane <= row) & (lane // BLOCK == row // BLOCK)
        )
        stack = stacked(r.qkv[rows, pl.ds(lanes, TILE)])
        keys = r.qkv[rows, pl.ds(wc + lanes, TILE)]
        scores = dot_nt(stack, keys) * HD ** (-0.5)
        allowed2 = jnp.concatenate([allowed, allowed], axis=0)
        masked = jnp.where(allowed2, scores, F32(-1e30))
        top = jnp.max(masked, axis=-1, keepdims=True)
        expd = jnp.exp(masked - top)
        probs = expd * (1.0 / jnp.sum(expd, axis=-1, keepdims=True))
        return probs, stack, keys

    head_pairs = wc // TILE
    tiles = CHUNK // TILE

    def tile_of(c, i):
        tile = c * tiles + i // head_pairs
        lanes = mult((i % head_pairs) * TILE, TILE)
        rows = pl.ds(mult(tile * TILE, TILE), TILE)
        return tile, rows, lanes

    for copy in w_loads:
        copy.wait()
    wo_load.wait()

    def phase_one(c, carry):
        rows_all = pl.ds(base(c), CHUNK)
        load_tokens(c).wait()
        r.tok_own[kept(c), :] = r.n1[own_rows(c), :]

        def norm_piece(i, carry2):
            rows = pl.ds(mult(c * CHUNK + i * 32, 32), 32)
            x = r.n1[rows, :].astype(F32)
            r.n1[rows, :] = (x * rms_factor(x)).astype(BF16)
            return carry2

        lax.fori_loop(0, CHUNK // 32, norm_piece, 0)

        def project(t, carry2):
            cols = pl.ds(mult(t * wc, wc), wc)
            r.qkv[rows_all, cols] = dot_nn(r.n1[rows_all, :], r.w[:, cols]).astype(BF16)
            return carry2

        lax.fori_loop(0, 3, project, 0)
        r.gate_now[...] = dot_nn(r.n1[rows_all, :], r.w[:, pl.ds(3 * wc, wc)])
        r.gate[rows_all, :] = r.gate_now[...].astype(BF16)

        def attend(i, carry2):
            tile, rows, lanes = tile_of(c, i)
            probs, _, _ = probs_of(tile, rows, lanes)
            values = r.qkv[rows, pl.ds(2 * wc + lanes, TILE)]
            attended = unstacked(dot_nn(probs.astype(BF16), values))
            r.attended[rows, pl.ds(lanes, TILE)] = attended.astype(BF16)
            factor = lax.rsqrt(head_mean(attended * attended) + EPS)
            near = pl.ds(mult((i // head_pairs) * TILE, TILE), TILE)
            sigma = jax.nn.sigmoid(r.gate_now[near, pl.ds(lanes, TILE)])
            r.gated[rows, pl.ds(lanes, TILE)] = (attended * factor * sigma).astype(BF16)
            return carry2

        lax.fori_loop(0, tiles * head_pairs, attend, 0)

        def out_piece(t, carry2):
            cols = pl.ds(mult(t * 256, 256), 256)
            r.part[c % 2, :, cols] = dot_nn(r.gated[rows_all, :], r.wo[:, cols]).astype(BF16)
            return carry2

        lax.fori_loop(0, width // 256, out_piece, 0)
        pair_copy(0, c).start()

        for i in range(4):

            @pl.when(c == i)
            def _():
                load_stage(i).wait()
                dst = r.wl if i < 2 else r.wr
                start = (i % 2) * (width // 2)
                for k in range(4):
                    rows = pl.ds(start + k * (width // 8), width // 8)
                    dst[rows, pl.ds(fp - 128, 128)] = jnp.zeros((width // 8, 128), BF16)
                    dst[rows, pl.ds(0, ff)] = r.stage[pl.ds(k * (width // 8), width // 8), :]
                if i < 3:
                    load_stage(i + 1).start()

        tick(0, c)
        return carry

    lax.fori_loop(0, chunks, phase_one, 0)

    wd_load.wait()
    r.wd[pl.ds(ff, fp - ff), :] = jnp.zeros((fp - ff, width), BF16)
    cot_load.wait()

    def phase_two(c, carry):
        for n in range(3):

            @pl.when(c == n)
            def _():
                late_tick(0, n)

        step_e(0, c)
        rows_all = pl.ds(base(c), CHUNK)
        rows_half = pl.ds(mult((c % half_chunks) * CHUNK, CHUNK), CHUNK)

        def hidden_units(t, carry2):
            cols = pl.ds(mult(t * 256, 256), 256)
            left = dot_nn(r.n2[rows_all, :], r.wl[:, cols])
            right = dot_nn(r.n2[rows_all, :], r.wr[:, cols])
            r.mixed[rows_all, cols] = (left * right).astype(BF16)
            d_mixed = dot_nt(r.cot[rows_all, :], r.wd[cols, :])
            r.d_left[rows_all, cols] = (d_mixed * right).astype(BF16)
            r.d_right[c // half_chunks, rows_half, cols] = (d_mixed * left).astype(BF16)
            return carry2

        lax.fori_loop(0, fp // 256, hidden_units, 0)

        def parts(t, carry2):
            cols = pl.ds(mult(t * 256, 256), 256)
            back = dot_nt(r.d_left[rows_all, :], r.wl[cols, :])
            back = back + dot_nt(r.d_right[c // half_chunks, rows_half, :], r.wr[cols, :])
            r.part[c % 2, :, cols] = back.astype(BF16)
            r.part_g[c % 2, :, cols] = dot_nn(r.mixed[rows_all, :], r.wd[:, cols]).astype(BF16)
            return carry2

        lax.fori_loop(0, width // 256, parts, 0)
        pair_copy(2, c).start()
        pair_copy(1, c).start()
        tick(2, c)

        @pl.when(c >= 1)
        def _():
            step_b(1, c - 1, send=False)

        return carry

    lax.fori_loop(0, chunks, phase_two, 0)
    late_tick(2, 0)
    step_b(1, chunks - 1, send=False)

    def send_glu(c, carry):
        across_copy(1, c).start()
        return carry

    lax.fori_loop(0, chunks, send_glu, 0)

    def transposed(src, i, dst):
        def piece(k, carry):
            rows = pl.ds(mult(k * 256, 256), 256)
            tile = src[rows, pl.ds(mult(i * 256, 256), 256)].T
            dst[k // 4, :, pl.ds(mult((k % 4) * 256, 256), 256)] = tile
            return carry

        lax.fori_loop(0, tokens // 256, piece, 0)

    def grad_of(turned, right, cols):
        total = None
        for k in range(2):
            rows = pl.ds(k * (tokens // 2), tokens // 2)
            operand = right[k, :, cols] if len(right.shape) == 3 else right[rows, cols]
            term = dot_nn(turned[k], operand)
            total = term if total is None else total + term
        return total.astype(BF16)

    def beside_copy(grads, arrivals, sems, g):
        block = 2 * g + 1 - parity
        send, recv = sems
        return remote(
            grads(pl.ds(mult(block * block_rows, block_rows), block_rows)),
            arrivals(pl.ds(mult(g * block_rows, block_rows), block_rows)),
            send.at[g],
            recv.at[g],
            beside,
        )

    def line_copy(grads, arrivals, sems, g):
        block = 2 * g + parity
        send, recv = sems
        return remote(
            grads(pl.ds(mult(block * block_rows, block_rows), block_rows)),
            arrivals(line),
            send.at[g],
            recv.at[line],
            (block, mp),
        )

    def glu_rows(rows):
        return r.grad_g.at[:, rows]

    def glu_beside(rows):
        return r.xg_h.at[:, rows]

    def glu_line(slot):
        return r.zg_h.at[slot]

    def att_rows(rows):
        return r.d_right.at[:, rows, pl.ds(0, wide)]

    def att_beside(rows):
        return r.xa_h.at[:, rows]

    def att_line(slot):
        return r.za_h.at[slot]

    glu_x = (glu_rows, glu_beside, (r.sem_xgs, r.sem_xgr))
    glu_z = (glu_rows, glu_line, (r.sem_zgs, r.sem_zgr))
    att_x = (att_rows, att_beside, (r.sem_xas, r.sem_xar))
    att_z = (att_rows, att_line, (r.sem_zas, r.sem_zar))

    def each(count, act):
        def one(j, carry):
            act(j)
            return carry

        if count == 1:
            act(0)
        else:
            lax.fori_loop(0, count, one, 0)

    def glu_group(i, carry):
        rows = pl.ds(mult(i * 256, 256), 256)
        transposed(r.n2, i, r.part)

        def sides(t, carry2):
            cols = pl.ds(mult(t * 256, 256), 256)
            r.grad_g[0, rows, cols] = grad_of(r.part, r.d_left, cols)
            r.grad_g[1, rows, cols] = grad_of(r.part, r.d_right, cols)
            return carry2

        lax.fori_loop(0, fp // 256, sides, 0)
        transposed(r.cot, i, r.part_g)

        def down(t, carry2):
            cols = pl.ds(mult(t * 256, 256), 256)
            r.grad_g[2, rows, cols] = grad_of(r.part_g, r.mixed, cols)
            return carry2

        lax.fori_loop(0, fp // 256, down, 0)
        each(per_group, lambda j: beside_copy(*glu_x, i * per_group + j).start())
        return carry

    lax.fori_loop(0, groups, glu_group, 0)

    def line_step(kinds, lanes, x, z, arrivals_h, stage, grads, g):
        copy = beside_copy(*x, g)
        copy.wait_recv()
        copy.wait_send()
        here = pl.ds(mult(g * block_rows, block_rows), block_rows)
        loads = []
        for t in range(kinds):
            load = pltpu.make_async_copy(
                arrivals_h.at[t, here],
                stage.at[pl.ds(t * block_rows, block_rows), pl.ds(0, lanes)],
                r.sem_stage.at[t],
            )
            load.start()
            loads.append(load)
        for load in loads:
            load.wait()
        step = min(16, block_rows)
        cols = pl.ds(0, lanes)

        for t in range(kinds):

            def piece(i, carry):
                sub = mult(i * step, step)
                there = pl.ds(mult((2 * g + parity) * block_rows + sub, step), step)
                mine = grads[t, there, cols].astype(F32)
                theirs = stage[pl.ds(mult(t * block_rows + sub, step), step), cols].astype(F32)
                grads[t, there, cols] = (mine + theirs).astype(BF16)
                return carry

            lax.fori_loop(0, block_rows // step, piece, 0)

        @pl.when(g != line)
        def _():
            line_copy(*z, g).start()

    def glu_line_step(g):
        line_step(3, fp, glu_x, glu_z, r.xg_h, r.mixed, r.grad_g, g)

    def att_line_step(g):
        line_step(2, wide, att_x, att_z, r.xa_h, r.d_left, r.d_right, g)

    def phase_three(c, carry):
        for n in range(2):

            @pl.when(c == n)
            def _():
                late_tick(2, n + 1)

        step_e(2, c)
        rows_all = pl.ds(base(c), CHUNK)
        r.gate_now[...] = dot_nt(r.do[rows_all, :], r.wo[...])

        def attend_back(i, carry2):
            tile, rows, lanes = tile_of(c, i)
            near = pl.ds(mult((i // head_pairs) * TILE, TILE), TILE)
            here = pl.ds(lanes, TILE)
            d_gated = r.gate_now[near, here]
            sigma = jax.nn.sigmoid(r.gate[rows, here].astype(F32))
            attended = r.attended[rows, here].astype(F32)
            factor = lax.rsqrt(head_mean(attended * attended) + EPS)
            head_normed = attended * factor
            d_head = d_gated * sigma
            d_gate = d_head * head_normed * (1.0 - sigma)
            r.d_all[rows, pl.ds(3 * wc + lanes, TILE)] = d_gate.astype(BF16)
            d_att = factor * (d_head - head_normed * head_mean(d_head * head_normed))
            d_stack = stacked(d_att.astype(BF16))
            probs, stack, keys = probs_of(tile, rows, lanes)
            values = r.qkv[rows, pl.ds(2 * wc + lanes, TILE)]
            d_probs = dot_nt(d_stack, values)
            d_values = dot_tn(probs.astype(BF16), d_stack)
            r.d_all[rows, pl.ds(2 * wc + lanes, TILE)] = d_values.astype(BF16)
            delta = jnp.sum(probs * d_probs, axis=-1, keepdims=True)
            d_scores = (probs * (d_probs - delta)).astype(BF16)
            d_queries = unstacked(dot_nn(d_scores, keys)) * HD ** (-0.5)
            r.d_all[rows, here] = d_queries.astype(BF16)
            d_keys = dot_tn(d_scores, stack) * HD ** (-0.5)
            r.d_all[rows, pl.ds(wc + lanes, TILE)] = d_keys.astype(BF16)
            return carry2

        lax.fori_loop(0, tiles * head_pairs, attend_back, 0)

        def back_piece(t, carry2):
            cols = pl.ds(mult(t * 256, 256), 256)
            r.part[c % 2, :, cols] = dot_nt(r.d_all[rows_all, :], r.w[cols, :]).astype(BF16)
            return carry2

        lax.fori_loop(0, width // 256, back_piece, 0)
        pair_copy(3, c).start()
        tick(3, c)

        for i in range(groups):

            @pl.when(c == 2 * i + 1)
            def _():
                each(per_group, lambda j: glu_line_step(i * per_group + j))

        return carry

    lax.fori_loop(0, chunks, phase_three, 0)
    late_tick(3, 0)

    def att_group(i, carry):
        rows = pl.ds(mult(i * 256, 256), 256)
        transposed(r.n1, i, r.part_g)

        def store(t, total):
            for u in range(wc // 128):
                at_col = t * (wc // 128) + u
                cols = pl.ds(mult((at_col % (wide // 128)) * 128, 128), 128)
                r.d_right[at_col // (wide // 128), rows, cols] = total[:, u * 128 : u * 128 + 128]

        def four(t, carry2):
            store(t, grad_of(r.part_g, r.d_all, pl.ds(mult(t * wc, wc), wc)))
            return carry2

        lax.fori_loop(0, 4, four, 0)
        transposed(r.do, i, r.part_g)
        store(4, grad_of(r.part_g, r.gated, pl.ds(0, wc)))
        each(per_group, lambda j: beside_copy(*att_x, i * per_group + j).start())
        for n in range(2):

            @pl.when(i == n)
            def _():
                late_tick(3, n + 1)

        return carry

    lax.fori_loop(0, groups, att_group, 0)

    def glu_result(c, carry):
        step_c(1, c)
        return carry

    lax.fori_loop(0, chunks, glu_result, 0)

    def att_lines(g, carry):
        att_line_step(g)
        return carry

    lax.fori_loop(0, pairs, att_lines, 0)

    def glu_forward(c, carry):
        step_d(1, c)
        return carry

    lax.fori_loop(0, chunks, glu_forward, 0)

    def finish(kinds, lanes, z, arrivals_h, stage, grads, out):
        cols = pl.ds(0, lanes)

        def arrived(j, carry):
            @pl.when(j != line)
            def _():
                block = 2 * j + parity
                remote(
                    z[0](pl.ds(mult(dp * block_rows, block_rows), block_rows)),
                    z[1](j),
                    z[2][0].at[j],
                    z[2][1].at[j],
                    (block, mp),
                ).wait_recv()
                line_copy(*z, j).wait_send()

            return carry

        lax.fori_loop(0, pairs, arrived, 0)
        for t in range(kinds):

            def fetch(j):
                return pltpu.make_async_copy(
                    arrivals_h.at[j, t],
                    stage.at[pl.ds(mult(j * block_rows, block_rows), block_rows), cols],
                    r.sem_stage.at[t],
                )

            def get(j, carry):
                @pl.when(j != line)
                def _():
                    fetch(j).start()
                    fetch(j).wait()

                return carry

            lax.fori_loop(0, pairs, get, 0)
            step = min(16, block_rows)

            def piece(i, carry):
                sub = mult(i * step, step)
                total = grads[t, pl.ds(mult(dp * block_rows + sub, step), step), cols].astype(F32)
                for j in range(pairs):
                    term = stage[pl.ds(mult(j * block_rows + sub, step), step), cols].astype(F32)
                    total = total + jnp.where(j == line, 0.0, term)
                out[t, pl.ds(sub, step), :] = total
                return carry

            lax.fori_loop(0, block_rows // step, piece, 0)

    finish(3, fp, glu_z, r.zg_h, r.mixed, r.grad_g, r.out_g)
    finish(2, wide, att_z, r.za_h, r.d_left, r.d_right, r.out_a)

    def ends(c, carry):
        step_e(1, c)
        step_e(3, c)
        return carry

    lax.fori_loop(0, chunks, ends, 0)


def fused(ndp, args):
    tokens, seg, wq, wk, wv, wg, wo, wl, wr, wd, cot = args
    rows, width = tokens.shape
    wc, ff = wq.shape[1], wl.shape[1]
    fp = (ff + 255) // 256 * 256
    chunks = rows // CHUNK
    quarter = CHUNK // 4
    own = rows // 4
    br = width // ndp
    pairs = ndp // 2
    wide = 5 * wc // 2
    hbm = pl.BlockSpec(memory_space=pl.ANY)
    vmem = pl.BlockSpec(memory_space=pltpu.VMEM)
    ins = [
        ("tok_h", tokens, hbm),
        ("seg", seg.reshape(rows // TILE, TILE), vmem),
        ("wq_h", wq, hbm),
        ("wk_h", wk, hbm),
        ("wv_h", wv, hbm),
        ("wg_h", wg, hbm),
        ("wo_h", wo, hbm),
        ("wl_h", wl, hbm),
        ("wr_h", wr, hbm),
        ("wd_h", wd, hbm),
        ("cot_h", cot, hbm),
    ]
    outs = [
        ("out_h", (rows, width), BF16, hbm),
        ("gt_h", (rows, width), BF16, hbm),
        ("out_g", (3, br, fp), F32, vmem),
        ("out_a", (2, br, wide), F32, vmem),
        ("xg_h", (3, pairs * br, fp), BF16, hbm),
        ("xa_h", (2, pairs * br, wide), BF16, hbm),
        ("zg_h", (pairs, 3, br, fp), BF16, hbm),
        ("za_h", (pairs, 2, br, wide), BF16, hbm),
    ]
    dma = pltpu.SemaphoreType.DMA
    scratch = [
        ("n1", pltpu.VMEM((rows, width), BF16)),
        ("tok_own", pltpu.VMEM((own, width), BF16)),
        ("cot", pltpu.VMEM((rows, width), BF16)),
        ("w", pltpu.VMEM((width, 4 * wc), BF16)),
        ("wo", pltpu.VMEM((wc, width), BF16)),
        ("wl", pltpu.VMEM((width, fp), BF16)),
        ("wr", pltpu.VMEM((width, fp), BF16)),
        ("wd", pltpu.VMEM((fp, width), BF16)),
        ("stage", pltpu.VMEM((width // 2, ff), BF16)),
        ("qkv", pltpu.VMEM((rows, 3 * wc), BF16)),
        ("gate", pltpu.VMEM((rows, wc), BF16)),
        ("gate_now", pltpu.VMEM((CHUNK, wc), F32)),
        ("attended", pltpu.VMEM((rows, wc), BF16)),
        ("gated", pltpu.VMEM((rows, wc), BF16)),
        ("n2", pltpu.VMEM((rows, width), BF16)),
        ("mixed", pltpu.VMEM((rows, fp), BF16)),
        ("d_left", pltpu.VMEM((rows, fp), BF16)),
        ("d_right", pltpu.VMEM((2, rows // 2, fp), BF16)),
        ("do", pltpu.VMEM((rows, width), BF16)),
        ("part", pltpu.VMEM((2, CHUNK, width), BF16)),
        ("part_g", pltpu.VMEM((2, CHUNK, width), BF16)),
        ("pair", pltpu.VMEM((RING, CHUNK // 2, width), BF16)),
        ("pair_g", pltpu.VMEM((RING, CHUNK // 2, width), BF16)),
        ("sent", pltpu.VMEM((own, width), BF16)),
        ("sent_g", pltpu.VMEM((own, width), BF16)),
        ("got", pltpu.VMEM((own, width), BF16)),
        ("got_g", pltpu.VMEM((own, width), BF16)),
        ("own", pltpu.VMEM((2, quarter, width), F32)),
        ("own_g", pltpu.VMEM((own, width), BF16)),
        ("hidden", pltpu.VMEM((own, width), F32)),
        ("d_hidden", pltpu.VMEM((own, width), F32)),
        ("grad_g", pltpu.VMEM((3, width, fp), BF16)),
        ("sem_tok", dma((chunks,))),
        ("sem_w", dma((8,))),
        ("sem_stage", dma((5,))),
    ]
    for name in ("as", "ar", "bs", "br", "cs", "cr", "ps", "pr", "ds", "dr"):
        scratch.append(("sem_" + name, dma((4 * chunks,))))
    scratch.append(("sem_o", dma((2 * chunks,))))
    for name in ("xgs", "xgr", "zgs", "zgr", "xas", "xar", "zas", "zar"):
        scratch.append(("sem_" + name, dma((pairs,))))
    names = [n for n, *_ in ins] + [n for n, *_ in outs] + [n for n, _ in scratch]

    def call(*refs):
        named = dict(zip(names, refs))
        named["d_all"] = named["n2"]
        kernel(list(named), ndp, *named.values())

    flops = 6 * rows * width * (5 * wc + 3 * ff)
    result = pl.pallas_call(
        call,
        out_shape=[jax.ShapeDtypeStruct(s, d) for _, s, d, _ in outs],
        in_specs=[s for *_, s in ins],
        out_specs=[s for *_, s in outs],
        scratch_shapes=[s for _, s in scratch],
        compiler_params=pltpu.CompilerParams(
            collective_id=0, has_side_effects=True, vmem_limit_bytes=67043328
        ),
        cost_estimate=pl.CostEstimate(flops=flops, bytes_accessed=1 << 25, transcendentals=1 << 22),
        name="fused_layer",
    )(*[a for _, a, _ in ins])
    return result[:4]


def body(ndp, *args):
    out, grad_tokens, glu, att = fused(ndp, args)
    ff, wc = args[7].shape[1], args[2].shape[1]
    att = jnp.concatenate([att[0], att[1]], axis=1)
    return (
        out,
        grad_tokens,
        att[:, :wc],
        att[:, wc : 2 * wc],
        att[:, 2 * wc : 3 * wc],
        att[:, 3 * wc : 4 * wc],
        att[:, 4 * wc :].T,
        glu[0, :, :ff],
        glu[1, :, :ff],
        glu[2, :, :ff].T,
    )


def solution(mesh):
    rows, cols, down = P("dp", None), P(None, "mp"), P("mp", None)
    grad = P("dp", "mp")
    return jax.shard_map(
        functools.partial(body, mesh.shape["dp"]),
        mesh=mesh,
        in_specs=(rows, rows, cols, cols, cols, cols, down, cols, cols, down, rows),
        out_specs=(rows, rows, grad, grad, grad, grad, P("mp", "dp"), grad, grad, P("mp", "dp")),
        check_vma=False,
    )
```

```python
import functools

import jax
import jax.numpy as jnp
from jax import lax
from jax.experimental import pallas as pl
from jax.experimental.pallas import tpu as pltpu
from jax.sharding import PartitionSpec as P

HD = 64
BLOCK = 64
CHUNK = 256
TILE = 128
RING = 4
EPS = 1e-06
F32 = jnp.float32
BF16 = jnp.bfloat16
MESH = pl.DeviceIdType.MESH


def dot_nn(a, b):
    return lax.dot_general(a, b, (((1,), (0,)), ((), ())), preferred_element_type=F32)


def dot_nt(a, b):
    return lax.dot_general(a, b, (((1,), (1,)), ((), ())), preferred_element_type=F32)


def dot_tn(a, b):
    return lax.dot_general(a, b, (((0,), (0,)), ((), ())), preferred_element_type=F32)


def rms_factor(v):
    return lax.rsqrt(jnp.mean(v * v, axis=-1, keepdims=True) + EPS)


def norm_back(grad, normed, factor):
    return factor * (grad - normed * jnp.mean(grad * normed, axis=-1, keepdims=True))


def mult(v, n):
    return pl.multiple_of(v, n)


class Refs:
    pass


def kernel(names, ndp, *refs):
    r = Refs()
    for name, ref in zip(names, refs):
        setattr(r, name, ref)
    tokens, width = r.n1.shape
    chunks = tokens // CHUNK
    half, quarter = CHUNK // 2, CHUNK // 4
    wc = r.wo_h.shape[0]
    fp, ff = r.wl.shape[0], r.wl_h.shape[0]
    block_rows = width // ndp
    pairs = ndp // 2
    groups = width // 256
    per_group = pairs // groups
    half_chunks = chunks // 2
    wide = 5 * wc // 2

    dp = lax.axis_index("dp")
    mp = lax.axis_index("mp")
    core = mp % 2
    side = mp // 2
    partner = (dp, mp + 1 - 2 * core)
    across = (dp, mp + 2 - 4 * side)
    parity = dp % 2
    line = dp // 2
    beside = (dp + 1 - 2 * parity, mp)

    def remote(src, dst, send, recv, device):
        return pltpu.make_async_remote_copy(
            src_ref=src,
            dst_ref=dst,
            send_sem=send,
            recv_sem=recv,
            device_id=device,
            device_id_type=MESH,
        )

    barrier = pltpu.get_barrier_semaphore()
    for device in (partner, across, beside):
        pl.semaphore_signal(barrier, inc=1, device_id=device, device_id_type=MESH)

    def greet(j, carry):
        @pl.when(j != line)
        def _():
            pl.semaphore_signal(
                barrier, inc=1, device_id=(2 * j + parity, mp), device_id_type=MESH
            )

        return carry

    lax.fori_loop(0, pairs, greet, 0)

    pair_mp = mp + 1 - 2 * core
    across_mp = mp + 2 - 4 * side

    def group_of(who):
        return pl.ds(mult(who * wc, wc), wc)

    def wo_across():
        there = r.wof.at[group_of(mp)]
        return remote(r.wo_h, there, r.sem_wos.at[0], r.sem_wor.at[0], across)

    def wo_partner():
        there = r.wof.at[group_of(mp)]
        return remote(r.wo_h, there, r.sem_wos.at[1], r.sem_wor.at[1], partner)

    def wo_forward():
        here = r.wof.at[group_of(across_mp)]
        return remote(here, here, r.sem_wos.at[2], r.sem_wor.at[2], partner)

    def load_tokens(c):
        rows = pl.ds(mult(c * CHUNK, CHUNK), CHUNK)
        return pltpu.make_async_copy(r.tok_h.at[rows], r.n1.at[rows], r.sem_tok.at[c])

    load_tokens(0).start()
    w_loads = [
        pltpu.make_async_copy(h, r.w.at[:, pl.ds(i * wc, wc)], r.sem_w.at[i])
        for i, h in enumerate((r.wq_h, r.wk_h, r.wv_h, r.wg_h))
    ]
    for copy in w_loads:
        copy.start()
    wo_load = pltpu.make_async_copy(
        r.wo_h, r.wof.at[pl.ds(mult(mp * wc, wc), wc)], r.sem_w.at[4]
    )
    wo_load.start()
    for c in range(1, chunks):
        load_tokens(c).start()
    glu_loads = [
        pltpu.make_async_copy(h, v.at[pl.ds(0, ff)], r.sem_w.at[i])
        for i, h, v in ((5, r.wd_h, r.wd), (6, r.wl_h, r.wl), (7, r.wr_h, r.wr))
    ]
    for copy in glu_loads:
        copy.start()
    cot_load = pltpu.make_async_copy(r.cot_h, r.cot, r.sem_w.at[8])
    cot_load.start()

    pl.semaphore_wait(barrier, 3 + pairs - 1)
    for copy in (wo_across(), wo_partner()):
        copy.start()

    def base(c):
        return mult(c * CHUNK, CHUNK)

    def half_rows(c):
        return pl.ds(mult(c * CHUNK + core * half, half), half)

    def own_rows(c):
        return pl.ds(mult(c * CHUNK + core * half + side * quarter, quarter), quarter)

    def other_rows(c):
        return pl.ds(mult(c * CHUNK + core * half + (1 - side) * quarter, quarter), quarter)

    def partner_own_rows(c):
        return pl.ds(mult(c * CHUNK + (1 - core) * half + side * quarter, quarter), quarter)

    def partner_other_rows(c):
        return pl.ds(mult(c * CHUNK + (1 - core) * half + (1 - side) * quarter, quarter), quarter)

    def kept(c):
        return pl.ds(mult(c * quarter, quarter), quarter)

    def part_of(s):
        return r.part_g if s == 1 else r.part

    def pair_of(s):
        return r.pair_g if s == 1 else r.pair

    def sent_of(s):
        return r.sent_g if s == 1 else r.sent

    def got_of(s):
        return r.got_g if s == 1 else r.got

    def full_of(s):
        return (None, r.out_h, r.do, r.gt_h)[s]

    def at(s, c):
        return s * chunks + c

    def pair_copy(s, c):
        slot = c % RING
        return remote(
            part_of(s).at[c % 2, pl.ds(mult((1 - core) * half, half), half)],
            pair_of(s).at[slot],
            r.sem_as.at[at(s, c)],
            r.sem_ar.at[at(s, c)],
            partner,
        )

    def across_copy(s, c):
        return remote(
            sent_of(s).at[kept(c)],
            got_of(s).at[kept(c)],
            r.sem_bs.at[at(s, c)],
            r.sem_br.at[at(s, c)],
            across,
        )

    def result_src(s, c):
        if s == 2:
            return full_of(s).at[own_rows(c)]
        return sent_of(s).at[kept(c)]

    def result_across(s, c):
        return remote(
            result_src(s, c),
            full_of(s).at[own_rows(c)],
            r.sem_cs.at[at(s, c)],
            r.sem_cr.at[at(s, c)],
            across,
        )

    def result_partner(s, c):
        return remote(
            result_src(s, c),
            full_of(s).at[own_rows(c)],
            r.sem_ps.at[at(s, c)],
            r.sem_pr.at[at(s, c)],
            partner,
        )

    def result_own(s, c):
        return pltpu.make_async_copy(
            sent_of(s).at[kept(c)], full_of(s).at[own_rows(c)], r.sem_o.at[at(s // 2, c)]
        )

    def forward(s, c):
        return remote(
            full_of(s).at[other_rows(c)],
            full_of(s).at[other_rows(c)],
            r.sem_ds.at[at(s, c)],
            r.sem_dr.at[at(s, c)],
            partner,
        )

    def step_b(s, c, send=True):
        copy = pair_copy(s, c)
        copy.wait_recv()
        copy.wait_send()
        part, pair = part_of(s), pair_of(s)
        slot, ring = c % 2, c % RING

        def piece(i, carry):
            rows = mult(i * 32, 32)
            away = pl.ds(mult(core * half + (1 - side) * quarter + rows, 32), 32)
            away_pair = pl.ds(mult((1 - side) * quarter + rows, 32), 32)
            total = part[slot, away, :].astype(F32) + pair[ring, away_pair, :].astype(F32)
            sent_of(s)[pl.ds(mult(c * quarter + rows, 32), 32), :] = total.astype(BF16)
            mine = pl.ds(mult(core * half + side * quarter + rows, 32), 32)
            mine_pair = pl.ds(mult(side * quarter + rows, 32), 32)
            total = part[slot, mine, :].astype(F32) + pair[ring, mine_pair, :].astype(F32)
            if s == 1:
                r.own_g[pl.ds(mult(c * quarter + rows, 32), 32), :] = total.astype(BF16)
            else:
                r.own[slot, pl.ds(rows, 32), :] = total
            return carry

        lax.fori_loop(0, quarter // 32, piece, 0, unroll=True)
        if send:
            across_copy(s, c).start()

    def step_c(s, c):
        copy = across_copy(s, c)
        copy.wait_recv()
        copy.wait_send()
        slot = c % 2

        def piece(i, carry):
            rows = mult(i * 32, 32)
            mine = pl.ds(mult(c * quarter + rows, 32), 32)
            full = pl.ds(mult(c * CHUNK + core * half + side * quarter + rows, 32), 32)
            arrived = got_of(s)[mine, :].astype(F32)
            if s == 1:
                total = r.own_g[mine, :].astype(F32) + arrived
            else:
                total = r.own[slot, pl.ds(rows, 32), :] + arrived
            if s == 1:
                r.sent_g[mine, :] = (r.hidden[mine, :] + total).astype(BF16)
            elif s == 2:
                hidden = r.hidden[mine, :]
                factor = rms_factor(hidden)
                d_hidden = r.cot[full, :].astype(F32) + norm_back(total, hidden * factor, factor)
                r.d_hidden[mine, :] = d_hidden
                r.do[full, :] = d_hidden.astype(BF16)
            else:
                held = pl.ds(mult(c * half + side * quarter + rows, 32), 32)
                source = r.tok_half[held, :].astype(F32)
                factor = rms_factor(source)
                d_source = r.d_hidden[mine, :] + norm_back(total, source * factor, factor)
                r.sent[mine, :] = d_source.astype(BF16)
            return carry

        lax.fori_loop(0, quarter // 32, piece, 0, unroll=True)
        result_across(s, c).start()
        result_partner(s, c).start()
        if s in (1, 3):
            result_own(s, c).start()

    def step_d(s, c):
        result_across(s, c).wait_recv()
        forward(s, c).start()

    def step_e(s, c):
        remote(
            result_src(s, c),
            full_of(s).at[partner_own_rows(c)],
            r.sem_ps.at[at(s, c)],
            r.sem_pr.at[at(s, c)],
            partner,
        ).wait_recv()
        remote(
            full_of(s).at[other_rows(c)],
            full_of(s).at[partner_other_rows(c)],
            r.sem_ds.at[at(s, c)],
            r.sem_dr.at[at(s, c)],
            partner,
        ).wait_recv()
        result_across(s, c).wait_send()
        result_partner(s, c).wait_send()
        forward(s, c).wait_send()
        if s in (1, 3):
            result_own(s, c).wait()

    def tick(s, c):
        @pl.when(c >= 1)
        def _():
            step_b(s, c - 1)

        @pl.when(c >= 2)
        def _():
            step_c(s, c - 2)

        @pl.when(c >= 3)
        def _():
            step_d(s, c - 3)

    def late_tick(s, n):
        if n == 0:
            step_b(s, chunks - 1)
        if n <= 1:
            step_c(s, chunks - 2 + n)
        step_d(s, chunks - 3 + n)

    def gated_across(c):
        here = r.do.at[pl.ds(base(c), CHUNK), group_of(mp)]
        return remote(here, here, r.sem_bs.at[c], r.sem_br.at[c], across)

    def gated_partner(c):
        here = r.do.at[pl.ds(base(c), CHUNK), group_of(mp)]
        return remote(here, here, r.sem_as.at[c], r.sem_ar.at[c], partner)

    def gated_forward(c):
        here = r.do.at[pl.ds(base(c), CHUNK), group_of(across_mp)]
        return remote(here, here, r.sem_ds.at[c], r.sem_dr.at[c], partner)

    def n2_partner(c):
        here = r.n2.at[half_rows(c)]
        return remote(here, here, r.sem_ps.at[c], r.sem_pr.at[c], partner)

    def gated_pass(c):
        gated_across(c).wait_recv()
        gated_forward(c).start()

    def gated_project(c):
        gated_partner(c).wait_recv()
        gated_forward(c).wait_recv()
        rows = half_rows(c)
        for t in range(width // 256):
            cols = pl.ds(t * 256, 256)
            total = dot_nn(r.do[rows, :], r.wof[:, cols])
            r.own[0, :, cols] = total[:quarter]
            r.own[1, :, cols] = total[quarter:]

        def piece(i, carry):
            q, sub = i // 2, mult((i % 2) * 32, 32)
            held = pl.ds(mult(c * half + i * 32, 32), 32)
            full = pl.ds(mult(c * CHUNK + core * half + i * 32, 32), 32)
            hidden = r.tok_half[held, :].astype(F32) + r.own[q, pl.ds(sub, 32), :]
            r.n2[full, :] = (hidden * rms_factor(hidden)).astype(BF16)

            @pl.when(q == side)
            def _():
                r.hidden[pl.ds(mult(c * quarter + sub, 32), 32), :] = hidden

            return carry

        lax.fori_loop(0, half // 32, piece, 0, unroll=True)
        n2_partner(c).start()

    def gated_end(c):
        n2_partner(c).wait_recv()
        for copy in (gated_across(c), gated_partner(c), gated_forward(c), n2_partner(c)):
            copy.wait_send()

    lane = lax.broadcasted_iota(jnp.int32, (TILE, TILE), 1)
    row = lax.broadcasted_iota(jnp.int32, (TILE, TILE), 0)
    first = lane < HD

    def stacked(v):
        zero = jnp.zeros_like(v)
        return jnp.concatenate([jnp.where(first, v, zero), jnp.where(first, zero, v)], axis=0)

    def unstacked(v):
        return jnp.where(first, v[:TILE], v[TILE:])

    def head_mean(v):
        zero = jnp.zeros_like(v)
        low = jnp.sum(jnp.where(first, v, zero), axis=-1, keepdims=True)
        high = jnp.sum(jnp.where(first, zero, v), axis=-1, keepdims=True)
        return jnp.where(first, low, high) * (1.0 / HD)

    def probs_of(tile, rows, lanes):
        ids = r.seg[pl.ds(tile, 1), :].astype(F32)
        across_ids = jnp.broadcast_to(ids, (TILE, TILE))
        allowed = (
            (across_ids == across_ids.T) & (lane <= row) & (lane // BLOCK == row // BLOCK)
        )
        stack = stacked(r.qkv[rows, pl.ds(lanes, TILE)])
        keys = r.qkv[rows, pl.ds(wc + lanes, TILE)]
        scores = dot_nt(stack, keys) * HD ** (-0.5)
        allowed2 = jnp.concatenate([allowed, allowed], axis=0)
        masked = jnp.where(allowed2, scores, F32(-1e30))
        top = jnp.max(masked, axis=-1, keepdims=True)
        expd = jnp.exp(masked - top)
        probs = expd * (1.0 / jnp.sum(expd, axis=-1, keepdims=True))
        return probs, stack, keys

    head_pairs = wc // TILE
    tiles = CHUNK // TILE

    def tile_of(c, i):
        tile = c * tiles + i // head_pairs
        lanes = mult((i % head_pairs) * TILE, TILE)
        rows = pl.ds(mult(tile * TILE, TILE), TILE)
        return tile, rows, lanes

    for copy in w_loads:
        copy.wait()

    def phase_one(c, carry):
        rows_all = pl.ds(base(c), CHUNK)
        load_tokens(c).wait()
        r.tok_half[pl.ds(mult(c * half, half), half), :] = r.n1[half_rows(c), :]

        def norm_piece(i, carry2):
            rows = pl.ds(mult(c * CHUNK + i * 32, 32), 32)
            x = r.n1[rows, :].astype(F32)
            r.n1[rows, :] = (x * rms_factor(x)).astype(BF16)
            return carry2

        lax.fori_loop(0, CHUNK // 32, norm_piece, 0)

        def project(t, carry2):
            cols = pl.ds(mult(t * wc, wc), wc)
            r.qkv[rows_all, cols] = dot_nn(r.n1[rows_all, :], r.w[:, cols]).astype(BF16)
            return carry2

        lax.fori_loop(0, 3, project, 0, unroll=True)
        r.gate_now[...] = dot_nn(r.n1[rows_all, :], r.w[:, pl.ds(3 * wc, wc)])
        r.gate[rows_all, :] = r.gate_now[...].astype(BF16)

        def attend(i, carry2):
            tile, rows, lanes = tile_of(c, i)
            probs, _, _ = probs_of(tile, rows, lanes)
            values = r.qkv[rows, pl.ds(2 * wc + lanes, TILE)]
            attended = unstacked(dot_nn(probs.astype(BF16), values))
            r.attended[rows, pl.ds(lanes, TILE)] = attended.astype(BF16)
            factor = lax.rsqrt(head_mean(attended * attended) + EPS)
            near = pl.ds(mult((i // head_pairs) * TILE, TILE), TILE)
            sigma = jax.nn.sigmoid(r.gate_now[near, pl.ds(lanes, TILE)])
            gated = (attended * factor * sigma).astype(BF16)
            r.gated[rows, pl.ds(lanes, TILE)] = gated
            r.do[rows, pl.ds(mult(mp * wc + lanes, TILE), TILE)] = gated
            return carry2

        lax.fori_loop(0, tiles * head_pairs, attend, 0, unroll=True)

        gated_across(c).start()
        gated_partner(c).start()

        @pl.when(c == 1)
        def _():
            wo_across().wait_recv()
            wo_forward().start()

        @pl.when(c >= 1)
        def _():
            gated_pass(c - 1)

        @pl.when(c == 2)
        def _():
            wo_load.wait()
            wo_partner().wait_recv()
            wo_forward().wait_recv()
            for copy in (wo_across(), wo_partner(), wo_forward()):
                copy.wait_send()

        @pl.when(c >= 2)
        def _():
            gated_project(c - 2)

        return carry

    lax.fori_loop(0, chunks, phase_one, 0)

    for copy in glu_loads:
        copy.wait()
    for weights in (r.wd, r.wl, r.wr):
        weights[pl.ds(ff, fp - ff), :] = jnp.zeros((fp - ff, width), BF16)
    cot_load.wait()

    def phase_two(c, carry):
        @pl.when(c == 0)
        def _():
            gated_pass(chunks - 1)
            gated_project(chunks - 2)

        @pl.when(c == 1)
        def _():
            gated_project(chunks - 1)

        gated_end(c)
        rows_all = pl.ds(base(c), CHUNK)
        rows_half = pl.ds(mult((c % half_chunks) * CHUNK, CHUNK), CHUNK)

        def hidden_units(t, carry2):
            cols = pl.ds(mult(t * 256, 256), 256)
            left = dot_nt(r.n2[rows_all, :], r.wl[cols, :])
            right = dot_nt(r.n2[rows_all, :], r.wr[cols, :])
            r.mixed[rows_all, cols] = (left * right).astype(BF16)
            d_mixed = dot_nt(r.cot[rows_all, :], r.wd[cols, :])
            r.d_left[rows_all, cols] = (d_mixed * right).astype(BF16)
            r.d_right[c // half_chunks, rows_half, cols] = (d_mixed * left).astype(BF16)
            return carry2

        lax.fori_loop(0, fp // 256, hidden_units, 0, unroll=True)

        def parts(t, carry2):
            cols = pl.ds(mult(t * 256, 256), 256)
            back = dot_nn(r.d_left[rows_all, :], r.wl[:, cols])
            back = back + dot_nn(r.d_right[c // half_chunks, rows_half, :], r.wr[:, cols])
            r.part[c % 2, :, cols] = back.astype(BF16)
            r.part_g[c % 2, :, cols] = dot_nn(r.mixed[rows_all, :], r.wd[:, cols]).astype(BF16)
            return carry2

        lax.fori_loop(0, width // 256, parts, 0, unroll=True)
        pair_copy(2, c).start()
        pair_copy(1, c).start()
        tick(2, c)

        @pl.when(c >= 1)
        def _():
            step_b(1, c - 1, send=False)

        return carry

    lax.fori_loop(0, chunks, phase_two, 0)
    late_tick(2, 0)
    step_b(1, chunks - 1, send=False)

    def send_glu(c, carry):
        across_copy(1, c).start()
        return carry

    lax.fori_loop(0, chunks, send_glu, 0)

    def transposed(src, i, dst):
        def piece(k, carry):
            rows = pl.ds(mult(k * 256, 256), 256)
            tile = src[rows, pl.ds(mult(i * 256, 256), 256)].T
            dst[k // 4, :, pl.ds(mult((k % 4) * 256, 256), 256)] = tile
            return carry

        lax.fori_loop(0, tokens // 256, piece, 0)

    def grad_of(turned, right, cols):
        total = None
        for k in range(2):
            rows = pl.ds(k * (tokens // 2), tokens // 2)
            operand = right[k, :, cols] if len(right.shape) == 3 else right[rows, cols]
            term = dot_nn(turned[k], operand)
            total = term if total is None else total + term
        return total.astype(BF16)

    def beside_copy(grads, arrivals, sems, g):
        block = 2 * g + 1 - parity
        send, recv = sems
        return remote(
            grads(pl.ds(mult(block * block_rows, block_rows), block_rows)),
            arrivals(pl.ds(mult(g * block_rows, block_rows), block_rows)),
            send.at[g],
            recv.at[g],
            beside,
        )

    def line_copy(grads, arrivals, sems, g):
        block = 2 * g + parity
        send, recv = sems
        return remote(
            grads(pl.ds(mult(block * block_rows, block_rows), block_rows)),
            arrivals(line),
            send.at[g],
            recv.at[line],
            (block, mp),
        )

    def glu_rows(rows):
        return r.grad_g.at[:, rows]

    def glu_beside(rows):
        return r.xg_h.at[:, rows]

    def glu_line(slot):
        return r.zg_h.at[slot]

    def att_rows(rows):
        return r.d_right.at[:, rows, pl.ds(0, wide)]

    def att_beside(rows):
        return r.xa_h.at[:, rows]

    def att_line(slot):
        return r.za_h.at[slot]

    glu_x = (glu_rows, glu_beside, (r.sem_xgs, r.sem_xgr))
    glu_z = (glu_rows, glu_line, (r.sem_zgs, r.sem_zgr))
    att_x = (att_rows, att_beside, (r.sem_xas, r.sem_xar))
    att_z = (att_rows, att_line, (r.sem_zas, r.sem_zar))

    def each(count, act):
        def one(j, carry):
            act(j)
            return carry

        if count == 1:
            act(0)
        else:
            lax.fori_loop(0, count, one, 0)

    def glu_group(i, carry):
        rows = pl.ds(mult(i * 256, 256), 256)
        transposed(r.n2, i, r.part)

        def sides(t, carry2):
            cols = pl.ds(mult(t * 256, 256), 256)
            r.grad_g[0, rows, cols] = grad_of(r.part, r.d_left, cols)
            r.grad_g[1, rows, cols] = grad_of(r.part, r.d_right, cols)
            return carry2

        lax.fori_loop(0, fp // 256, sides, 0, unroll=True)
        transposed(r.cot, i, r.part_g)

        def down(t, carry2):
            cols = pl.ds(mult(t * 256, 256), 256)
            r.grad_g[2, rows, cols] = grad_of(r.part_g, r.mixed, cols)
            return carry2

        lax.fori_loop(0, fp // 256, down, 0, unroll=True)
        each(per_group, lambda j: beside_copy(*glu_x, i * per_group + j).start())
        return carry

    lax.fori_loop(0, groups, glu_group, 0)

    def line_step(kinds, lanes, x, z, arrivals_h, stage, grads, g):
        copy = beside_copy(*x, g)
        copy.wait_recv()
        copy.wait_send()
        here = pl.ds(mult(g * block_rows, block_rows), block_rows)
        loads = []
        for t in range(kinds):
            load = pltpu.make_async_copy(
                arrivals_h.at[t, here],
                stage.at[pl.ds(t * block_rows, block_rows), pl.ds(0, lanes)],
                r.sem_stage.at[t],
            )
            load.start()
            loads.append(load)
        for load in loads:
            load.wait()
        step = min(16, block_rows)
        cols = pl.ds(0, lanes)

        for t in range(kinds):

            def piece(i, carry):
                sub = mult(i * step, step)
                there = pl.ds(mult((2 * g + parity) * block_rows + sub, step), step)
                mine = grads[t, there, cols].astype(F32)
                theirs = stage[pl.ds(mult(t * block_rows + sub, step), step), cols].astype(F32)
                grads[t, there, cols] = (mine + theirs).astype(BF16)
                return carry

            lax.fori_loop(0, block_rows // step, piece, 0)

        @pl.when(g != line)
        def _():
            line_copy(*z, g).start()

    def glu_line_step(g):
        line_step(3, fp, glu_x, glu_z, r.xg_h, r.mixed, r.grad_g, g)

    def att_line_step(g):
        line_step(2, wide, att_x, att_z, r.xa_h, r.d_left, r.d_right, g)

    def phase_three(c, carry):
        for n in range(2):

            @pl.when(c == n)
            def _():
                late_tick(2, n + 1)

        step_e(2, c)
        rows_all = pl.ds(base(c), CHUNK)
        r.gate_now[...] = dot_nt(r.do[rows_all, :], r.wof[group_of(mp), :])

        def attend_back(i, carry2):
            tile, rows, lanes = tile_of(c, i)
            near = pl.ds(mult((i // head_pairs) * TILE, TILE), TILE)
            here = pl.ds(lanes, TILE)
            d_gated = r.gate_now[near, here]
            sigma = jax.nn.sigmoid(r.gate[rows, here].astype(F32))
            attended = r.attended[rows, here].astype(F32)
            factor = lax.rsqrt(head_mean(attended * attended) + EPS)
            head_normed = attended * factor
            d_head = d_gated * sigma
            d_gate = d_head * head_normed * (1.0 - sigma)
            r.d_all[rows, pl.ds(3 * wc + lanes, TILE)] = d_gate.astype(BF16)
            d_att = factor * (d_head - head_normed * head_mean(d_head * head_normed))
            d_stack = stacked(d_att.astype(BF16))
            probs, stack, keys = probs_of(tile, rows, lanes)
            values = r.qkv[rows, pl.ds(2 * wc + lanes, TILE)]
            d_probs = dot_nt(d_stack, values)
            d_values = dot_tn(probs.astype(BF16), d_stack)
            r.d_all[rows, pl.ds(2 * wc + lanes, TILE)] = d_values.astype(BF16)
            delta = jnp.sum(probs * d_probs, axis=-1, keepdims=True)
            d_scores = (probs * (d_probs - delta)).astype(BF16)
            d_queries = unstacked(dot_nn(d_scores, keys)) * HD ** (-0.5)
            r.d_all[rows, here] = d_queries.astype(BF16)
            d_keys = dot_tn(d_scores, stack) * HD ** (-0.5)
            r.d_all[rows, pl.ds(wc + lanes, TILE)] = d_keys.astype(BF16)
            return carry2

        lax.fori_loop(0, tiles * head_pairs, attend_back, 0, unroll=True)

        def back_piece(t, carry2):
            cols = pl.ds(mult(t * 256, 256), 256)
            r.part[c % 2, :, cols] = dot_nt(r.d_all[rows_all, :], r.w[cols, :]).astype(BF16)
            return carry2

        lax.fori_loop(0, width // 256, back_piece, 0, unroll=True)
        pair_copy(3, c).start()
        tick(3, c)

        for i in range(groups):

            @pl.when(c == 2 * i + 1)
            def _():
                each(per_group, lambda j: glu_line_step(i * per_group + j))

        return carry

    lax.fori_loop(0, chunks, phase_three, 0)
    late_tick(3, 0)

    def att_group(i, carry):
        rows = pl.ds(mult(i * 256, 256), 256)
        transposed(r.n1, i, r.part_g)

        def store(t, total):
            for u in range(wc // 128):
                at_col = t * (wc // 128) + u
                cols = pl.ds(mult((at_col % (wide // 128)) * 128, 128), 128)
                r.d_right[at_col // (wide // 128), rows, cols] = total[:, u * 128 : u * 128 + 128]

        def four(t, carry2):
            store(t, grad_of(r.part_g, r.d_all, pl.ds(mult(t * wc, wc), wc)))
            return carry2

        lax.fori_loop(0, 4, four, 0, unroll=True)
        transposed(r.do, i, r.part_g)
        store(4, grad_of(r.part_g, r.gated, pl.ds(0, wc)))
        each(per_group, lambda j: beside_copy(*att_x, i * per_group + j).start())
        for n in range(2):

            @pl.when(i == n)
            def _():
                late_tick(3, n + 1)

        return carry

    lax.fori_loop(0, groups, att_group, 0)

    def glu_result(c, carry):
        step_c(1, c)
        return carry

    lax.fori_loop(0, chunks, glu_result, 0)

    def att_lines(g, carry):
        att_line_step(g)
        return carry

    lax.fori_loop(0, pairs, att_lines, 0)

    def glu_forward(c, carry):
        step_d(1, c)
        return carry

    lax.fori_loop(0, chunks, glu_forward, 0)

    def settle(z, sem):
        grads, arrivals, sems = z
        here = pl.ds(mult(dp * block_rows, block_rows), block_rows)
        mine = pltpu.make_async_copy(grads(here), arrivals(line), sem)
        mine.start()

        def arrived(j, carry):
            @pl.when(j != line)
            def _():
                remote(
                    grads(here), arrivals(j), sems[0].at[j], sems[1].at[j], (2 * j + parity, mp)
                ).wait_recv()
                line_copy(*z, j).wait_send()

            return carry

        lax.fori_loop(0, pairs, arrived, 0)
        mine.wait()

    settle(glu_z, r.sem_stage.at[0])
    settle(att_z, r.sem_stage.at[1])

    def ends(c, carry):
        step_e(1, c)
        step_e(3, c)
        return carry

    lax.fori_loop(0, chunks, ends, 0)


def fused(ndp, args):
    tokens, seg, wq, wk, wv, wg, wo, wl, wr, wd, cot = args
    rows, width = tokens.shape
    wc, ff = wq.shape[1], wl.shape[1]
    fp = (ff + 255) // 256 * 256
    chunks = rows // CHUNK
    quarter = CHUNK // 4
    own = rows // 4
    br = width // ndp
    pairs = ndp // 2
    wide = 5 * wc // 2
    hbm = pl.BlockSpec(memory_space=pl.ANY)
    vmem = pl.BlockSpec(memory_space=pltpu.VMEM)
    ins = [
        ("tok_h", tokens, hbm),
        ("seg", seg.reshape(rows // TILE, TILE), vmem),
        ("wq_h", wq, hbm),
        ("wk_h", wk, hbm),
        ("wv_h", wv, hbm),
        ("wg_h", wg, hbm),
        ("wo_h", wo, hbm),
        ("wl_h", wl.T, hbm),
        ("wr_h", wr.T, hbm),
        ("wd_h", wd, hbm),
        ("cot_h", cot, hbm),
    ]
    outs = [
        ("out_h", (rows, width), BF16, hbm),
        ("gt_h", (rows, width), BF16, hbm),
        ("xg_h", (3, pairs * br, fp), BF16, hbm),
        ("xa_h", (2, pairs * br, wide), BF16, hbm),
        ("zg_h", (pairs, 3, br, fp), BF16, hbm),
        ("za_h", (pairs, 2, br, wide), BF16, hbm),
    ]
    dma = pltpu.SemaphoreType.DMA
    scratch = [
        ("n1", pltpu.VMEM((rows, width), BF16)),
        ("tok_half", pltpu.VMEM((rows // 2, width), BF16)),
        ("cot", pltpu.VMEM((rows, width), BF16)),
        ("w", pltpu.VMEM((width, 4 * wc), BF16)),
        ("wof", pltpu.VMEM((width, width), BF16)),
        ("wl", pltpu.VMEM((fp, width), BF16)),
        ("wr", pltpu.VMEM((fp, width), BF16)),
        ("wd", pltpu.VMEM((fp, width), BF16)),
        ("qkv", pltpu.VMEM((rows, 3 * wc), BF16)),
        ("gate", pltpu.VMEM((rows, wc), BF16)),
        ("gate_now", pltpu.VMEM((CHUNK, wc), F32)),
        ("attended", pltpu.VMEM((rows, wc), BF16)),
        ("gated", pltpu.VMEM((rows, wc), BF16)),
        ("n2", pltpu.VMEM((rows, width), BF16)),
        ("mixed", pltpu.VMEM((rows, fp), BF16)),
        ("d_left", pltpu.VMEM((rows, fp), BF16)),
        ("d_right", pltpu.VMEM((2, rows // 2, fp), BF16)),
        ("do", pltpu.VMEM((rows, width), BF16)),
        ("part", pltpu.VMEM((2, CHUNK, width), BF16)),
        ("part_g", pltpu.VMEM((2, CHUNK, width), BF16)),
        ("pair", pltpu.VMEM((RING, CHUNK // 2, width), BF16)),
        ("pair_g", pltpu.VMEM((RING, CHUNK // 2, width), BF16)),
        ("sent", pltpu.VMEM((own, width), BF16)),
        ("sent_g", pltpu.VMEM((own, width), BF16)),
        ("got", pltpu.VMEM((own, width), BF16)),
        ("got_g", pltpu.VMEM((own, width), BF16)),
        ("own", pltpu.VMEM((2, quarter, width), F32)),
        ("own_g", pltpu.VMEM((own, width), BF16)),
        ("hidden", pltpu.VMEM((own, width), F32)),
        ("d_hidden", pltpu.VMEM((own, width), F32)),
        ("grad_g", pltpu.VMEM((3, width, fp), BF16)),
        ("sem_tok", dma((chunks,))),
        ("sem_w", dma((9,))),
        ("sem_stage", dma((3 * pairs,))),
    ]
    for name in ("as", "ar", "bs", "br", "cs", "cr", "ps", "pr", "ds", "dr"):
        scratch.append(("sem_" + name, dma((4 * chunks,))))
    scratch.append(("sem_wos", dma((3,))))
    scratch.append(("sem_wor", dma((3,))))
    scratch.append(("sem_o", dma((2 * chunks,))))
    for name in ("xgs", "xgr", "zgs", "zgr", "xas", "xar", "zas", "zar"):
        scratch.append(("sem_" + name, dma((pairs,))))
    names = [n for n, *_ in ins] + [n for n, *_ in outs] + [n for n, _ in scratch]

    def call(*refs):
        named = dict(zip(names, refs))
        named["d_all"] = named["n2"]
        kernel(list(named), ndp, *named.values())

    flops = 6 * rows * width * (5 * wc + 3 * ff)
    result = pl.pallas_call(
        call,
        out_shape=[jax.ShapeDtypeStruct(s, d) for _, s, d, _ in outs],
        in_specs=[s for *_, s in ins],
        out_specs=[s for *_, s in outs],
        scratch_shapes=[s for _, s in scratch],
        compiler_params=pltpu.CompilerParams(
            collective_id=0, has_side_effects=True, vmem_limit_bytes=67043328
        ),
        cost_estimate=pl.CostEstimate(flops=flops, bytes_accessed=1 << 25, transcendentals=1 << 22),
        name="fused_layer",
    )(*[a for _, a, _ in ins])
    return result[0], result[1], result[4], result[5]


def collect(br, wc, ff, refs):
    out_h, gt_h, zg_h, za_h = refs[:4]
    out_o, gt_o, *grads_o = refs[4:14]
    held, zg, za, sem_in, sem_out, sem_z, *grads = refs[14:]
    pairs = zg.shape[0]
    pieces = held.shape[1]
    rows = held.shape[2]
    loads = [
        pltpu.make_async_copy(zg_h, zg, sem_z.at[0]),
        pltpu.make_async_copy(za_h, za, sem_z.at[1]),
    ]
    moves = []
    for i in range(pieces):
        for k, (src, dst) in enumerate(((out_h, out_o), (gt_h, gt_o))):
            span = pl.ds(i * rows, rows)
            get = pltpu.make_async_copy(src.at[span], held.at[k, i], sem_in.at[k * pieces + i])
            put = pltpu.make_async_copy(held.at[k, i], dst.at[span], sem_out.at[k * pieces + i])
            moves.append((get, put))
    for copy in loads:
        copy.start()
    for get, _ in moves:
        get.start()
    for copy in loads:
        copy.wait()

    def total(ref, t, cols):
        value = ref[0, t, :, cols].astype(F32)
        for j in range(1, pairs):
            value = value + ref[j, t, :, cols].astype(F32)
        return value

    stores = [pltpu.make_async_copy(v, h, sem_z.at[2 + i]) for i, (v, h) in enumerate(zip(grads, grads_o))]
    wide = za.shape[3]
    todo = list(moves)

    def pump():
        if todo:
            get, put = todo.pop(0)
            get.wait()
            put.start()

    for kind in range(5):
        for u in range(wc // 128):
            at_col = kind * (wc // 128) + u
            col = (at_col % (wide // 128)) * 128
            value = total(za, at_col // (wide // 128), pl.ds(col, 128))
            if kind < 4:
                grads[kind][:, pl.ds(u * 128, 128)] = value
            else:
                grads[kind][pl.ds(u * 128, 128), :] = value.T
        stores[kind].start()
        pump()
    for t in range(3):
        for start in range(0, ff, 128):
            size = min(128, ff - start)
            value = total(zg, t, pl.ds(start, 128)).T
            grads[5 + t][pl.ds(start, size), :] = value[:size]
        stores[5 + t].start()
        pump()
    while todo:
        pump()
    for _, put in moves:
        put.wait()
    for copy in stores:
        copy.wait()


def collected(arrays, br, wc, ff):
    rows, width = arrays[0].shape
    pieces = 8
    hbm = pl.BlockSpec(memory_space=pl.ANY)
    dma = pltpu.SemaphoreType.DMA
    shapes = [(br, wc)] * 4 + [(wc, br)] + [(ff, br)] * 3
    outs = [((rows, width), BF16)] * 2 + [(s, F32) for s in shapes]
    return pl.pallas_call(
        lambda *refs: collect(br, wc, ff, refs),
        out_shape=[jax.ShapeDtypeStruct(s, d) for s, d in outs],
        in_specs=[hbm] * 4,
        out_specs=[hbm] * 10,
        scratch_shapes=[
            pltpu.VMEM((2, pieces, rows // pieces, width), BF16),
            pltpu.VMEM(arrays[2].shape, BF16),
            pltpu.VMEM(arrays[3].shape, BF16),
            dma((2 * pieces,)),
            dma((2 * pieces,)),
            dma((10,)),
        ]
        + [pltpu.VMEM(s, F32) for s in shapes],
        compiler_params=pltpu.CompilerParams(vmem_limit_bytes=67043328),
        name="collect",
    )(*arrays)


def body(ndp, *args):
    arrays = fused(ndp, args)
    ff, wc, width = args[7].shape[1], args[2].shape[1], args[0].shape[1]
    out, grad_tokens, query, key, value, gate, proj, left, right, down = collected(
        arrays, width // ndp, wc, ff
    )
    return out, grad_tokens, query, key, value, gate, proj, left.T, right.T, down


def solution(mesh):
    rows, cols, down = P("dp", None), P(None, "mp"), P("mp", None)
    grad = P("dp", "mp")
    return jax.shard_map(
        functools.partial(body, mesh.shape["dp"]),
        mesh=mesh,
        in_specs=(rows, rows, cols, cols, cols, cols, down, cols, cols, down, rows),
        out_specs=(rows, rows, grad, grad, grad, grad, P("mp", "dp"), grad, grad, P("mp", "dp")),
        check_vma=False,
    )
```

```python
import functools

import jax
import jax.numpy as jnp
from jax import lax
from jax.experimental import pallas as pl
from jax.experimental.pallas import tpu as pltpu
from jax.sharding import PartitionSpec as P

HD = 64
BLOCK = 64
CHUNK = 256
TILE = 128
RING = 4
EPS = 1e-06
EARLY = 4
FORWARD = 5
PASS = 3
F32 = jnp.float32
BF16 = jnp.bfloat16
MESH = pl.DeviceIdType.MESH


def dot_nn(a, b):
    return lax.dot_general(a, b, (((1,), (0,)), ((), ())), preferred_element_type=F32)


def dot_nt(a, b):
    return lax.dot_general(a, b, (((1,), (1,)), ((), ())), preferred_element_type=F32)


def dot_tn(a, b):
    return lax.dot_general(a, b, (((0,), (0,)), ((), ())), preferred_element_type=F32)


def rms_factor(v):
    return lax.rsqrt(jnp.mean(v * v, axis=-1, keepdims=True) + EPS)


def norm_back(grad, normed, factor):
    return factor * (grad - normed * jnp.mean(grad * normed, axis=-1, keepdims=True))


def mult(v, n):
    return pl.multiple_of(v, n)


class Refs:
    pass


def kernel(names, ndp, *refs):
    r = Refs()
    for name, ref in zip(names, refs):
        setattr(r, name, ref)
    tokens, width = r.n1.shape
    chunks = tokens // CHUNK
    half, quarter = CHUNK // 2, CHUNK // 4
    wc = r.wo_h.shape[0]
    fp, ff = r.wl.shape[0], r.wl_h.shape[0]
    block_rows = width // ndp
    pairs = ndp // 2
    groups = width // 256
    per_group = pairs // groups
    half_chunks = chunks // 2
    wide = 5 * wc // 2

    dp = lax.axis_index("dp")
    mp = lax.axis_index("mp")
    core = mp % 2
    side = mp // 2
    partner = (dp, mp + 1 - 2 * core)
    across = (dp, mp + 2 - 4 * side)
    parity = dp % 2
    line = dp // 2
    beside = (dp + 1 - 2 * parity, mp)

    def remote(src, dst, send, recv, device):
        return pltpu.make_async_remote_copy(
            src_ref=src,
            dst_ref=dst,
            send_sem=send,
            recv_sem=recv,
            device_id=device,
            device_id_type=MESH,
        )

    barrier = pltpu.get_barrier_semaphore()
    for device in (partner, across, beside):
        pl.semaphore_signal(barrier, inc=1, device_id=device, device_id_type=MESH)

    def greet(j, carry):
        @pl.when(j != line)
        def _():
            pl.semaphore_signal(
                barrier, inc=1, device_id=(2 * j + parity, mp), device_id_type=MESH
            )

        return carry

    lax.fori_loop(0, pairs, greet, 0)

    pair_mp = mp + 1 - 2 * core
    across_mp = mp + 2 - 4 * side

    def group_of(who):
        return pl.ds(mult(who * wc, wc), wc)

    def wo_across():
        there = r.wof.at[group_of(mp)]
        return remote(r.wo_h, there, r.sem_wos.at[0], r.sem_wor.at[0], across)

    def wo_partner():
        there = r.wof.at[group_of(mp)]
        return remote(r.wo_h, there, r.sem_wos.at[1], r.sem_wor.at[1], partner)

    def wo_forward():
        here = r.wof.at[group_of(across_mp)]
        return remote(here, here, r.sem_wos.at[2], r.sem_wor.at[2], partner)

    def load_tokens(c):
        rows = pl.ds(mult(c * CHUNK, CHUNK), CHUNK)
        return pltpu.make_async_copy(r.tok_h.at[rows], r.n1.at[rows], r.sem_tok.at[c])

    load_tokens(0).start()
    w_loads = [
        pltpu.make_async_copy(h, r.w.at[:, pl.ds(i * wc, wc)], r.sem_w.at[i])
        for i, h in enumerate((r.wq_h, r.wk_h, r.wv_h, r.wg_h))
    ]
    for copy in w_loads:
        copy.start()
    wo_load = pltpu.make_async_copy(
        r.wo_h, r.wof.at[pl.ds(mult(mp * wc, wc), wc)], r.sem_w.at[4]
    )
    wo_load.start()
    for c in range(1, chunks):
        load_tokens(c).start()
    glu_loads = [
        pltpu.make_async_copy(h, v.at[pl.ds(0, ff)], r.sem_w.at[i])
        for i, h, v in ((5, r.wd_h, r.wd), (6, r.wl_h, r.wl), (7, r.wr_h, r.wr))
    ]
    for copy in glu_loads:
        copy.start()
    cot_load = pltpu.make_async_copy(r.cot_h, r.cot, r.sem_w.at[8])
    cot_load.start()

    pl.semaphore_wait(barrier, 3 + pairs - 1)
    for copy in (wo_across(), wo_partner()):
        copy.start()

    def base(c):
        return mult(c * CHUNK, CHUNK)

    def half_rows(c):
        return pl.ds(mult(c * CHUNK + core * half, half), half)

    def own_rows(c):
        return pl.ds(mult(c * CHUNK + core * half + side * quarter, quarter), quarter)

    def other_rows(c):
        return pl.ds(mult(c * CHUNK + core * half + (1 - side) * quarter, quarter), quarter)

    def partner_own_rows(c):
        return pl.ds(mult(c * CHUNK + (1 - core) * half + side * quarter, quarter), quarter)

    def partner_other_rows(c):
        return pl.ds(mult(c * CHUNK + (1 - core) * half + (1 - side) * quarter, quarter), quarter)

    def kept(c):
        return pl.ds(mult(c * quarter, quarter), quarter)

    def part_of(s):
        return r.part_g if s == 1 else r.part

    def pair_of(s):
        return r.pair_g if s == 1 else r.pair

    def sent_of(s):
        return r.sent_g if s == 1 else r.sent

    def got_of(s):
        return r.got_g if s == 1 else r.got

    def full_of(s):
        return (None, r.out_h, r.do, r.gt_h)[s]

    def at(s, c):
        return s * chunks + c

    def pair_copy(s, c):
        slot = c % RING
        return remote(
            part_of(s).at[c % 2, pl.ds(mult((1 - core) * half, half), half)],
            pair_of(s).at[slot],
            r.sem_as.at[at(s, c)],
            r.sem_ar.at[at(s, c)],
            partner,
        )

    def across_copy(s, c):
        return remote(
            sent_of(s).at[kept(c)],
            got_of(s).at[kept(c)],
            r.sem_bs.at[at(s, c)],
            r.sem_br.at[at(s, c)],
            across,
        )

    def result_src(s, c):
        if s == 2:
            return full_of(s).at[own_rows(c)]
        return sent_of(s).at[kept(c)]

    def result_across(s, c):
        return remote(
            result_src(s, c),
            full_of(s).at[own_rows(c)],
            r.sem_cs.at[at(s, c)],
            r.sem_cr.at[at(s, c)],
            across,
        )

    def result_partner(s, c):
        return remote(
            result_src(s, c),
            full_of(s).at[own_rows(c)],
            r.sem_ps.at[at(s, c)],
            r.sem_pr.at[at(s, c)],
            partner,
        )

    def result_own(s, c):
        return pltpu.make_async_copy(
            sent_of(s).at[kept(c)], full_of(s).at[own_rows(c)], r.sem_o.at[at(s // 2, c)]
        )

    def forward(s, c):
        return remote(
            full_of(s).at[other_rows(c)],
            full_of(s).at[other_rows(c)],
            r.sem_ds.at[at(s, c)],
            r.sem_dr.at[at(s, c)],
            partner,
        )

    def step_b(s, c, send=True):
        copy = pair_copy(s, c)
        copy.wait_recv()
        copy.wait_send()
        part, pair = part_of(s), pair_of(s)
        slot, ring = c % 2, c % RING

        def piece(i, carry):
            rows = mult(i * 32, 32)
            away = pl.ds(mult(core * half + (1 - side) * quarter + rows, 32), 32)
            away_pair = pl.ds(mult((1 - side) * quarter + rows, 32), 32)
            total = part[slot, away, :].astype(F32) + pair[ring, away_pair, :].astype(F32)
            sent_of(s)[pl.ds(mult(c * quarter + rows, 32), 32), :] = total.astype(BF16)
            mine = pl.ds(mult(core * half + side * quarter + rows, 32), 32)
            mine_pair = pl.ds(mult(side * quarter + rows, 32), 32)
            total = part[slot, mine, :].astype(F32) + pair[ring, mine_pair, :].astype(F32)
            if s == 1:
                r.own_g[pl.ds(mult(c * quarter + rows, 32), 32), :] = total.astype(BF16)
            else:
                r.own[slot, pl.ds(rows, 32), :] = total
            return carry

        lax.fori_loop(0, quarter // 32, piece, 0, unroll=True)
        if send:
            across_copy(s, c).start()

    def step_c(s, c):
        copy = across_copy(s, c)
        copy.wait_recv()
        copy.wait_send()
        slot = c % 2

        def piece(i, carry):
            rows = mult(i * 32, 32)
            mine = pl.ds(mult(c * quarter + rows, 32), 32)
            full = pl.ds(mult(c * CHUNK + core * half + side * quarter + rows, 32), 32)
            arrived = got_of(s)[mine, :].astype(F32)
            if s == 1:
                total = r.own_g[mine, :].astype(F32) + arrived
            else:
                total = r.own[slot, pl.ds(rows, 32), :] + arrived
            if s == 1:
                r.sent_g[mine, :] = (r.hidden[mine, :] + total).astype(BF16)
            elif s == 2:
                hidden = r.hidden[mine, :]
                factor = rms_factor(hidden)
                d_hidden = r.cot[full, :].astype(F32) + norm_back(total, hidden * factor, factor)
                r.d_hidden[mine, :] = d_hidden
                r.do[full, :] = d_hidden.astype(BF16)
            else:
                held = pl.ds(mult(c * half + side * quarter + rows, 32), 32)
                source = r.tok_half[held, :].astype(F32)
                factor = rms_factor(source)
                d_source = r.d_hidden[mine, :] + norm_back(total, source * factor, factor)
                r.sent[mine, :] = d_source.astype(BF16)
            return carry

        lax.fori_loop(0, quarter // 32, piece, 0, unroll=True)
        result_across(s, c).start()
        result_partner(s, c).start()
        if s in (1, 3):
            result_own(s, c).start()

    def step_d(s, c):
        result_across(s, c).wait_recv()
        forward(s, c).start()

    def step_e(s, c):
        remote(
            result_src(s, c),
            full_of(s).at[partner_own_rows(c)],
            r.sem_ps.at[at(s, c)],
            r.sem_pr.at[at(s, c)],
            partner,
        ).wait_recv()
        remote(
            full_of(s).at[other_rows(c)],
            full_of(s).at[partner_other_rows(c)],
            r.sem_ds.at[at(s, c)],
            r.sem_dr.at[at(s, c)],
            partner,
        ).wait_recv()
        result_across(s, c).wait_send()
        result_partner(s, c).wait_send()
        forward(s, c).wait_send()
        if s in (1, 3):
            result_own(s, c).wait()

    def tick(s, c):
        @pl.when(c >= 1)
        def _():
            step_b(s, c - 1)

        @pl.when(c >= 2)
        def _():
            step_c(s, c - 2)

        @pl.when(c >= FORWARD)
        def _():
            step_d(s, c - FORWARD)

    def late_tick(s, n):
        if n == 0:
            step_b(s, chunks - 1)
        if n <= 1:
            step_c(s, chunks - 2 + n)
        step_d(s, chunks - FORWARD + n)

    def gated_across(c):
        here = r.do.at[pl.ds(base(c), CHUNK), group_of(mp)]
        return remote(here, here, r.sem_bs.at[c], r.sem_br.at[c], across)

    def gated_partner(c):
        here = r.do.at[pl.ds(base(c), CHUNK), group_of(mp)]
        return remote(here, here, r.sem_as.at[c], r.sem_ar.at[c], partner)

    def gated_forward(c):
        here = r.do.at[pl.ds(base(c), CHUNK), group_of(across_mp)]
        return remote(here, here, r.sem_ds.at[c], r.sem_dr.at[c], partner)

    def n2_partner(c):
        here = r.n2.at[half_rows(c)]
        return remote(here, here, r.sem_ps.at[c], r.sem_pr.at[c], partner)

    def gated_pass(c):
        gated_across(c).wait_recv()
        gated_forward(c).start()

    def gated_project(c):
        gated_partner(c).wait_recv()
        gated_forward(c).wait_recv()
        rows = half_rows(c)
        for t in range(width // 256):
            cols = pl.ds(t * 256, 256)
            total = dot_nn(r.do[rows, :], r.wof[:, cols])
            r.branch[:, cols] = total

        def piece(i, carry):
            q, sub = i // 2, mult((i % 2) * 32, 32)
            held = pl.ds(mult(c * half + i * 32, 32), 32)
            full = pl.ds(mult(c * CHUNK + core * half + i * 32, 32), 32)
            hidden = r.tok_half[held, :].astype(F32) + r.branch[pl.ds(mult(i * 32, 32), 32), :]
            r.n2[full, :] = (hidden * rms_factor(hidden)).astype(BF16)

            @pl.when(q == side)
            def _():
                r.hidden[pl.ds(mult(c * quarter + sub, 32), 32), :] = hidden

            return carry

        lax.fori_loop(0, half // 32, piece, 0, unroll=True)
        n2_partner(c).start()

    def gated_end(c):
        n2_partner(c).wait_recv()
        for copy in (gated_across(c), gated_partner(c), gated_forward(c), n2_partner(c)):
            copy.wait_send()

    lane = lax.broadcasted_iota(jnp.int32, (TILE, TILE), 1)
    row = lax.broadcasted_iota(jnp.int32, (TILE, TILE), 0)
    first = lane < HD

    def stacked(v):
        zero = jnp.zeros_like(v)
        return jnp.concatenate([jnp.where(first, v, zero), jnp.where(first, zero, v)], axis=0)

    def unstacked(v):
        return jnp.where(first, v[:TILE], v[TILE:])

    def head_mean(v):
        zero = jnp.zeros_like(v)
        low = jnp.sum(jnp.where(first, v, zero), axis=-1, keepdims=True)
        high = jnp.sum(jnp.where(first, zero, v), axis=-1, keepdims=True)
        return jnp.where(first, low, high) * (1.0 / HD)

    def probs_of(tile, rows, lanes):
        ids = r.seg[pl.ds(tile, 1), :].astype(F32)
        across_ids = jnp.broadcast_to(ids, (TILE, TILE))
        allowed = (
            (across_ids == across_ids.T) & (lane <= row) & (lane // BLOCK == row // BLOCK)
        )
        stack = stacked(r.qkv[rows, pl.ds(lanes, TILE)])
        keys = r.qkv[rows, pl.ds(wc + lanes, TILE)]
        scores = dot_nt(stack, keys) * HD ** (-0.5)
        allowed2 = jnp.concatenate([allowed, allowed], axis=0)
        masked = jnp.where(allowed2, scores, F32(-1e30))
        top = jnp.max(masked, axis=-1, keepdims=True)
        expd = jnp.exp(masked - top)
        probs = expd * (1.0 / jnp.sum(expd, axis=-1, keepdims=True))
        return probs, stack, keys

    head_pairs = wc // TILE
    tiles = CHUNK // TILE

    def tile_of(c, i):
        tile = c * tiles + i // head_pairs
        lanes = mult((i % head_pairs) * TILE, TILE)
        rows = pl.ds(mult(tile * TILE, TILE), TILE)
        return tile, rows, lanes

    def beside_copy(grads, arrivals, sems, g):
        block = 2 * g + 1 - parity
        send, recv = sems
        return remote(
            grads(pl.ds(mult(block * block_rows, block_rows), block_rows)),
            arrivals(pl.ds(mult(g * block_rows, block_rows), block_rows)),
            send.at[g],
            recv.at[g],
            beside,
        )

    def line_copy(grads, arrivals, sems, g):
        block = 2 * g + parity
        send, recv = sems
        return remote(
            grads(pl.ds(mult(block * block_rows, block_rows), block_rows)),
            arrivals(line),
            send.at[g],
            recv.at[line],
            (block, mp),
        )

    def glu_rows(rows):
        return r.grad_g.at[:, rows]

    def glu_beside(rows):
        return r.xg_h.at[:, rows]

    def glu_line(slot):
        return r.zg_h.at[slot]

    def att_rows(rows):
        return r.d_right.at[:, rows, pl.ds(0, wide)]

    def att_beside(rows):
        return r.xa_h.at[:, rows]

    def att_line(slot):
        return r.za_h.at[slot]

    glu_x = (glu_rows, glu_beside, (r.sem_xgs, r.sem_xgr))
    glu_z = (glu_rows, glu_line, (r.sem_zgs, r.sem_zgr))
    att_x = (att_rows, att_beside, (r.sem_xas, r.sem_xar))
    att_z = (att_rows, att_line, (r.sem_zas, r.sem_zar))

    def each(count, act):
        def one(j, carry):
            act(j)
            return carry

        if count == 1:
            act(0)
        else:
            lax.fori_loop(0, count, one, 0)

    def turn(k):
        return (line // per_group + 1 + k) % groups

    def turned_half(src, i, h):
        for k in range(tokens // 512):
            rows = pl.ds(h * (tokens // 2) + k * 256, 256)
            r.turned[:, pl.ds(k * 256, 256)] = src[rows, pl.ds(mult(i * 256, 256), 256)].T

    def gathered(h, old, term):
        return (term if h == 0 else old.astype(F32) + term).astype(BF16)

    def glu_half(i, h):
        rows = pl.ds(mult(i * 256, 256), 256)
        half_rows_all = pl.ds(h * (tokens // 2), tokens // 2)
        turned_half(r.n2, i, h)
        for t in range(fp // 256):
            cols = pl.ds(t * 256, 256)
            term = dot_nn(r.turned[...], r.d_left[half_rows_all, cols])
            r.grad_g[0, rows, cols] = gathered(h, r.grad_g[0, rows, cols], term)
            term = dot_nn(r.turned[...], r.d_right[h, :, cols])
            r.grad_g[1, rows, cols] = gathered(h, r.grad_g[1, rows, cols], term)
        turned_half(r.cot, i, h)
        for t in range(fp // 256):
            cols = pl.ds(t * 256, 256)
            term = dot_nn(r.turned[...], r.mixed[half_rows_all, cols])
            r.grad_g[2, rows, cols] = gathered(h, r.grad_g[2, rows, cols], term)

    def att_half(i, h):
        rows = pl.ds(mult(i * 256, 256), 256)
        half_rows_all = pl.ds(h * (tokens // 2), tokens // 2)

        def store(kind, term):
            for u in range(wc // 128):
                at_col = kind * (wc // 128) + u
                cols = pl.ds((at_col % (wide // 128)) * 128, 128)
                place = at_col // (wide // 128)
                piece = term[:, u * 128 : u * 128 + 128]
                r.d_right[place, rows, cols] = gathered(h, r.d_right[place, rows, cols], piece)

        turned_half(r.n1, i, h)
        for kind in range(4):
            cols = pl.ds(kind * wc, wc)
            store(kind, dot_nn(r.turned[...], r.d_all[half_rows_all, cols]))
        turned_half(r.do, i, h)
        store(4, dot_nn(r.turned[...], r.gated[half_rows_all, :]))

    for copy in w_loads:
        copy.wait()

    def phase_one(c, carry):
        rows_all = pl.ds(base(c), CHUNK)
        load_tokens(c).wait()
        r.tok_half[pl.ds(mult(c * half, half), half), :] = r.n1[half_rows(c), :]

        def norm_piece(i, carry2):
            rows = pl.ds(mult(c * CHUNK + i * 32, 32), 32)
            x = r.n1[rows, :].astype(F32)
            r.n1[rows, :] = (x * rms_factor(x)).astype(BF16)
            return carry2

        lax.fori_loop(0, CHUNK // 32, norm_piece, 0)

        def project(t, carry2):
            cols = pl.ds(mult(t * wc, wc), wc)
            r.qkv[rows_all, cols] = dot_nn(r.n1[rows_all, :], r.w[:, cols]).astype(BF16)
            return carry2

        lax.fori_loop(0, 3, project, 0, unroll=True)
        r.gate_now[...] = dot_nn(r.n1[rows_all, :], r.w[:, pl.ds(3 * wc, wc)])
        r.gate[rows_all, :] = r.gate_now[...].astype(BF16)

        def attend(i, carry2):
            tile, rows, lanes = tile_of(c, i)
            probs, _, _ = probs_of(tile, rows, lanes)
            values = r.qkv[rows, pl.ds(2 * wc + lanes, TILE)]
            attended = unstacked(dot_nn(probs.astype(BF16), values))
            r.attended[rows, pl.ds(lanes, TILE)] = attended.astype(BF16)
            factor = lax.rsqrt(head_mean(attended * attended) + EPS)
            near = pl.ds(mult((i // head_pairs) * TILE, TILE), TILE)
            sigma = jax.nn.sigmoid(r.gate_now[near, pl.ds(lanes, TILE)])
            gated = (attended * factor * sigma).astype(BF16)
            r.gated[rows, pl.ds(lanes, TILE)] = gated
            r.do[rows, pl.ds(mult(mp * wc + lanes, TILE), TILE)] = gated
            return carry2

        lax.fori_loop(0, tiles * head_pairs, attend, 0, unroll=True)

        gated_across(c).start()
        gated_partner(c).start()

        @pl.when(c == PASS - 1)
        def _():
            wo_across().wait_recv()
            wo_forward().start()

        @pl.when(c >= PASS)
        def _():
            gated_pass(c - PASS)

        @pl.when(c == PASS + 1)
        def _():
            wo_load.wait()
            wo_partner().wait_recv()
            wo_forward().wait_recv()
            for copy in (wo_across(), wo_partner(), wo_forward()):
                copy.wait_send()

        @pl.when(c >= PASS + 1)
        def _():
            gated_project(c - PASS - 1)

        return carry

    lax.fori_loop(0, chunks, phase_one, 0)

    for copy in glu_loads:
        copy.wait()
    for weights in (r.wd, r.wl, r.wr):
        weights[pl.ds(ff, fp - ff), :] = jnp.zeros((fp - ff, width), BF16)
    cot_load.wait()

    def phase_two(c, carry):
        @pl.when(c < PASS)
        def _():
            gated_pass(chunks - PASS + c)

        @pl.when(c <= PASS)
        def _():
            gated_project(chunks - PASS - 1 + c)

        gated_end(c)
        rows_all = pl.ds(base(c), CHUNK)
        rows_half = pl.ds(mult((c % half_chunks) * CHUNK, CHUNK), CHUNK)

        def hidden_units(t, carry2):
            cols = pl.ds(mult(t * 256, 256), 256)
            left = dot_nt(r.n2[rows_all, :], r.wl[cols, :])
            right = dot_nt(r.n2[rows_all, :], r.wr[cols, :])
            r.mixed[rows_all, cols] = (left * right).astype(BF16)
            d_mixed = dot_nt(r.cot[rows_all, :], r.wd[cols, :])
            r.d_left[rows_all, cols] = (d_mixed * right).astype(BF16)
            r.d_right[c // half_chunks, rows_half, cols] = (d_mixed * left).astype(BF16)
            return carry2

        lax.fori_loop(0, fp // 256, hidden_units, 0, unroll=True)

        def parts(t, carry2):
            cols = pl.ds(mult(t * 256, 256), 256)
            back = dot_nn(r.d_left[rows_all, :], r.wl[:, cols])
            back = back + dot_nn(r.d_right[c // half_chunks, rows_half, :], r.wr[:, cols])
            r.part[c % 2, :, cols] = back.astype(BF16)
            r.part_g[c % 2, :, cols] = dot_nn(r.mixed[rows_all, :], r.wd[:, cols]).astype(BF16)
            return carry2

        lax.fori_loop(0, width // 256, parts, 0, unroll=True)
        pair_copy(2, c).start()
        pair_copy(1, c).start()

        @pl.when(c >= half_chunks)
        def _():
            glu_half(turn(c - half_chunks), 0)

        tick(2, c)

        @pl.when(c >= 1)
        def _():
            step_b(1, c - 1, send=False)

        return carry

    lax.fori_loop(0, chunks, phase_two, 0)
    late_tick(2, 0)
    step_b(1, chunks - 1, send=False)

    def send_glu(c, carry):
        across_copy(1, c).start()
        return carry

    lax.fori_loop(0, EARLY, send_glu, 0)

    def glu_group(k, carry):
        i = turn(k)
        glu_half(i, 1)
        each(per_group, lambda j: beside_copy(*glu_x, i * per_group + j).start())
        for n in range(FORWARD - 1):

            @pl.when(k == n)
            def _():
                late_tick(2, n + 1)

        return carry

    lax.fori_loop(0, groups, glu_group, 0)

    def line_loads(kinds, lanes, arrivals_h, stage, g):
        here = pl.ds(mult(g * block_rows, block_rows), block_rows)
        return [
            pltpu.make_async_copy(
                arrivals_h.at[t, here],
                stage.at[pl.ds(t * block_rows, block_rows), pl.ds(0, lanes)],
                r.sem_stage.at[t],
            )
            for t in range(kinds)
        ]

    def line_arrive(kinds, lanes, x, z, arrivals_h, stage, grads, g):
        copy = beside_copy(*x, g)
        copy.wait_recv()
        copy.wait_send()
        for load in line_loads(kinds, lanes, arrivals_h, stage, g):
            load.start()

    def line_sum(kinds, lanes, x, z, arrivals_h, stage, grads, g):
        for load in line_loads(kinds, lanes, arrivals_h, stage, g):
            load.wait()
        step = min(16, block_rows)
        cols = pl.ds(0, lanes)

        def piece(i, carry):
            sub = mult(i * step, step)
            there = pl.ds(mult((2 * g + parity) * block_rows + sub, step), step)
            for t in range(kinds):
                mine = grads[t, there, cols].astype(F32)
                theirs = stage[pl.ds(mult(t * block_rows + sub, step), step), cols].astype(F32)
                grads[t, there, cols] = (mine + theirs).astype(BF16)
            return carry

        lax.fori_loop(0, block_rows // step, piece, 0)

        @pl.when(g != line)
        def _():
            line_copy(*z, g).start()

    glu_line = (3, fp, glu_x, glu_z, r.xg_h, r.mixed, r.grad_g)
    att_line_of = (2, wide, att_x, att_z, r.xa_h, r.d_left, r.d_right)

    def line_both(what, k):
        if per_group == 1:
            line_sum(*what, turn(k))
            return

        def one(j):
            g = turn(k) * per_group + j
            line_arrive(*what, g)
            line_sum(*what, g)

        each(per_group, one)

    def line_start(what, k):
        if per_group == 1:
            line_arrive(*what, turn(k))

    def phase_three(c, carry):
        step_e(2, c)
        rows_all = pl.ds(base(c), CHUNK)
        r.gate_now[...] = dot_nt(r.do[rows_all, :], r.wof[group_of(mp), :])

        def attend_back(i, carry2):
            tile, rows, lanes = tile_of(c, i)
            near = pl.ds(mult((i // head_pairs) * TILE, TILE), TILE)
            here = pl.ds(lanes, TILE)
            d_gated = r.gate_now[near, here]
            sigma = jax.nn.sigmoid(r.gate[rows, here].astype(F32))
            attended = r.attended[rows, here].astype(F32)
            factor = lax.rsqrt(head_mean(attended * attended) + EPS)
            head_normed = attended * factor
            d_head = d_gated * sigma
            d_gate = d_head * head_normed * (1.0 - sigma)
            r.d_all[rows, pl.ds(3 * wc + lanes, TILE)] = d_gate.astype(BF16)
            d_att = factor * (d_head - head_normed * head_mean(d_head * head_normed))
            d_stack = stacked(d_att.astype(BF16))
            probs, stack, keys = probs_of(tile, rows, lanes)
            values = r.qkv[rows, pl.ds(2 * wc + lanes, TILE)]
            d_probs = dot_nt(d_stack, values)
            d_values = dot_tn(probs.astype(BF16), d_stack)
            r.d_all[rows, pl.ds(2 * wc + lanes, TILE)] = d_values.astype(BF16)
            delta = jnp.sum(probs * d_probs, axis=-1, keepdims=True)
            d_scores = (probs * (d_probs - delta)).astype(BF16)
            d_queries = unstacked(dot_nn(d_scores, keys)) * HD ** (-0.5)
            r.d_all[rows, here] = d_queries.astype(BF16)
            d_keys = dot_tn(d_scores, stack) * HD ** (-0.5)
            r.d_all[rows, pl.ds(wc + lanes, TILE)] = d_keys.astype(BF16)
            return carry2

        lax.fori_loop(0, tiles * head_pairs, attend_back, 0, unroll=True)

        def back_piece(t, carry2):
            cols = pl.ds(mult(t * 256, 256), 256)
            r.part[c % 2, :, cols] = dot_nt(r.d_all[rows_all, :], r.w[cols, :]).astype(BF16)
            return carry2

        lax.fori_loop(0, width // 256, back_piece, 0, unroll=True)
        pair_copy(3, c).start()

        @pl.when(c >= half_chunks)
        def _():
            att_half(turn(c - half_chunks), 0)

        tick(3, c)

        for i in range(groups):

            @pl.when(c == 2 * i + 1)
            def _():
                line_start(glu_line, i)

            if i > 0:

                @pl.when(c == 2 * i)
                def _():
                    line_both(glu_line, i - 1)

        return carry

    lax.fori_loop(0, chunks, phase_three, 0)
    late_tick(3, 0)

    line_both(glu_line, groups - 1)
    lax.fori_loop(EARLY, chunks, send_glu, 0)

    def att_group(k, carry):
        i = turn(k)
        att_half(i, 1)
        each(per_group, lambda j: beside_copy(*att_x, i * per_group + j).start())
        for n in range(FORWARD - 1):

            @pl.when(k == n)
            def _():
                late_tick(3, n + 1)

        return carry

    lax.fori_loop(0, groups, att_group, 0)

    def glu_result(c, carry):
        step_c(1, c)
        return carry

    lax.fori_loop(0, EARLY, glu_result, 0)

    def att_lines(k, carry):
        line_start(att_line_of, k)
        first_left = EARLY + k * (chunks - EARLY) // groups
        last_left = EARLY + (k + 1) * (chunks - EARLY) // groups
        lax.fori_loop(first_left, last_left, glu_result, 0)
        line_both(att_line_of, k)
        return carry

    lax.fori_loop(0, groups, att_lines, 0)

    def glu_forward(c, carry):
        step_d(1, c)
        return carry

    lax.fori_loop(0, chunks, glu_forward, 0)

    def settle(z, sem):
        grads, arrivals, sems = z
        here = pl.ds(mult(dp * block_rows, block_rows), block_rows)
        mine = pltpu.make_async_copy(grads(here), arrivals(line), sem)
        mine.start()

        def arrived(j, carry):
            @pl.when(j != line)
            def _():
                remote(
                    grads(here), arrivals(j), sems[0].at[j], sems[1].at[j], (2 * j + parity, mp)
                ).wait_recv()
                line_copy(*z, j).wait_send()

            return carry

        lax.fori_loop(0, pairs, arrived, 0)
        mine.wait()

    settle(glu_z, r.sem_stage.at[0])
    settle(att_z, r.sem_stage.at[1])

    def ends(c, carry):
        step_e(1, c)
        step_e(3, c)
        return carry

    lax.fori_loop(0, chunks, ends, 0)


def fused(ndp, args):
    tokens, seg, wq, wk, wv, wg, wo, wl, wr, wd, cot = args
    rows, width = tokens.shape
    wc, ff = wq.shape[1], wl.shape[1]
    fp = (ff + 255) // 256 * 256
    chunks = rows // CHUNK
    quarter = CHUNK // 4
    own = rows // 4
    br = width // ndp
    pairs = ndp // 2
    wide = 5 * wc // 2
    hbm = pl.BlockSpec(memory_space=pl.ANY)
    vmem = pl.BlockSpec(memory_space=pltpu.VMEM)
    ins = [
        ("tok_h", tokens, hbm),
        ("seg", seg.reshape(rows // TILE, TILE), vmem),
        ("wq_h", wq, hbm),
        ("wk_h", wk, hbm),
        ("wv_h", wv, hbm),
        ("wg_h", wg, hbm),
        ("wo_h", wo, hbm),
        ("wl_h", wl.T, hbm),
        ("wr_h", wr.T, hbm),
        ("wd_h", wd, hbm),
        ("cot_h", cot, hbm),
    ]
    outs = [
        ("out_h", (rows, width), BF16, hbm),
        ("gt_h", (rows, width), BF16, hbm),
        ("xg_h", (3, pairs * br, fp), BF16, hbm),
        ("xa_h", (2, pairs * br, wide), BF16, hbm),
        ("zg_h", (pairs, 3, br, fp), BF16, hbm),
        ("za_h", (pairs, 2, br, wide), BF16, hbm),
    ]
    dma = pltpu.SemaphoreType.DMA
    scratch = [
        ("n1", pltpu.VMEM((rows, width), BF16)),
        ("tok_half", pltpu.VMEM((rows // 2, width), BF16)),
        ("cot", pltpu.VMEM((rows, width), BF16)),
        ("w", pltpu.VMEM((width, 4 * wc), BF16)),
        ("wof", pltpu.VMEM((width, width), BF16)),
        ("wl", pltpu.VMEM((fp, width), BF16)),
        ("wr", pltpu.VMEM((fp, width), BF16)),
        ("wd", pltpu.VMEM((fp, width), BF16)),
        ("qkv", pltpu.VMEM((rows, 3 * wc), BF16)),
        ("gate", pltpu.VMEM((rows, wc), BF16)),
        ("gate_now", pltpu.VMEM((CHUNK, wc), F32)),
        ("attended", pltpu.VMEM((rows, wc), BF16)),
        ("gated", pltpu.VMEM((rows, wc), BF16)),
        ("n2", pltpu.VMEM((rows, width), BF16)),
        ("mixed", pltpu.VMEM((rows, fp), BF16)),
        ("d_left", pltpu.VMEM((rows, fp), BF16)),
        ("d_right", pltpu.VMEM((2, rows // 2, fp), BF16)),
        ("do", pltpu.VMEM((rows, width), BF16)),
        ("turned", pltpu.VMEM((256, rows // 2), BF16)),
        ("part", pltpu.VMEM((2, CHUNK, width), BF16)),
        ("part_g", pltpu.VMEM((2, CHUNK, width), BF16)),
        ("pair", pltpu.VMEM((RING, CHUNK // 2, width), BF16)),
        ("pair_g", pltpu.VMEM((RING, CHUNK // 2, width), BF16)),
        ("sent", pltpu.VMEM((own, width), BF16)),
        ("sent_g", pltpu.VMEM((own, width), BF16)),
        ("got", pltpu.VMEM((own, width), BF16)),
        ("got_g", pltpu.VMEM((own, width), BF16)),
        ("own", pltpu.VMEM((2, quarter, width), F32)),
        ("branch", pltpu.VMEM((CHUNK // 2, width), F32)),
        ("own_g", pltpu.VMEM((own, width), BF16)),
        ("hidden", pltpu.VMEM((own, width), F32)),
        ("d_hidden", pltpu.VMEM((own, width), F32)),
        ("grad_g", pltpu.VMEM((3, width, fp), BF16)),
        ("sem_tok", dma((chunks,))),
        ("sem_w", dma((9,))),
        ("sem_stage", dma((3 * pairs,))),
    ]
    for name in ("as", "ar", "bs", "br", "cs", "cr", "ps", "pr", "ds", "dr"):
        scratch.append(("sem_" + name, dma((4 * chunks,))))
    scratch.append(("sem_wos", dma((3,))))
    scratch.append(("sem_wor", dma((3,))))
    scratch.append(("sem_o", dma((2 * chunks,))))
    for name in ("xgs", "xgr", "zgs", "zgr", "xas", "xar", "zas", "zar"):
        scratch.append(("sem_" + name, dma((pairs,))))
    names = [n for n, *_ in ins] + [n for n, *_ in outs] + [n for n, _ in scratch]

    def call(*refs):
        named = dict(zip(names, refs))
        named["d_all"] = named["n2"]
        kernel(list(named), ndp, *named.values())

    flops = 6 * rows * width * (5 * wc + 3 * ff)
    result = pl.pallas_call(
        call,
        out_shape=[jax.ShapeDtypeStruct(s, d) for _, s, d, _ in outs],
        in_specs=[s for *_, s in ins],
        out_specs=[s for *_, s in outs],
        scratch_shapes=[s for _, s in scratch],
        compiler_params=pltpu.CompilerParams(
            collective_id=0, has_side_effects=True, vmem_limit_bytes=67043328
        ),
        cost_estimate=pl.CostEstimate(flops=flops, bytes_accessed=1 << 25, transcendentals=1 << 22),
        name="fused_layer",
    )(*[a for _, a, _ in ins])
    return result[0], result[1], result[4], result[5]


def collect(br, wc, ff, refs):
    out_h, gt_h, zg_h, za_h = refs[:4]
    out_o, gt_o, *grads_o = refs[4:14]
    held, zg, za, sem_in, sem_out, sem_z, *grads = refs[14:]
    pairs = zg.shape[0]
    pieces = held.shape[1]
    rows = held.shape[2]
    loads = [
        pltpu.make_async_copy(zg_h, zg, sem_z.at[0]),
        pltpu.make_async_copy(za_h, za, sem_z.at[1]),
    ]
    moves = []
    for i in range(pieces):
        for k, (src, dst) in enumerate(((out_h, out_o), (gt_h, gt_o))):
            span = pl.ds(i * rows, rows)
            get = pltpu.make_async_copy(src.at[span], held.at[k, i], sem_in.at[k * pieces + i])
            put = pltpu.make_async_copy(held.at[k, i], dst.at[span], sem_out.at[k * pieces + i])
            moves.append((get, put))
    for copy in loads:
        copy.start()
    for get, _ in moves:
        get.start()
    for copy in loads:
        copy.wait()

    def total(ref, t, cols):
        value = ref[0, t, :, cols].astype(F32)
        for j in range(1, pairs):
            value = value + ref[j, t, :, cols].astype(F32)
        return value

    stores = [pltpu.make_async_copy(v, h, sem_z.at[2 + i]) for i, (v, h) in enumerate(zip(grads, grads_o))]
    wide = za.shape[3]
    todo = list(moves)

    def pump():
        if todo:
            get, put = todo.pop(0)
            get.wait()
            put.start()

    for kind in range(5):
        for u in range(wc // 128):
            at_col = kind * (wc // 128) + u
            col = (at_col % (wide // 128)) * 128
            value = total(za, at_col // (wide // 128), pl.ds(col, 128))
            if kind < 4:
                grads[kind][:, pl.ds(u * 128, 128)] = value
            else:
                grads[kind][pl.ds(u * 128, 128), :] = value.T
        stores[kind].start()
        pump()
    for t in range(3):
        for start in range(0, ff, 128):
            size = min(128, ff - start)
            value = total(zg, t, pl.ds(start, 128)).T
            grads[5 + t][pl.ds(start, size), :] = value[:size]
        stores[5 + t].start()
        pump()
    while todo:
        pump()
    for _, put in moves:
        put.wait()
    for copy in stores:
        copy.wait()


def collected(arrays, br, wc, ff):
    rows, width = arrays[0].shape
    pieces = 8
    hbm = pl.BlockSpec(memory_space=pl.ANY)
    dma = pltpu.SemaphoreType.DMA
    shapes = [(br, wc)] * 4 + [(wc, br)] + [(ff, br)] * 3
    outs = [((rows, width), BF16)] * 2 + [(s, F32) for s in shapes]
    return pl.pallas_call(
        lambda *refs: collect(br, wc, ff, refs),
        out_shape=[jax.ShapeDtypeStruct(s, d) for s, d in outs],
        in_specs=[hbm] * 4,
        out_specs=[hbm] * 10,
        scratch_shapes=[
            pltpu.VMEM((2, pieces, rows // pieces, width), BF16),
            pltpu.VMEM(arrays[2].shape, BF16),
            pltpu.VMEM(arrays[3].shape, BF16),
            dma((2 * pieces,)),
            dma((2 * pieces,)),
            dma((10,)),
        ]
        + [pltpu.VMEM(s, F32) for s in shapes],
        compiler_params=pltpu.CompilerParams(vmem_limit_bytes=67043328),
        name="collect",
    )(*arrays)


def body(ndp, *args):
    arrays = fused(ndp, args)
    ff, wc, width = args[7].shape[1], args[2].shape[1], args[0].shape[1]
    out, grad_tokens, query, key, value, gate, proj, left, right, down = collected(
        arrays, width // ndp, wc, ff
    )
    return out, grad_tokens, query, key, value, gate, proj, left.T, right.T, down


def solution(mesh):
    rows, cols, down = P("dp", None), P(None, "mp"), P("mp", None)
    grad = P("dp", "mp")
    return jax.shard_map(
        functools.partial(body, mesh.shape["dp"]),
        mesh=mesh,
        in_specs=(rows, rows, cols, cols, cols, cols, down, cols, cols, down, rows),
        out_specs=(rows, rows, grad, grad, grad, grad, P("mp", "dp"), grad, grad, P("mp", "dp")),
        check_vma=False,
    )
```

```python
import functools

import jax
import jax.numpy as jnp
from jax import lax
from jax.experimental import pallas as pl
from jax.experimental.pallas import tpu as pltpu
from jax.sharding import PartitionSpec as P

HD = 64
BLOCK = 64
CHUNK = 256
TILE = 128
RING = 4
EPS = 1e-06
EARLY = 4
FORWARD = 5
PASS = 6
F32 = jnp.float32
BF16 = jnp.bfloat16
MESH = pl.DeviceIdType.MESH


def dot_nn(a, b):
    return lax.dot_general(a, b, (((1,), (0,)), ((), ())), preferred_element_type=F32)


def dot_nt(a, b):
    return lax.dot_general(a, b, (((1,), (1,)), ((), ())), preferred_element_type=F32)


def dot_tn(a, b):
    return lax.dot_general(a, b, (((0,), (0,)), ((), ())), preferred_element_type=F32)


def rms_factor(v):
    return lax.rsqrt(jnp.mean(v * v, axis=-1, keepdims=True) + EPS)


def norm_back(grad, normed, factor):
    return factor * (grad - normed * jnp.mean(grad * normed, axis=-1, keepdims=True))


def mult(v, n):
    return pl.multiple_of(v, n)


class Refs:
    pass


def kernel(names, ndp, *refs):
    r = Refs()
    for name, ref in zip(names, refs):
        setattr(r, name, ref)
    tokens, width = r.n1.shape
    chunks = tokens // CHUNK
    half, quarter = CHUNK // 2, CHUNK // 4
    wc = r.wo_h.shape[0]
    fp, ff = r.wl.shape[0], r.wl_h.shape[0]
    block_rows = width // ndp
    pairs = ndp // 2
    groups = width // 256
    per_group = pairs // groups
    half_chunks = chunks // 2
    wide = 5 * wc // 2

    dp = lax.axis_index("dp")
    mp = lax.axis_index("mp")
    core = mp % 2
    side = mp // 2
    partner = (dp, mp + 1 - 2 * core)
    across = (dp, mp + 2 - 4 * side)
    parity = dp % 2
    line = dp // 2
    beside = (dp + 1 - 2 * parity, mp)

    def remote(src, dst, send, recv, device):
        return pltpu.make_async_remote_copy(
            src_ref=src,
            dst_ref=dst,
            send_sem=send,
            recv_sem=recv,
            device_id=device,
            device_id_type=MESH,
        )

    barrier = pltpu.get_barrier_semaphore()
    for device in (partner, across):
        pl.semaphore_signal(barrier, inc=1, device_id=device, device_id_type=MESH)
    near = min(8, ndp)
    near_at = dp % near
    near_base = dp - near_at

    def greet(j, carry):
        @pl.when((j != dp) & ((j % 2 == parity) | (j // near == dp // near)))
        def _():
            pl.semaphore_signal(barrier, inc=1, device_id=(j, mp), device_id_type=MESH)

        return carry

    lax.fori_loop(0, ndp, greet, 0)

    pair_mp = mp + 1 - 2 * core
    across_mp = mp + 2 - 4 * side

    def group_of(who):
        return pl.ds(mult(who * wc, wc), wc)

    share = wc // near

    def share_of(who, place):
        return pl.ds(mult(who * wc + place * share, share), share)

    def wo_across():
        return remote(
            r.wo_h.at[pl.ds(mult(near_at * share, share), share)],
            r.wof.at[share_of(mp, near_at)],
            r.sem_wos.at[0],
            r.sem_wor.at[0],
            across,
        )

    def wo_spread(j):
        here = r.wof.at[share_of(across_mp, near_at)]
        return remote(
            here, here, r.sem_wos.at[3 + j], r.sem_wor.at[3 + near_at], (near_base + j, mp)
        )

    def wo_arrival(j):
        here = r.wof.at[share_of(across_mp, j)]
        return remote(here, here, r.sem_wos.at[3 + j], r.sem_wor.at[3 + j], (near_base + j, mp))

    def to_near(act):
        def one(j, carry):
            @pl.when(j != near_at)
            def _():
                act(j)

            return carry

        lax.fori_loop(0, near, one, 0)

    def wo_partner():
        there = r.wof.at[group_of(mp)]
        return remote(r.wo_h, there, r.sem_wos.at[1], r.sem_wor.at[1], partner)

    def wo_forward():
        here = r.wof.at[group_of(across_mp)]
        return remote(here, here, r.sem_wos.at[2], r.sem_wor.at[2], partner)

    def load_tokens(c):
        rows = pl.ds(mult(c * CHUNK, CHUNK), CHUNK)
        return pltpu.make_async_copy(r.tok_h.at[rows], r.n1.at[rows], r.sem_tok.at[c])

    load_tokens(0).start()
    w_loads = [
        pltpu.make_async_copy(h, r.w.at[:, pl.ds(i * wc, wc)], r.sem_w.at[i])
        for i, h in enumerate((r.wq_h, r.wk_h, r.wv_h, r.wg_h))
    ]
    for copy in w_loads:
        copy.start()
    wo_load = pltpu.make_async_copy(
        r.wo_h, r.wof.at[pl.ds(mult(mp * wc, wc), wc)], r.sem_w.at[4]
    )
    wo_load.start()
    for c in range(1, chunks):
        load_tokens(c).start()
    glu_loads = [
        pltpu.make_async_copy(h, v.at[pl.ds(0, ff)], r.sem_w.at[i])
        for i, h, v in ((5, r.wd_h, r.wd), (6, r.wl_h, r.wl), (7, r.wr_h, r.wr))
    ]
    for copy in glu_loads:
        copy.start()
    cot_load = pltpu.make_async_copy(r.cot_h, r.cot, r.sem_w.at[8])
    cot_load.start()

    pl.semaphore_wait(barrier, 2 + pairs - 1 + near // 2)
    for copy in (wo_across(), wo_partner()):
        copy.start()

    def base(c):
        return mult(c * CHUNK, CHUNK)

    def half_rows(c):
        return pl.ds(mult(c * CHUNK + core * half, half), half)

    def own_rows(c):
        return pl.ds(mult(c * CHUNK + core * half + side * quarter, quarter), quarter)

    def other_rows(c):
        return pl.ds(mult(c * CHUNK + core * half + (1 - side) * quarter, quarter), quarter)

    def partner_own_rows(c):
        return pl.ds(mult(c * CHUNK + (1 - core) * half + side * quarter, quarter), quarter)

    def partner_other_rows(c):
        return pl.ds(mult(c * CHUNK + (1 - core) * half + (1 - side) * quarter, quarter), quarter)

    def kept(c):
        return pl.ds(mult(c * quarter, quarter), quarter)

    def part_of(s):
        return r.part_g if s == 1 else r.part

    def pair_of(s):
        return r.pair_g if s == 1 else r.pair

    def sent_of(s):
        return r.sent_g if s == 1 else r.sent

    def got_of(s):
        return r.got_g if s == 1 else r.got

    def full_of(s):
        return (None, r.out_h, r.do, r.gt_h)[s]

    def at(s, c):
        return s * chunks + c

    def pair_copy(s, c):
        slot = c % RING
        return remote(
            part_of(s).at[c % 2, pl.ds(mult((1 - core) * half, half), half)],
            pair_of(s).at[slot],
            r.sem_as.at[at(s, c)],
            r.sem_ar.at[at(s, c)],
            partner,
        )

    def across_copy(s, c):
        return remote(
            sent_of(s).at[kept(c)],
            got_of(s).at[kept(c)],
            r.sem_bs.at[at(s, c)],
            r.sem_br.at[at(s, c)],
            across,
        )

    def result_src(s, c):
        if s == 2:
            return full_of(s).at[own_rows(c)]
        return sent_of(s).at[kept(c)]

    def result_across(s, c):
        return remote(
            result_src(s, c),
            full_of(s).at[own_rows(c)],
            r.sem_cs.at[at(s, c)],
            r.sem_cr.at[at(s, c)],
            across,
        )

    def result_partner(s, c):
        return remote(
            result_src(s, c),
            full_of(s).at[own_rows(c)],
            r.sem_ps.at[at(s, c)],
            r.sem_pr.at[at(s, c)],
            partner,
        )

    def result_own(s, c):
        return pltpu.make_async_copy(
            sent_of(s).at[kept(c)], full_of(s).at[own_rows(c)], r.sem_o.at[at(s // 2, c)]
        )

    def forward(s, c):
        return remote(
            full_of(s).at[other_rows(c)],
            full_of(s).at[other_rows(c)],
            r.sem_ds.at[at(s, c)],
            r.sem_dr.at[at(s, c)],
            partner,
        )

    def step_b(s, c, send=True):
        copy = pair_copy(s, c)
        copy.wait_recv()
        copy.wait_send()
        part, pair = part_of(s), pair_of(s)
        slot, ring = c % 2, c % RING

        def piece(i, carry):
            rows = mult(i * 32, 32)
            away = pl.ds(mult(core * half + (1 - side) * quarter + rows, 32), 32)
            away_pair = pl.ds(mult((1 - side) * quarter + rows, 32), 32)
            total = part[slot, away, :].astype(F32) + pair[ring, away_pair, :].astype(F32)
            sent_of(s)[pl.ds(mult(c * quarter + rows, 32), 32), :] = total.astype(BF16)
            mine = pl.ds(mult(core * half + side * quarter + rows, 32), 32)
            mine_pair = pl.ds(mult(side * quarter + rows, 32), 32)
            total = part[slot, mine, :].astype(F32) + pair[ring, mine_pair, :].astype(F32)
            if s == 1:
                r.own_g[pl.ds(mult(c * quarter + rows, 32), 32), :] = total.astype(BF16)
            else:
                r.own[slot, pl.ds(rows, 32), :] = total
            return carry

        lax.fori_loop(0, quarter // 32, piece, 0, unroll=True)
        if send:
            across_copy(s, c).start()

    def step_c(s, c):
        copy = across_copy(s, c)
        copy.wait_recv()
        copy.wait_send()
        slot = c % 2

        def piece(i, carry):
            rows = mult(i * 32, 32)
            mine = pl.ds(mult(c * quarter + rows, 32), 32)
            full = pl.ds(mult(c * CHUNK + core * half + side * quarter + rows, 32), 32)
            arrived = got_of(s)[mine, :].astype(F32)
            if s == 1:
                total = r.own_g[mine, :].astype(F32) + arrived
            else:
                total = r.own[slot, pl.ds(rows, 32), :] + arrived
            if s == 1:
                r.sent_g[mine, :] = (r.hidden[mine, :] + total).astype(BF16)
            elif s == 2:
                hidden = r.hidden[mine, :]
                factor = rms_factor(hidden)
                d_hidden = r.cot[full, :].astype(F32) + norm_back(total, hidden * factor, factor)
                r.d_hidden[mine, :] = d_hidden
                r.do[full, :] = d_hidden.astype(BF16)
            else:
                held = pl.ds(mult(c * half + side * quarter + rows, 32), 32)
                source = r.tok_half[held, :].astype(F32)
                factor = rms_factor(source)
                d_source = r.d_hidden[mine, :] + norm_back(total, source * factor, factor)
                r.sent[mine, :] = d_source.astype(BF16)
            return carry

        lax.fori_loop(0, quarter // 32, piece, 0, unroll=True)
        result_across(s, c).start()
        result_partner(s, c).start()
        if s in (1, 3):
            result_own(s, c).start()

    def step_d(s, c):
        result_across(s, c).wait_recv()
        forward(s, c).start()

    def step_e(s, c):
        remote(
            result_src(s, c),
            full_of(s).at[partner_own_rows(c)],
            r.sem_ps.at[at(s, c)],
            r.sem_pr.at[at(s, c)],
            partner,
        ).wait_recv()
        remote(
            full_of(s).at[other_rows(c)],
            full_of(s).at[partner_other_rows(c)],
            r.sem_ds.at[at(s, c)],
            r.sem_dr.at[at(s, c)],
            partner,
        ).wait_recv()
        result_across(s, c).wait_send()
        result_partner(s, c).wait_send()
        forward(s, c).wait_send()
        if s in (1, 3):
            result_own(s, c).wait()

    def tick(s, c):
        @pl.when(c >= 1)
        def _():
            step_b(s, c - 1)

        @pl.when(c >= 2)
        def _():
            step_c(s, c - 2)

        @pl.when(c >= FORWARD)
        def _():
            step_d(s, c - FORWARD)

    def late_tick(s, n):
        if n == 0:
            step_b(s, chunks - 1)
        if n <= 1:
            step_c(s, chunks - 2 + n)
        step_d(s, chunks - FORWARD + n)

    def gated_across(c):
        here = r.do.at[pl.ds(base(c), CHUNK), group_of(mp)]
        return remote(here, here, r.sem_bs.at[c], r.sem_br.at[c], across)

    def gated_partner(c):
        here = r.do.at[pl.ds(base(c), CHUNK), group_of(mp)]
        return remote(here, here, r.sem_as.at[c], r.sem_ar.at[c], partner)

    def gated_forward(c):
        here = r.do.at[pl.ds(base(c), CHUNK), group_of(across_mp)]
        return remote(here, here, r.sem_ds.at[c], r.sem_dr.at[c], partner)

    def n2_partner(c):
        here = r.n2.at[half_rows(c)]
        return remote(here, here, r.sem_ps.at[c], r.sem_pr.at[c], partner)

    def gated_pass(c):
        gated_across(c).wait_recv()
        gated_forward(c).start()

    def gated_project(c):
        gated_partner(c).wait_recv()
        gated_forward(c).wait_recv()
        rows = half_rows(c)
        for t in range(width // 256):
            cols = pl.ds(t * 256, 256)
            total = dot_nn(r.do[rows, :], r.wof[:, cols])
            r.branch[:, cols] = total

        def piece(i, carry):
            q, sub = i // 2, mult((i % 2) * 32, 32)
            held = pl.ds(mult(c * half + i * 32, 32), 32)
            full = pl.ds(mult(c * CHUNK + core * half + i * 32, 32), 32)
            hidden = r.tok_half[held, :].astype(F32) + r.branch[pl.ds(mult(i * 32, 32), 32), :]
            r.n2[full, :] = (hidden * rms_factor(hidden)).astype(BF16)

            @pl.when(q == side)
            def _():
                r.hidden[pl.ds(mult(c * quarter + sub, 32), 32), :] = hidden

            return carry

        lax.fori_loop(0, half // 32, piece, 0, unroll=True)
        n2_partner(c).start()

    def gated_end(c):
        n2_partner(c).wait_recv()
        for copy in (gated_across(c), gated_partner(c), gated_forward(c), n2_partner(c)):
            copy.wait_send()

    lane = lax.broadcasted_iota(jnp.int32, (TILE, TILE), 1)
    row = lax.broadcasted_iota(jnp.int32, (TILE, TILE), 0)
    first = lane < HD

    def stacked(v):
        zero = jnp.zeros_like(v)
        return jnp.concatenate([jnp.where(first, v, zero), jnp.where(first, zero, v)], axis=0)

    def unstacked(v):
        return jnp.where(first, v[:TILE], v[TILE:])

    def head_mean(v):
        zero = jnp.zeros_like(v)
        low = jnp.sum(jnp.where(first, v, zero), axis=-1, keepdims=True)
        high = jnp.sum(jnp.where(first, zero, v), axis=-1, keepdims=True)
        return jnp.where(first, low, high) * (1.0 / HD)

    def probs_of(tile, rows, lanes):
        ids = r.seg[pl.ds(tile, 1), :].astype(F32)
        across_ids = jnp.broadcast_to(ids, (TILE, TILE))
        allowed = (
            (across_ids == across_ids.T) & (lane <= row) & (lane // BLOCK == row // BLOCK)
        )
        stack = stacked(r.qkv[rows, pl.ds(lanes, TILE)])
        keys = r.qkv[rows, pl.ds(wc + lanes, TILE)]
        scores = dot_nt(stack, keys) * HD ** (-0.5)
        allowed2 = jnp.concatenate([allowed, allowed], axis=0)
        masked = jnp.where(allowed2, scores, F32(-1e30))
        top = jnp.max(masked, axis=-1, keepdims=True)
        expd = jnp.exp(masked - top)
        probs = expd * (1.0 / jnp.sum(expd, axis=-1, keepdims=True))
        return probs, stack, keys

    head_pairs = wc // TILE
    tiles = CHUNK // TILE

    def tile_of(c, i):
        tile = c * tiles + i // head_pairs
        lanes = mult((i % head_pairs) * TILE, TILE)
        rows = pl.ds(mult(tile * TILE, TILE), TILE)
        return tile, rows, lanes

    def beside_copy(grads, arrivals, sems, g):
        block = 2 * g + 1 - parity
        send, recv = sems
        return remote(
            grads(pl.ds(mult(block * block_rows, block_rows), block_rows)),
            arrivals(pl.ds(mult(g * block_rows, block_rows), block_rows)),
            send.at[g],
            recv.at[g],
            beside,
        )

    def line_copy(grads, arrivals, sems, g):
        block = 2 * g + parity
        send, recv = sems
        return remote(
            grads(pl.ds(mult(block * block_rows, block_rows), block_rows)),
            arrivals(line),
            send.at[g],
            recv.at[line],
            (block, mp),
        )

    def glu_rows(rows):
        return r.grad_g.at[:, rows]

    def glu_beside(rows):
        return r.xg_h.at[:, rows]

    def glu_line(slot):
        return r.zg_h.at[slot]

    def att_rows(rows):
        return r.d_right.at[:, rows, pl.ds(0, wide)]

    def att_beside(rows):
        return r.xa_h.at[:, rows]

    def att_line(slot):
        return r.za_h.at[slot]

    glu_x = (glu_rows, glu_beside, (r.sem_xgs, r.sem_xgr))
    glu_z = (glu_rows, glu_line, (r.sem_zgs, r.sem_zgr))
    att_x = (att_rows, att_beside, (r.sem_xas, r.sem_xar))
    att_z = (att_rows, att_line, (r.sem_zas, r.sem_zar))

    def each(count, act):
        def one(j, carry):
            act(j)
            return carry

        if count == 1:
            act(0)
        else:
            lax.fori_loop(0, count, one, 0)

    def turn(k):
        return (line // per_group + 1 + k) % groups

    def turned_half(src, i, h):
        for k in range(tokens // 512):
            rows = pl.ds(h * (tokens // 2) + k * 256, 256)
            r.turned[:, pl.ds(k * 256, 256)] = src[rows, pl.ds(mult(i * 256, 256), 256)].T

    def gathered(h, old, term):
        return (term if h == 0 else old.astype(F32) + term).astype(BF16)

    def glu_half(i, h):
        rows = pl.ds(mult(i * 256, 256), 256)
        half_rows_all = pl.ds(h * (tokens // 2), tokens // 2)
        turned_half(r.n2, i, h)
        for t in range(fp // 256):
            cols = pl.ds(t * 256, 256)
            term = dot_nn(r.turned[...], r.d_left[half_rows_all, cols])
            r.grad_g[0, rows, cols] = gathered(h, r.grad_g[0, rows, cols], term)
            term = dot_nn(r.turned[...], r.d_right[h, :, cols])
            r.grad_g[1, rows, cols] = gathered(h, r.grad_g[1, rows, cols], term)
        turned_half(r.cot, i, h)
        for t in range(fp // 256):
            cols = pl.ds(t * 256, 256)
            term = dot_nn(r.turned[...], r.mixed[half_rows_all, cols])
            r.grad_g[2, rows, cols] = gathered(h, r.grad_g[2, rows, cols], term)

    def att_half(i, h):
        rows = pl.ds(mult(i * 256, 256), 256)
        half_rows_all = pl.ds(h * (tokens // 2), tokens // 2)

        def store(kind, term):
            for u in range(wc // 128):
                at_col = kind * (wc // 128) + u
                cols = pl.ds((at_col % (wide // 128)) * 128, 128)
                place = at_col // (wide // 128)
                piece = term[:, u * 128 : u * 128 + 128]
                r.d_right[place, rows, cols] = gathered(h, r.d_right[place, rows, cols], piece)

        turned_half(r.n1, i, h)
        for kind in range(4):
            cols = pl.ds(kind * wc, wc)
            store(kind, dot_nn(r.turned[...], r.d_all[half_rows_all, cols]))
        turned_half(r.do, i, h)
        store(4, dot_nn(r.turned[...], r.gated[half_rows_all, :]))

    for copy in w_loads:
        copy.wait()

    def phase_one(c, carry):
        rows_all = pl.ds(base(c), CHUNK)
        load_tokens(c).wait()
        r.tok_half[pl.ds(mult(c * half, half), half), :] = r.n1[half_rows(c), :]

        def norm_piece(i, carry2):
            rows = pl.ds(mult(c * CHUNK + i * 32, 32), 32)
            x = r.n1[rows, :].astype(F32)
            r.n1[rows, :] = (x * rms_factor(x)).astype(BF16)
            return carry2

        lax.fori_loop(0, CHUNK // 32, norm_piece, 0, unroll=True)

        def project(t, carry2):
            cols = pl.ds(mult(t * wc, wc), wc)
            r.qkv[rows_all, cols] = dot_nn(r.n1[rows_all, :], r.w[:, cols]).astype(BF16)
            return carry2

        lax.fori_loop(0, 3, project, 0, unroll=True)
        r.gate_now[...] = dot_nn(r.n1[rows_all, :], r.w[:, pl.ds(3 * wc, wc)])
        r.gate[rows_all, :] = r.gate_now[...].astype(BF16)

        def attend(i, carry2):
            tile, rows, lanes = tile_of(c, i)
            probs, _, _ = probs_of(tile, rows, lanes)
            values = r.qkv[rows, pl.ds(2 * wc + lanes, TILE)]
            attended = unstacked(dot_nn(probs.astype(BF16), values))
            r.attended[rows, pl.ds(lanes, TILE)] = attended.astype(BF16)
            factor = lax.rsqrt(head_mean(attended * attended) + EPS)
            near = pl.ds(mult((i // head_pairs) * TILE, TILE), TILE)
            sigma = jax.nn.sigmoid(r.gate_now[near, pl.ds(lanes, TILE)])
            gated = (attended * factor * sigma).astype(BF16)
            r.gated[rows, pl.ds(lanes, TILE)] = gated
            r.do[rows, pl.ds(mult(mp * wc + lanes, TILE), TILE)] = gated
            return carry2

        lax.fori_loop(0, tiles * head_pairs, attend, 0, unroll=True)

        gated_across(c).start()
        gated_partner(c).start()

        @pl.when(c == 0)
        def _():
            wo_across().wait_recv()
            to_near(lambda j: wo_spread(j).start())

        @pl.when(c == PASS)
        def _():
            to_near(lambda j: wo_arrival(j).wait_recv())
            wo_forward().start()

        @pl.when(c >= PASS)
        def _():
            gated_pass(c - PASS)

        @pl.when(c == PASS + 1)
        def _():
            wo_load.wait()
            wo_partner().wait_recv()
            wo_forward().wait_recv()
            for copy in (wo_across(), wo_partner(), wo_forward()):
                copy.wait_send()
            to_near(lambda j: wo_spread(j).wait_send())

        @pl.when(c >= PASS + 1)
        def _():
            gated_project(c - PASS - 1)

        return carry

    lax.fori_loop(0, chunks, phase_one, 0)

    for copy in glu_loads:
        copy.wait()
    for weights in (r.wd, r.wl, r.wr):
        weights[pl.ds(ff, fp - ff), :] = jnp.zeros((fp - ff, width), BF16)
    cot_load.wait()

    def phase_two(c, carry):
        @pl.when(c < PASS)
        def _():
            gated_pass(chunks - PASS + c)

        @pl.when(c <= PASS)
        def _():
            gated_project(chunks - PASS - 1 + c)

        gated_end(c)
        rows_all = pl.ds(base(c), CHUNK)
        rows_half = pl.ds(mult((c % half_chunks) * CHUNK, CHUNK), CHUNK)

        def hidden_units(t, carry2):
            cols = pl.ds(mult(t * 256, 256), 256)
            left = dot_nt(r.n2[rows_all, :], r.wl[cols, :])
            right = dot_nt(r.n2[rows_all, :], r.wr[cols, :])
            r.mixed[rows_all, cols] = (left * right).astype(BF16)
            d_mixed = dot_nt(r.cot[rows_all, :], r.wd[cols, :])
            r.d_left[rows_all, cols] = (d_mixed * right).astype(BF16)
            r.d_right[c // half_chunks, rows_half, cols] = (d_mixed * left).astype(BF16)
            return carry2

        lax.fori_loop(0, fp // 256, hidden_units, 0, unroll=True)

        def parts(t, carry2):
            cols = pl.ds(mult(t * 256, 256), 256)
            back = dot_nn(r.d_left[rows_all, :], r.wl[:, cols])
            back = back + dot_nn(r.d_right[c // half_chunks, rows_half, :], r.wr[:, cols])
            r.part[c % 2, :, cols] = back.astype(BF16)
            r.part_g[c % 2, :, cols] = dot_nn(r.mixed[rows_all, :], r.wd[:, cols]).astype(BF16)
            return carry2

        lax.fori_loop(0, width // 256, parts, 0, unroll=True)
        pair_copy(2, c).start()
        pair_copy(1, c).start()

        @pl.when(c >= half_chunks)
        def _():
            glu_half(turn(c - half_chunks), 0)

        tick(2, c)

        @pl.when(c >= 1)
        def _():
            step_b(1, c - 1, send=False)

        return carry

    lax.fori_loop(0, chunks, phase_two, 0)
    late_tick(2, 0)
    step_b(1, chunks - 1, send=False)

    def send_glu(c, carry):
        across_copy(1, c).start()
        return carry

    lax.fori_loop(0, EARLY, send_glu, 0)

    def glu_group(k, carry):
        i = turn(k)
        glu_half(i, 1)
        each(per_group, lambda j: beside_copy(*glu_x, i * per_group + j).start())
        for n in range(FORWARD - 1):

            @pl.when(k == n)
            def _():
                late_tick(2, n + 1)

        return carry

    lax.fori_loop(0, groups, glu_group, 0)

    def line_loads(kinds, lanes, arrivals_h, stage, g):
        here = pl.ds(mult(g * block_rows, block_rows), block_rows)
        return [
            pltpu.make_async_copy(
                arrivals_h.at[t, here],
                stage.at[pl.ds(t * block_rows, block_rows), pl.ds(0, lanes)],
                r.sem_stage.at[t],
            )
            for t in range(kinds)
        ]

    def line_arrive(kinds, lanes, x, z, arrivals_h, stage, grads, g):
        copy = beside_copy(*x, g)
        copy.wait_recv()
        copy.wait_send()
        for load in line_loads(kinds, lanes, arrivals_h, stage, g):
            load.start()

    def line_sum(kinds, lanes, x, z, arrivals_h, stage, grads, g):
        for load in line_loads(kinds, lanes, arrivals_h, stage, g):
            load.wait()
        step = min(16, block_rows)
        cols = pl.ds(0, lanes)

        def piece(i, carry):
            sub = mult(i * step, step)
            there = pl.ds(mult((2 * g + parity) * block_rows + sub, step), step)
            for t in range(kinds):
                mine = grads[t, there, cols].astype(F32)
                theirs = stage[pl.ds(mult(t * block_rows + sub, step), step), cols].astype(F32)
                grads[t, there, cols] = (mine + theirs).astype(BF16)
            return carry

        lax.fori_loop(0, block_rows // step, piece, 0)

        @pl.when(g != line)
        def _():
            line_copy(*z, g).start()

    glu_line = (3, fp, glu_x, glu_z, r.xg_h, r.mixed, r.grad_g)
    att_line_of = (2, wide, att_x, att_z, r.xa_h, r.d_left, r.d_right)

    def line_both(what, k):
        if per_group == 1:
            line_sum(*what, turn(k))
            return

        def one(j):
            g = turn(k) * per_group + j
            line_arrive(*what, g)
            line_sum(*what, g)

        each(per_group, one)

    def line_start(what, k):
        if per_group == 1:
            line_arrive(*what, turn(k))

    def phase_three(c, carry):
        step_e(2, c)
        rows_all = pl.ds(base(c), CHUNK)
        r.gate_now[...] = dot_nt(r.do[rows_all, :], r.wof[group_of(mp), :])

        def attend_back(i, carry2):
            tile, rows, lanes = tile_of(c, i)
            near = pl.ds(mult((i // head_pairs) * TILE, TILE), TILE)
            here = pl.ds(lanes, TILE)
            d_gated = r.gate_now[near, here]
            sigma = jax.nn.sigmoid(r.gate[rows, here].astype(F32))
            attended = r.attended[rows, here].astype(F32)
            factor = lax.rsqrt(head_mean(attended * attended) + EPS)
            head_normed = attended * factor
            d_head = d_gated * sigma
            d_gate = d_head * head_normed * (1.0 - sigma)
            r.d_all[rows, pl.ds(3 * wc + lanes, TILE)] = d_gate.astype(BF16)
            d_att = factor * (d_head - head_normed * head_mean(d_head * head_normed))
            d_stack = stacked(d_att.astype(BF16))
            probs, stack, keys = probs_of(tile, rows, lanes)
            values = r.qkv[rows, pl.ds(2 * wc + lanes, TILE)]
            d_probs = dot_nt(d_stack, values)
            d_values = dot_tn(probs.astype(BF16), d_stack)
            r.d_all[rows, pl.ds(2 * wc + lanes, TILE)] = d_values.astype(BF16)
            delta = jnp.sum(probs * d_probs, axis=-1, keepdims=True)
            d_scores = (probs * (d_probs - delta)).astype(BF16)
            d_queries = unstacked(dot_nn(d_scores, keys)) * HD ** (-0.5)
            r.d_all[rows, here] = d_queries.astype(BF16)
            d_keys = dot_tn(d_scores, stack) * HD ** (-0.5)
            r.d_all[rows, pl.ds(wc + lanes, TILE)] = d_keys.astype(BF16)
            return carry2

        lax.fori_loop(0, tiles * head_pairs, attend_back, 0, unroll=True)

        def back_piece(t, carry2):
            cols = pl.ds(mult(t * 256, 256), 256)
            r.part[c % 2, :, cols] = dot_nt(r.d_all[rows_all, :], r.w[cols, :]).astype(BF16)
            return carry2

        lax.fori_loop(0, width // 256, back_piece, 0, unroll=True)
        pair_copy(3, c).start()

        @pl.when(c >= half_chunks)
        def _():
            att_half(turn(c - half_chunks), 0)

        tick(3, c)

        for i in range(groups):

            @pl.when(c == 2 * i + 1)
            def _():
                line_start(glu_line, i)

            if i > 0:

                @pl.when(c == 2 * i)
                def _():
                    line_both(glu_line, i - 1)

        return carry

    lax.fori_loop(0, chunks, phase_three, 0)
    late_tick(3, 0)

    line_both(glu_line, groups - 1)
    lax.fori_loop(EARLY, chunks, send_glu, 0)

    def att_group(k, carry):
        i = turn(k)
        att_half(i, 1)
        each(per_group, lambda j: beside_copy(*att_x, i * per_group + j).start())
        for n in range(FORWARD - 1):

            @pl.when(k == n)
            def _():
                late_tick(3, n + 1)

        return carry

    lax.fori_loop(0, groups, att_group, 0)

    def glu_result(c, carry):
        step_c(1, c)
        return carry

    lax.fori_loop(0, EARLY, glu_result, 0)

    def att_lines(k, carry):
        line_start(att_line_of, k)
        first_left = EARLY + k * (chunks - EARLY) // groups
        last_left = EARLY + (k + 1) * (chunks - EARLY) // groups
        lax.fori_loop(first_left, last_left, glu_result, 0)
        line_both(att_line_of, k)
        return carry

    lax.fori_loop(0, groups, att_lines, 0)

    def glu_forward(c, carry):
        step_d(1, c)
        return carry

    lax.fori_loop(0, chunks, glu_forward, 0)

    def settle(z, sem):
        grads, arrivals, sems = z
        here = pl.ds(mult(dp * block_rows, block_rows), block_rows)
        mine = pltpu.make_async_copy(grads(here), arrivals(line), sem)
        mine.start()

        def arrived(j, carry):
            @pl.when(j != line)
            def _():
                remote(
                    grads(here), arrivals(j), sems[0].at[j], sems[1].at[j], (2 * j + parity, mp)
                ).wait_recv()
                line_copy(*z, j).wait_send()

            return carry

        lax.fori_loop(0, pairs, arrived, 0)
        mine.wait()

    settle(glu_z, r.sem_stage.at[0])
    settle(att_z, r.sem_stage.at[1])

    def ends(c, carry):
        step_e(1, c)
        step_e(3, c)
        return carry

    lax.fori_loop(0, chunks, ends, 0)


def fused(ndp, args):
    tokens, seg, wq, wk, wv, wg, wo, wl, wr, wd, cot = args
    rows, width = tokens.shape
    wc, ff = wq.shape[1], wl.shape[1]
    fp = (ff + 255) // 256 * 256
    chunks = rows // CHUNK
    quarter = CHUNK // 4
    own = rows // 4
    br = width // ndp
    pairs = ndp // 2
    wide = 5 * wc // 2
    hbm = pl.BlockSpec(memory_space=pl.ANY)
    vmem = pl.BlockSpec(memory_space=pltpu.VMEM)
    ins = [
        ("tok_h", tokens, hbm),
        ("seg", seg.reshape(rows // TILE, TILE), vmem),
        ("wq_h", wq, hbm),
        ("wk_h", wk, hbm),
        ("wv_h", wv, hbm),
        ("wg_h", wg, hbm),
        ("wo_h", wo, hbm),
        ("wl_h", wl.T, hbm),
        ("wr_h", wr.T, hbm),
        ("wd_h", wd, hbm),
        ("cot_h", cot, hbm),
    ]
    outs = [
        ("out_h", (rows, width), BF16, hbm),
        ("gt_h", (rows, width), BF16, hbm),
        ("xg_h", (3, pairs * br, fp), BF16, hbm),
        ("xa_h", (2, pairs * br, wide), BF16, hbm),
        ("zg_h", (pairs, 3, br, fp), BF16, hbm),
        ("za_h", (pairs, 2, br, wide), BF16, hbm),
    ]
    dma = pltpu.SemaphoreType.DMA
    scratch = [
        ("n1", pltpu.VMEM((rows, width), BF16)),
        ("tok_half", pltpu.VMEM((rows // 2, width), BF16)),
        ("cot", pltpu.VMEM((rows, width), BF16)),
        ("w", pltpu.VMEM((width, 4 * wc), BF16)),
        ("wof", pltpu.VMEM((width, width), BF16)),
        ("wl", pltpu.VMEM((fp, width), BF16)),
        ("wr", pltpu.VMEM((fp, width), BF16)),
        ("wd", pltpu.VMEM((fp, width), BF16)),
        ("qkv", pltpu.VMEM((rows, 3 * wc), BF16)),
        ("gate", pltpu.VMEM((rows, wc), BF16)),
        ("gate_now", pltpu.VMEM((CHUNK, wc), F32)),
        ("attended", pltpu.VMEM((rows, wc), BF16)),
        ("gated", pltpu.VMEM((rows, wc), BF16)),
        ("n2", pltpu.VMEM((rows, width), BF16)),
        ("mixed", pltpu.VMEM((rows, fp), BF16)),
        ("d_left", pltpu.VMEM((rows, fp), BF16)),
        ("d_right", pltpu.VMEM((2, rows // 2, fp), BF16)),
        ("do", pltpu.VMEM((rows, width), BF16)),
        ("turned", pltpu.VMEM((256, rows // 2), BF16)),
        ("part", pltpu.VMEM((2, CHUNK, width), BF16)),
        ("part_g", pltpu.VMEM((2, CHUNK, width), BF16)),
        ("pair", pltpu.VMEM((RING, CHUNK // 2, width), BF16)),
        ("pair_g", pltpu.VMEM((RING, CHUNK // 2, width), BF16)),
        ("sent", pltpu.VMEM((own, width), BF16)),
        ("sent_g", pltpu.VMEM((own, width), BF16)),
        ("got", pltpu.VMEM((own, width), BF16)),
        ("got_g", pltpu.VMEM((own, width), BF16)),
        ("own", pltpu.VMEM((2, quarter, width), F32)),
        ("branch", pltpu.VMEM((CHUNK // 2, width), F32)),
        ("own_g", pltpu.VMEM((own, width), BF16)),
        ("hidden", pltpu.VMEM((own, width), F32)),
        ("d_hidden", pltpu.VMEM((own, width), F32)),
        ("grad_g", pltpu.VMEM((3, width, fp), BF16)),
        ("sem_tok", dma((chunks,))),
        ("sem_w", dma((9,))),
        ("sem_stage", dma((3 * pairs,))),
    ]
    for name in ("as", "ar", "bs", "br", "cs", "cr", "ps", "pr", "ds", "dr"):
        scratch.append(("sem_" + name, dma((4 * chunks,))))
    scratch.append(("sem_wos", dma((11,))))
    scratch.append(("sem_wor", dma((11,))))
    scratch.append(("sem_o", dma((2 * chunks,))))
    for name in ("xgs", "xgr", "zgs", "zgr", "xas", "xar", "zas", "zar"):
        scratch.append(("sem_" + name, dma((pairs,))))
    names = [n for n, *_ in ins] + [n for n, *_ in outs] + [n for n, _ in scratch]

    def call(*refs):
        named = dict(zip(names, refs))
        named["d_all"] = named["n2"]
        kernel(list(named), ndp, *named.values())

    flops = 6 * rows * width * (5 * wc + 3 * ff)
    result = pl.pallas_call(
        call,
        out_shape=[jax.ShapeDtypeStruct(s, d) for _, s, d, _ in outs],
        in_specs=[s for *_, s in ins],
        out_specs=[s for *_, s in outs],
        scratch_shapes=[s for _, s in scratch],
        compiler_params=pltpu.CompilerParams(
            collective_id=0, has_side_effects=True, vmem_limit_bytes=67043328
        ),
        cost_estimate=pl.CostEstimate(flops=flops, bytes_accessed=1 << 25, transcendentals=1 << 22),
        name="fused_layer",
    )(*[a for _, a, _ in ins])
    return result[0], result[1], result[4], result[5]


def collect(br, wc, ff, refs):
    out_h, gt_h, zg_h, za_h = refs[:4]
    out_o, gt_o, *grads_o = refs[4:14]
    held, zg, za, sem_in, sem_out, sem_z, *grads = refs[14:]
    pairs = zg.shape[0]
    pieces = held.shape[1]
    rows = held.shape[2]
    loads = [
        pltpu.make_async_copy(zg_h, zg, sem_z.at[0]),
        pltpu.make_async_copy(za_h, za, sem_z.at[1]),
    ]
    moves = []
    for i in range(pieces):
        for k, (src, dst) in enumerate(((out_h, out_o), (gt_h, gt_o))):
            span = pl.ds(i * rows, rows)
            get = pltpu.make_async_copy(src.at[span], held.at[k, i], sem_in.at[k * pieces + i])
            put = pltpu.make_async_copy(held.at[k, i], dst.at[span], sem_out.at[k * pieces + i])
            moves.append((get, put))
    for copy in loads:
        copy.start()
    for get, _ in moves:
        get.start()
    for copy in loads:
        copy.wait()

    def total(ref, t, cols):
        value = ref[0, t, :, cols].astype(F32)
        for j in range(1, pairs):
            value = value + ref[j, t, :, cols].astype(F32)
        return value

    stores = [pltpu.make_async_copy(v, h, sem_z.at[2 + i]) for i, (v, h) in enumerate(zip(grads, grads_o))]
    wide = za.shape[3]
    todo = list(moves)

    def pump():
        if todo:
            get, put = todo.pop(0)
            get.wait()
            put.start()

    for kind in range(5):
        for u in range(wc // 128):
            at_col = kind * (wc // 128) + u
            col = (at_col % (wide // 128)) * 128
            value = total(za, at_col // (wide // 128), pl.ds(col, 128))
            if kind < 4:
                grads[kind][:, pl.ds(u * 128, 128)] = value
            else:
                grads[kind][pl.ds(u * 128, 128), :] = value.T
        stores[kind].start()
        pump()
    for t in range(3):
        for start in range(0, ff, 128):
            size = min(128, ff - start)
            value = total(zg, t, pl.ds(start, 128)).T
            grads[5 + t][pl.ds(start, size), :] = value[:size]
        stores[5 + t].start()
        pump()
    while todo:
        pump()
    for _, put in moves:
        put.wait()
    for copy in stores:
        copy.wait()


def collected(arrays, br, wc, ff):
    rows, width = arrays[0].shape
    pieces = 8
    hbm = pl.BlockSpec(memory_space=pl.ANY)
    dma = pltpu.SemaphoreType.DMA
    shapes = [(br, wc)] * 4 + [(wc, br)] + [(ff, br)] * 3
    outs = [((rows, width), BF16)] * 2 + [(s, F32) for s in shapes]
    return pl.pallas_call(
        lambda *refs: collect(br, wc, ff, refs),
        out_shape=[jax.ShapeDtypeStruct(s, d) for s, d in outs],
        in_specs=[hbm] * 4,
        out_specs=[hbm] * 10,
        scratch_shapes=[
            pltpu.VMEM((2, pieces, rows // pieces, width), BF16),
            pltpu.VMEM(arrays[2].shape, BF16),
            pltpu.VMEM(arrays[3].shape, BF16),
            dma((2 * pieces,)),
            dma((2 * pieces,)),
            dma((10,)),
        ]
        + [pltpu.VMEM(s, F32) for s in shapes],
        compiler_params=pltpu.CompilerParams(vmem_limit_bytes=67043328),
        name="collect",
    )(*arrays)


def body(ndp, *args):
    arrays = fused(ndp, args)
    ff, wc, width = args[7].shape[1], args[2].shape[1], args[0].shape[1]
    out, grad_tokens, query, key, value, gate, proj, left, right, down = collected(
        arrays, width // ndp, wc, ff
    )
    return out, grad_tokens, query, key, value, gate, proj, left.T, right.T, down


def solution(mesh):
    rows, cols, down = P("dp", None), P(None, "mp"), P("mp", None)
    grad = P("dp", "mp")
    return jax.shard_map(
        functools.partial(body, mesh.shape["dp"]),
        mesh=mesh,
        in_specs=(rows, rows, cols, cols, cols, cols, down, cols, cols, down, rows),
        out_specs=(rows, rows, grad, grad, grad, grad, P("mp", "dp"), grad, grad, P("mp", "dp")),
        check_vma=False,
    )
```

```python
import functools

import jax
import jax.numpy as jnp
from jax import lax
from jax.experimental import pallas as pl
from jax.experimental.pallas import tpu as pltpu
from jax.sharding import PartitionSpec as P

HD = 64
BLOCK = 64
CHUNK = 256
TILE = 128
RING = 4
EPS = 1e-06
EARLY = 4
FORWARD = 5
PASS = 5
SKEW = 7
F32 = jnp.float32
BF16 = jnp.bfloat16
MESH = pl.DeviceIdType.MESH


def dot_nn(a, b):
    return lax.dot_general(a, b, (((1,), (0,)), ((), ())), preferred_element_type=F32)


def dot_nt(a, b):
    return lax.dot_general(a, b, (((1,), (1,)), ((), ())), preferred_element_type=F32)


def dot_tn(a, b):
    return lax.dot_general(a, b, (((0,), (0,)), ((), ())), preferred_element_type=F32)


def rms_factor(v):
    return lax.rsqrt(jnp.mean(v * v, axis=-1, keepdims=True) + EPS)


def norm_back(grad, normed, factor):
    return factor * (grad - normed * jnp.mean(grad * normed, axis=-1, keepdims=True))


def mult(v, n):
    return pl.multiple_of(v, n)


class Refs:
    pass


def kernel(names, ndp, *refs):
    r = Refs()
    for name, ref in zip(names, refs):
        setattr(r, name, ref)
    tokens, width = r.n1.shape
    chunks = tokens // CHUNK
    half, quarter = CHUNK // 2, CHUNK // 4
    wc = r.wo_h.shape[0]
    fp, ff = r.wl.shape[0], r.wl_h.shape[0]
    block_rows = width // ndp
    pairs = ndp // 2
    groups = width // 256
    per_group = pairs // groups
    half_chunks = chunks // 2
    wide = 5 * wc // 2

    dp = lax.axis_index("dp")
    mp = lax.axis_index("mp")
    core = mp % 2
    side = mp // 2
    partner = (dp, mp + 1 - 2 * core)
    across = (dp, mp + 2 - 4 * side)
    parity = dp % 2
    line = dp // 2
    beside = (dp + 1 - 2 * parity, mp)

    def remote(src, dst, send, recv, device):
        return pltpu.make_async_remote_copy(
            src_ref=src,
            dst_ref=dst,
            send_sem=send,
            recv_sem=recv,
            device_id=device,
            device_id_type=MESH,
        )

    barrier = pltpu.get_barrier_semaphore()
    for device in (partner, across):
        pl.semaphore_signal(barrier, inc=1, device_id=device, device_id_type=MESH)
    near = min(8, ndp)
    near_at = dp % near
    near_base = dp - near_at

    def greet(j, carry):
        @pl.when((j != dp) & ((j % 2 == parity) | (j // near == dp // near)))
        def _():
            pl.semaphore_signal(barrier, inc=1, device_id=(j, mp), device_id_type=MESH)

        return carry

    lax.fori_loop(0, ndp, greet, 0)

    pair_mp = mp + 1 - 2 * core
    across_mp = mp + 2 - 4 * side

    def group_of(who):
        return pl.ds(mult(who * wc, wc), wc)

    share = wc // near

    def share_of(who, place):
        return pl.ds(mult(who * wc + place * share, share), share)

    def wo_across():
        return remote(
            r.wo_h.at[pl.ds(mult(near_at * share, share), share)],
            r.wof.at[share_of(mp, near_at)],
            r.sem_wos.at[0],
            r.sem_wor.at[0],
            across,
        )

    def wo_spread(j):
        here = r.wof.at[share_of(across_mp, near_at)]
        return remote(
            here, here, r.sem_wos.at[3 + j], r.sem_wor.at[3 + near_at], (near_base + j, mp)
        )

    def wo_arrival(j):
        here = r.wof.at[share_of(across_mp, j)]
        return remote(here, here, r.sem_wos.at[3 + j], r.sem_wor.at[3 + j], (near_base + j, mp))

    def to_near(act):
        def one(j, carry):
            @pl.when(j != near_at)
            def _():
                act(j)

            return carry

        lax.fori_loop(0, near, one, 0)

    def wo_partner():
        there = r.wof.at[group_of(mp)]
        return remote(r.wo_h, there, r.sem_wos.at[1], r.sem_wor.at[1], partner)

    def wo_forward():
        here = r.wof.at[group_of(across_mp)]
        return remote(here, here, r.sem_wos.at[2], r.sem_wor.at[2], partner)

    def load_tokens(c):
        rows = pl.ds(mult(c * CHUNK, CHUNK), CHUNK)
        return pltpu.make_async_copy(r.tok_h.at[rows], r.n1.at[rows], r.sem_tok.at[c])

    load_tokens(0).start()
    w_loads = [
        pltpu.make_async_copy(h, r.w.at[:, pl.ds(i * wc, wc)], r.sem_w.at[i])
        for i, h in enumerate((r.wq_h, r.wk_h, r.wv_h, r.wg_h))
    ]
    for copy in w_loads:
        copy.start()
    wo_load = pltpu.make_async_copy(
        r.wo_h, r.wof.at[pl.ds(mult(mp * wc, wc), wc)], r.sem_w.at[4]
    )
    wo_load.start()
    for c in range(1, chunks):
        load_tokens(c).start()
    glu_loads = [
        pltpu.make_async_copy(h, v.at[pl.ds(0, ff)], r.sem_w.at[i])
        for i, h, v in ((5, r.wd_h, r.wd), (6, r.wl_h, r.wl), (7, r.wr_h, r.wr))
    ]
    for copy in glu_loads:
        copy.start()
    cot_load = pltpu.make_async_copy(r.cot_h, r.cot, r.sem_w.at[8])
    cot_load.start()

    pl.semaphore_wait(barrier, 2 + pairs - 1 + near // 2)
    for copy in (wo_across(), wo_partner()):
        copy.start()

    def base(c):
        return mult(c * CHUNK, CHUNK)

    def half_rows(c):
        return pl.ds(mult(c * CHUNK + core * half, half), half)

    def own_rows(c):
        return pl.ds(mult(c * CHUNK + core * half + side * quarter, quarter), quarter)

    def other_rows(c):
        return pl.ds(mult(c * CHUNK + core * half + (1 - side) * quarter, quarter), quarter)

    def partner_own_rows(c):
        return pl.ds(mult(c * CHUNK + (1 - core) * half + side * quarter, quarter), quarter)

    def partner_other_rows(c):
        return pl.ds(mult(c * CHUNK + (1 - core) * half + (1 - side) * quarter, quarter), quarter)

    def kept(c):
        return pl.ds(mult(c * quarter, quarter), quarter)

    def part_of(s):
        return r.part_g if s == 1 else r.part

    def pair_of(s):
        return r.pair_g if s == 1 else r.pair

    def sent_of(s):
        return r.sent_g if s == 1 else r.sent

    def got_of(s):
        return r.got_g if s == 1 else r.got

    def full_of(s):
        return (None, r.out_h, r.do, r.gt_h)[s]

    def at(s, c):
        return s * chunks + c

    def pair_copy(s, c):
        slot = c % RING
        return remote(
            part_of(s).at[c % 2, pl.ds(mult((1 - core) * half, half), half)],
            pair_of(s).at[slot],
            r.sem_as.at[at(s, c)],
            r.sem_ar.at[at(s, c)],
            partner,
        )

    def across_copy(s, c):
        return remote(
            sent_of(s).at[kept(c)],
            got_of(s).at[kept(c)],
            r.sem_bs.at[at(s, c)],
            r.sem_br.at[at(s, c)],
            across,
        )

    def result_src(s, c):
        if s == 2:
            return full_of(s).at[own_rows(c)]
        return sent_of(s).at[kept(c)]

    def result_across(s, c):
        return remote(
            result_src(s, c),
            full_of(s).at[own_rows(c)],
            r.sem_cs.at[at(s, c)],
            r.sem_cr.at[at(s, c)],
            across,
        )

    def result_partner(s, c):
        return remote(
            result_src(s, c),
            full_of(s).at[own_rows(c)],
            r.sem_ps.at[at(s, c)],
            r.sem_pr.at[at(s, c)],
            partner,
        )

    def result_own(s, c):
        return pltpu.make_async_copy(
            sent_of(s).at[kept(c)], full_of(s).at[own_rows(c)], r.sem_o.at[at(s // 2, c)]
        )

    def forward(s, c):
        return remote(
            full_of(s).at[other_rows(c)],
            full_of(s).at[other_rows(c)],
            r.sem_ds.at[at(s, c)],
            r.sem_dr.at[at(s, c)],
            partner,
        )

    def step_b(s, c, send=True):
        copy = pair_copy(s, c)
        copy.wait_recv()
        copy.wait_send()
        part, pair = part_of(s), pair_of(s)
        slot, ring = c % 2, c % RING

        def piece(i, carry):
            rows = mult(i * 32, 32)
            away = pl.ds(mult(core * half + (1 - side) * quarter + rows, 32), 32)
            away_pair = pl.ds(mult((1 - side) * quarter + rows, 32), 32)
            total = part[slot, away, :].astype(F32) + pair[ring, away_pair, :].astype(F32)
            sent_of(s)[pl.ds(mult(c * quarter + rows, 32), 32), :] = total.astype(BF16)
            mine = pl.ds(mult(core * half + side * quarter + rows, 32), 32)
            mine_pair = pl.ds(mult(side * quarter + rows, 32), 32)
            total = part[slot, mine, :].astype(F32) + pair[ring, mine_pair, :].astype(F32)
            if s == 1:
                r.own_g[pl.ds(mult(c * quarter + rows, 32), 32), :] = total.astype(BF16)
            else:
                r.own[slot, pl.ds(rows, 32), :] = total
            return carry

        lax.fori_loop(0, quarter // 32, piece, 0, unroll=True)
        if send:
            across_copy(s, c).start()

    def step_c(s, c):
        copy = across_copy(s, c)
        copy.wait_recv()
        copy.wait_send()
        slot = c % 2

        def piece(i, carry):
            rows = mult(i * 32, 32)
            mine = pl.ds(mult(c * quarter + rows, 32), 32)
            full = pl.ds(mult(c * CHUNK + core * half + side * quarter + rows, 32), 32)
            arrived = got_of(s)[mine, :].astype(F32)
            if s == 1:
                total = r.own_g[mine, :].astype(F32) + arrived
            else:
                total = r.own[slot, pl.ds(rows, 32), :] + arrived
            if s == 1:
                r.sent_g[mine, :] = (r.hidden[mine, :] + total).astype(BF16)
            elif s == 2:
                hidden = r.hidden[mine, :]
                factor = rms_factor(hidden)
                d_hidden = r.cot[full, :].astype(F32) + norm_back(total, hidden * factor, factor)
                r.d_hidden[mine, :] = d_hidden
                r.do[full, :] = d_hidden.astype(BF16)
            else:
                held = pl.ds(mult(c * half + side * quarter + rows, 32), 32)
                source = r.tok_half[held, :].astype(F32)
                factor = rms_factor(source)
                d_source = r.d_hidden[mine, :] + norm_back(total, source * factor, factor)
                r.sent[mine, :] = d_source.astype(BF16)
            return carry

        lax.fori_loop(0, quarter // 32, piece, 0, unroll=True)
        result_across(s, c).start()
        result_partner(s, c).start()
        if s in (1, 3):
            result_own(s, c).start()

    def step_d(s, c):
        result_across(s, c).wait_recv()
        forward(s, c).start()

    def step_e(s, c):
        remote(
            result_src(s, c),
            full_of(s).at[partner_own_rows(c)],
            r.sem_ps.at[at(s, c)],
            r.sem_pr.at[at(s, c)],
            partner,
        ).wait_recv()
        remote(
            full_of(s).at[other_rows(c)],
            full_of(s).at[partner_other_rows(c)],
            r.sem_ds.at[at(s, c)],
            r.sem_dr.at[at(s, c)],
            partner,
        ).wait_recv()
        result_across(s, c).wait_send()
        result_partner(s, c).wait_send()
        forward(s, c).wait_send()
        if s in (1, 3):
            result_own(s, c).wait()

    def tick(s, c):
        @pl.when(c >= 1)
        def _():
            step_b(s, c - 1)

        @pl.when(c >= 2)
        def _():
            step_c(s, c - 2)

        @pl.when(c >= FORWARD)
        def _():
            step_d(s, c - FORWARD)

    def late_tick(s, n):
        if n == 0:
            step_b(s, chunks - 1)
        if n <= 1:
            step_c(s, chunks - 2 + n)
        step_d(s, chunks - FORWARD + n)

    def gated_across(c):
        here = r.do.at[pl.ds(base(c), CHUNK), group_of(mp)]
        return remote(here, here, r.sem_bs.at[c], r.sem_br.at[c], across)

    def gated_partner(c):
        here = r.do.at[pl.ds(base(c), CHUNK), group_of(mp)]
        return remote(here, here, r.sem_as.at[c], r.sem_ar.at[c], partner)

    def gated_forward(c):
        here = r.do.at[pl.ds(base(c), CHUNK), group_of(across_mp)]
        return remote(here, here, r.sem_ds.at[c], r.sem_dr.at[c], partner)

    def n2_partner(c):
        here = r.n2.at[half_rows(c)]
        return remote(here, here, r.sem_ps.at[c], r.sem_pr.at[c], partner)

    def gated_pass(c):
        gated_across(c).wait_recv()
        gated_forward(c).start()

    def gated_project(c):
        gated_partner(c).wait_recv()
        gated_forward(c).wait_recv()
        rows = half_rows(c)
        for t in range(width // 256):
            cols = pl.ds(t * 256, 256)
            total = dot_nn(r.do[rows, :], r.wof[:, cols])
            r.branch[:, cols] = total

        def piece(i, carry):
            q, sub = i // 2, mult((i % 2) * 32, 32)
            held = pl.ds(mult(c * half + i * 32, 32), 32)
            full = pl.ds(mult(c * CHUNK + core * half + i * 32, 32), 32)
            hidden = r.tok_half[held, :].astype(F32) + r.branch[pl.ds(mult(i * 32, 32), 32), :]
            r.n2[full, :] = (hidden * rms_factor(hidden)).astype(BF16)

            @pl.when(q == side)
            def _():
                r.hidden[pl.ds(mult(c * quarter + sub, 32), 32), :] = hidden

            return carry

        lax.fori_loop(0, half // 32, piece, 0, unroll=True)
        n2_partner(c).start()

    def gated_end(c):
        n2_partner(c).wait_recv()
        for copy in (gated_across(c), gated_partner(c), gated_forward(c), n2_partner(c)):
            copy.wait_send()

    lane = lax.broadcasted_iota(jnp.int32, (TILE, TILE), 1)
    row = lax.broadcasted_iota(jnp.int32, (TILE, TILE), 0)
    first = lane < HD

    def stacked(v):
        zero = jnp.zeros_like(v)
        return jnp.concatenate([jnp.where(first, v, zero), jnp.where(first, zero, v)], axis=0)

    def unstacked(v):
        return jnp.where(first, v[:TILE], v[TILE:])

    def head_mean(v):
        zero = jnp.zeros_like(v)
        low = jnp.sum(jnp.where(first, v, zero), axis=-1, keepdims=True)
        high = jnp.sum(jnp.where(first, zero, v), axis=-1, keepdims=True)
        return jnp.where(first, low, high) * (1.0 / HD)

    def probs_of(tile, rows, lanes):
        ids = r.seg[pl.ds(tile, 1), :].astype(F32)
        across_ids = jnp.broadcast_to(ids, (TILE, TILE))
        allowed = (
            (across_ids == across_ids.T) & (lane <= row) & (lane // BLOCK == row // BLOCK)
        )
        stack = stacked(r.qkv[rows, pl.ds(lanes, TILE)])
        keys = r.qkv[rows, pl.ds(wc + lanes, TILE)]
        scores = dot_nt(stack, keys) * HD ** (-0.5)
        allowed2 = jnp.concatenate([allowed, allowed], axis=0)
        masked = jnp.where(allowed2, scores, F32(-1e30))
        top = jnp.max(masked, axis=-1, keepdims=True)
        expd = jnp.exp(masked - top)
        probs = expd * (1.0 / jnp.sum(expd, axis=-1, keepdims=True))
        return probs

    head_pairs = wc // TILE
    tiles = CHUNK // TILE

    def tile_of(c, i):
        tile = c * tiles + i // head_pairs
        lanes = mult((i % head_pairs) * TILE, TILE)
        rows = pl.ds(mult(tile * TILE, TILE), TILE)
        return tile, rows, lanes

    def beside_copy(grads, arrivals, sems, g):
        block = 2 * g + 1 - parity
        send, recv = sems
        return remote(
            grads(pl.ds(mult(block * block_rows, block_rows), block_rows)),
            arrivals(pl.ds(mult(g * block_rows, block_rows), block_rows)),
            send.at[g],
            recv.at[g],
            beside,
        )

    def line_copy(grads, arrivals, sems, g):
        block = 2 * g + parity
        send, recv = sems
        return remote(
            grads(pl.ds(mult(block * block_rows, block_rows), block_rows)),
            arrivals(line),
            send.at[g],
            recv.at[line],
            (block, mp),
        )

    def glu_rows(rows):
        return r.grad_g.at[:, rows]

    def glu_beside(rows):
        return r.xg_h.at[:, rows]

    def glu_line(slot):
        return r.zg_h.at[slot]

    def att_rows(rows):
        return r.d_right.at[:, rows, pl.ds(0, wide)]

    def att_beside(rows):
        return r.xa_h.at[:, rows]

    def att_line(slot):
        return r.za_h.at[slot]

    glu_x = (glu_rows, glu_beside, (r.sem_xgs, r.sem_xgr))
    glu_z = (glu_rows, glu_line, (r.sem_zgs, r.sem_zgr))
    att_x = (att_rows, att_beside, (r.sem_xas, r.sem_xar))
    att_z = (att_rows, att_line, (r.sem_zas, r.sem_zar))

    def each(count, act):
        def one(j, carry):
            act(j)
            return carry

        if count == 1:
            act(0)
        else:
            lax.fori_loop(0, count, one, 0)

    def turn(k):
        return (line // per_group + 1 + k) % groups

    def turned_half(src, i, h):
        for k in range(tokens // 512):
            rows = pl.ds(h * (tokens // 2) + k * 256, 256)
            r.turned[:, pl.ds(k * 256, 256)] = src[rows, pl.ds(mult(i * 256, 256), 256)].T

    def gathered(h, old, term):
        return (term if h == 0 else old.astype(F32) + term).astype(BF16)

    def glu_half(i, h):
        rows = pl.ds(mult(i * 256, 256), 256)
        half_rows_all = pl.ds(h * (tokens // 2), tokens // 2)
        turned_half(r.n2, i, h)
        for t in range(fp // 256):
            cols = pl.ds(t * 256, 256)
            term = dot_nn(r.turned[...], r.d_left[half_rows_all, cols])
            r.grad_g[0, rows, cols] = gathered(h, r.grad_g[0, rows, cols], term)
            term = dot_nn(r.turned[...], r.d_right[h, :, cols])
            r.grad_g[1, rows, cols] = gathered(h, r.grad_g[1, rows, cols], term)
        turned_half(r.cot, i, h)
        for t in range(fp // 256):
            cols = pl.ds(t * 256, 256)
            term = dot_nn(r.turned[...], r.mixed[half_rows_all, cols])
            r.grad_g[2, rows, cols] = gathered(h, r.grad_g[2, rows, cols], term)

    def att_half(i, h):
        rows = pl.ds(mult(i * 256, 256), 256)
        half_rows_all = pl.ds(h * (tokens // 2), tokens // 2)

        def store(kind, term):
            for u in range(wc // 128):
                at_col = kind * (wc // 128) + u
                cols = pl.ds((at_col % (wide // 128)) * 128, 128)
                place = at_col // (wide // 128)
                piece = term[:, u * 128 : u * 128 + 128]
                r.d_right[place, rows, cols] = gathered(h, r.d_right[place, rows, cols], piece)

        turned_half(r.n1, i, h)
        for kind in range(4):
            cols = pl.ds(kind * wc, wc)
            store(kind, dot_nn(r.turned[...], r.d_all[half_rows_all, cols]))
        turned_half(r.do, i, h)
        store(4, dot_nn(r.turned[...], r.gated[half_rows_all, :]))

    def probs_out(c):
        return pltpu.make_async_copy(r.probs.at[c % 2], r.probs_h.at[c], r.sem_po.at[c % 2])

    def probs_in(c):
        return pltpu.make_async_copy(r.probs_h.at[c], r.probs.at[c % 2], r.sem_pi.at[c % 2])

    for copy in w_loads:
        copy.wait()

    def phase_one(c):
        rows_all = pl.ds(base(c), CHUNK)
        load_tokens(c).wait()
        r.tok_half[pl.ds(mult(c * half, half), half), :] = r.n1[half_rows(c), :]

        def norm_piece(i, carry2):
            rows = pl.ds(mult(c * CHUNK + i * 32, 32), 32)
            x = r.n1[rows, :].astype(F32)
            r.n1[rows, :] = (x * rms_factor(x)).astype(BF16)
            return carry2

        lax.fori_loop(0, CHUNK // 32, norm_piece, 0, unroll=True)

        def project(t, carry2):
            cols = pl.ds(mult(t * wc, wc), wc)
            r.qkv[rows_all, cols] = dot_nn(r.n1[rows_all, :], r.w[:, cols]).astype(BF16)
            return carry2

        lax.fori_loop(0, 3, project, 0, unroll=True)
        r.gate_now[...] = dot_nn(r.n1[rows_all, :], r.w[:, pl.ds(3 * wc, wc)])
        r.gate[rows_all, :] = r.gate_now[...].astype(BF16)

        @pl.when(c >= 2)
        def _():
            probs_out(c - 2).wait()

        def attend(i, carry2):
            tile, rows, lanes = tile_of(c, i)
            probs = probs_of(tile, rows, lanes).astype(BF16)
            r.probs[c % 2, i] = probs
            values = r.qkv[rows, pl.ds(2 * wc + lanes, TILE)]
            attended = unstacked(dot_nn(probs, values))
            r.attended[rows, pl.ds(lanes, TILE)] = attended.astype(BF16)
            factor = lax.rsqrt(head_mean(attended * attended) + EPS)
            near = pl.ds(mult((i // head_pairs) * TILE, TILE), TILE)
            sigma = jax.nn.sigmoid(r.gate_now[near, pl.ds(lanes, TILE)])
            gated = (attended * factor * sigma).astype(BF16)
            r.gated[rows, pl.ds(lanes, TILE)] = gated
            r.do[rows, pl.ds(mult(mp * wc + lanes, TILE), TILE)] = gated
            return carry2

        lax.fori_loop(0, tiles * head_pairs, attend, 0, unroll=True)

        probs_out(c).start()
        gated_across(c).start()
        gated_partner(c).start()

    def phase_two(c):
        gated_end(c)
        rows_all = pl.ds(base(c), CHUNK)
        rows_half = pl.ds(mult((c % half_chunks) * CHUNK, CHUNK), CHUNK)

        def hidden_units(t, carry2):
            cols = pl.ds(mult(t * 256, 256), 256)
            left = dot_nt(r.n2[rows_all, :], r.wl[cols, :])
            right = dot_nt(r.n2[rows_all, :], r.wr[cols, :])
            r.mixed[rows_all, cols] = (left * right).astype(BF16)
            d_mixed = dot_nt(r.cot[rows_all, :], r.wd[cols, :])
            r.d_left[rows_all, cols] = (d_mixed * right).astype(BF16)
            r.d_right[c // half_chunks, rows_half, cols] = (d_mixed * left).astype(BF16)
            return carry2

        lax.fori_loop(0, fp // 256, hidden_units, 0, unroll=True)

        def parts(t, carry2):
            cols = pl.ds(mult(t * 256, 256), 256)
            back = dot_nn(r.d_left[rows_all, :], r.wl[:, cols])
            back = back + dot_nn(r.d_right[c // half_chunks, rows_half, :], r.wr[:, cols])
            r.part[c % 2, :, cols] = back.astype(BF16)
            r.part_g[c % 2, :, cols] = dot_nn(r.mixed[rows_all, :], r.wd[:, cols]).astype(BF16)
            return carry2

        lax.fori_loop(0, width // 256, parts, 0, unroll=True)
        pair_copy(2, c).start()
        pair_copy(1, c).start()

        @pl.when(c >= half_chunks)
        def _():
            glu_half(turn(c - half_chunks), 0)

        tick(2, c)

        @pl.when(c >= 1)
        def _():
            step_b(1, c - 1, send=False)

    def both(it, carry):
        @pl.when(it < chunks)
        def _():
            phase_one(it)

        @pl.when(it == 0)
        def _():
            wo_across().wait_recv()
            to_near(lambda j: wo_spread(j).start())

        @pl.when(it == PASS)
        def _():
            to_near(lambda j: wo_arrival(j).wait_recv())
            wo_forward().start()

        @pl.when((it >= PASS) & (it < chunks + PASS))
        def _():
            gated_pass(it - PASS)

        @pl.when(it == PASS + 1)
        def _():
            wo_load.wait()
            wo_partner().wait_recv()
            wo_forward().wait_recv()
            for copy in (wo_across(), wo_partner(), wo_forward()):
                copy.wait_send()
            to_near(lambda j: wo_spread(j).wait_send())
            for copy in glu_loads:
                copy.wait()
            for weights in (r.wd, r.wl, r.wr):
                weights[pl.ds(ff, fp - ff), :] = jnp.zeros((fp - ff, width), BF16)
            cot_load.wait()

        @pl.when((it >= PASS + 1) & (it < chunks + PASS + 1))
        def _():
            gated_project(it - PASS - 1)

        @pl.when(it >= SKEW)
        def _():
            phase_two(it - SKEW)

        return carry

    lax.fori_loop(0, chunks + SKEW, both, 0)
    for c in range(chunks - 2, chunks):
        probs_out(c).wait()
    probs_in(0).start()
    late_tick(2, 0)
    step_b(1, chunks - 1, send=False)

    def send_glu(c, carry):
        across_copy(1, c).start()
        return carry

    lax.fori_loop(0, EARLY, send_glu, 0)

    def glu_group(k, carry):
        i = turn(k)
        glu_half(i, 1)
        each(per_group, lambda j: beside_copy(*glu_x, i * per_group + j).start())
        for n in range(FORWARD - 1):

            @pl.when(k == n)
            def _():
                late_tick(2, n + 1)

        return carry

    lax.fori_loop(0, groups, glu_group, 0)

    def line_loads(kinds, lanes, arrivals_h, stage, g):
        here = pl.ds(mult(g * block_rows, block_rows), block_rows)
        return [
            pltpu.make_async_copy(
                arrivals_h.at[t, here],
                stage.at[pl.ds(t * block_rows, block_rows), pl.ds(0, lanes)],
                r.sem_stage.at[t],
            )
            for t in range(kinds)
        ]

    def line_arrive(kinds, lanes, x, z, arrivals_h, stage, grads, g):
        copy = beside_copy(*x, g)
        copy.wait_recv()
        copy.wait_send()
        for load in line_loads(kinds, lanes, arrivals_h, stage, g):
            load.start()

    def line_sum(kinds, lanes, x, z, arrivals_h, stage, grads, g):
        for load in line_loads(kinds, lanes, arrivals_h, stage, g):
            load.wait()
        step = min(16, block_rows)
        cols = pl.ds(0, lanes)

        def piece(i, carry):
            sub = mult(i * step, step)
            there = pl.ds(mult((2 * g + parity) * block_rows + sub, step), step)
            for t in range(kinds):
                mine = grads[t, there, cols].astype(F32)
                theirs = stage[pl.ds(mult(t * block_rows + sub, step), step), cols].astype(F32)
                grads[t, there, cols] = (mine + theirs).astype(BF16)
            return carry

        lax.fori_loop(0, block_rows // step, piece, 0)

        @pl.when(g != line)
        def _():
            line_copy(*z, g).start()

    glu_line = (3, fp, glu_x, glu_z, r.xg_h, r.mixed, r.grad_g)
    att_line_of = (2, wide, att_x, att_z, r.xa_h, r.d_left, r.d_right)

    def line_both(what, k):
        if per_group == 1:
            line_sum(*what, turn(k))
            return

        def one(j):
            g = turn(k) * per_group + j
            line_arrive(*what, g)
            line_sum(*what, g)

        each(per_group, one)

    def line_start(what, k):
        if per_group == 1:
            line_arrive(*what, turn(k))

    def phase_three(c, carry):
        probs_in(c).wait()

        @pl.when(c + 1 < chunks)
        def _():
            probs_in(c + 1).start()

        step_e(2, c)
        rows_all = pl.ds(base(c), CHUNK)
        r.gate_now[...] = dot_nt(r.do[rows_all, :], r.wof[group_of(mp), :])

        def attend_back(i, carry2):
            tile, rows, lanes = tile_of(c, i)
            near = pl.ds(mult((i // head_pairs) * TILE, TILE), TILE)
            here = pl.ds(lanes, TILE)
            d_gated = r.gate_now[near, here]
            sigma = jax.nn.sigmoid(r.gate[rows, here].astype(F32))
            attended = r.attended[rows, here].astype(F32)
            factor = lax.rsqrt(head_mean(attended * attended) + EPS)
            head_normed = attended * factor
            d_head = d_gated * sigma
            d_gate = d_head * head_normed * (1.0 - sigma)
            r.d_all[rows, pl.ds(3 * wc + lanes, TILE)] = d_gate.astype(BF16)
            d_att = factor * (d_head - head_normed * head_mean(d_head * head_normed))
            d_stack = stacked(d_att.astype(BF16))
            probs_low = r.probs[c % 2, i]
            probs = probs_low.astype(F32)
            stack = stacked(r.qkv[rows, here])
            keys = r.qkv[rows, pl.ds(wc + lanes, TILE)]
            values = r.qkv[rows, pl.ds(2 * wc + lanes, TILE)]
            d_probs = dot_nt(d_stack, values)
            d_values = dot_tn(probs_low, d_stack)
            r.d_all[rows, pl.ds(2 * wc + lanes, TILE)] = d_values.astype(BF16)
            delta = jnp.sum(probs * d_probs, axis=-1, keepdims=True)
            d_scores = (probs * (d_probs - delta)).astype(BF16)
            d_queries = unstacked(dot_nn(d_scores, keys)) * HD ** (-0.5)
            r.d_all[rows, here] = d_queries.astype(BF16)
            d_keys = dot_tn(d_scores, stack) * HD ** (-0.5)
            r.d_all[rows, pl.ds(wc + lanes, TILE)] = d_keys.astype(BF16)
            return carry2

        lax.fori_loop(0, tiles * head_pairs, attend_back, 0, unroll=True)

        def back_piece(t, carry2):
            cols = pl.ds(mult(t * 256, 256), 256)
            r.part[c % 2, :, cols] = dot_nt(r.d_all[rows_all, :], r.w[cols, :]).astype(BF16)
            return carry2

        lax.fori_loop(0, width // 256, back_piece, 0, unroll=True)
        pair_copy(3, c).start()

        @pl.when(c >= half_chunks)
        def _():
            att_half(turn(c - half_chunks), 0)

        tick(3, c)

        for i in range(groups):

            @pl.when(c == 2 * i + 1)
            def _():
                line_start(glu_line, i)

            if i > 0:

                @pl.when(c == 2 * i)
                def _():
                    line_both(glu_line, i - 1)

        return carry

    lax.fori_loop(0, chunks, phase_three, 0)
    late_tick(3, 0)

    line_both(glu_line, groups - 1)
    lax.fori_loop(EARLY, chunks, send_glu, 0)

    def att_group(k, carry):
        i = turn(k)
        att_half(i, 1)
        each(per_group, lambda j: beside_copy(*att_x, i * per_group + j).start())
        for n in range(FORWARD - 1):

            @pl.when(k == n)
            def _():
                late_tick(3, n + 1)

        return carry

    lax.fori_loop(0, groups, att_group, 0)

    def glu_result(c, carry):
        step_c(1, c)
        return carry

    lax.fori_loop(0, EARLY, glu_result, 0)

    def att_lines(k, carry):
        line_start(att_line_of, k)
        first_left = EARLY + k * (chunks - EARLY) // groups
        last_left = EARLY + (k + 1) * (chunks - EARLY) // groups
        lax.fori_loop(first_left, last_left, glu_result, 0)
        line_both(att_line_of, k)
        return carry

    lax.fori_loop(0, groups, att_lines, 0)

    def glu_forward(c, carry):
        step_d(1, c)
        return carry

    lax.fori_loop(0, chunks, glu_forward, 0)

    def settle(z, sem):
        grads, arrivals, sems = z
        here = pl.ds(mult(dp * block_rows, block_rows), block_rows)
        mine = pltpu.make_async_copy(grads(here), arrivals(line), sem)
        mine.start()

        def arrived(j, carry):
            @pl.when(j != line)
            def _():
                remote(
                    grads(here), arrivals(j), sems[0].at[j], sems[1].at[j], (2 * j + parity, mp)
                ).wait_recv()
                line_copy(*z, j).wait_send()

            return carry

        lax.fori_loop(0, pairs, arrived, 0)
        mine.wait()

    settle(glu_z, r.sem_stage.at[0])
    settle(att_z, r.sem_stage.at[1])

    def ends(c, carry):
        step_e(1, c)
        step_e(3, c)
        return carry

    lax.fori_loop(0, chunks, ends, 0)


def fused(ndp, args):
    tokens, seg, wq, wk, wv, wg, wo, wl, wr, wd, cot = args
    rows, width = tokens.shape
    wc, ff = wq.shape[1], wl.shape[1]
    fp = (ff + 255) // 256 * 256
    chunks = rows // CHUNK
    quarter = CHUNK // 4
    own = rows // 4
    br = width // ndp
    pairs = ndp // 2
    wide = 5 * wc // 2
    probs_shape = (CHUNK // TILE * wc // TILE, 2 * TILE, TILE)
    hbm = pl.BlockSpec(memory_space=pl.ANY)
    vmem = pl.BlockSpec(memory_space=pltpu.VMEM)
    ins = [
        ("tok_h", tokens, hbm),
        ("seg", seg.reshape(rows // TILE, TILE), vmem),
        ("wq_h", wq, hbm),
        ("wk_h", wk, hbm),
        ("wv_h", wv, hbm),
        ("wg_h", wg, hbm),
        ("wo_h", wo, hbm),
        ("wl_h", wl.T, hbm),
        ("wr_h", wr.T, hbm),
        ("wd_h", wd, hbm),
        ("cot_h", cot, hbm),
    ]
    outs = [
        ("out_h", (rows, width), BF16, hbm),
        ("gt_h", (rows, width), BF16, hbm),
        ("xg_h", (3, pairs * br, fp), BF16, hbm),
        ("xa_h", (2, pairs * br, wide), BF16, hbm),
        ("zg_h", (pairs, 3, br, fp), BF16, hbm),
        ("za_h", (pairs, 2, br, wide), BF16, hbm),
        ("probs_h", (chunks,) + probs_shape, BF16, hbm),
    ]
    dma = pltpu.SemaphoreType.DMA
    scratch = [
        ("n1", pltpu.VMEM((rows, width), BF16)),
        ("tok_half", pltpu.VMEM((rows // 2, width), BF16)),
        ("cot", pltpu.VMEM((rows, width), BF16)),
        ("w", pltpu.VMEM((width, 4 * wc), BF16)),
        ("wof", pltpu.VMEM((width, width), BF16)),
        ("wl", pltpu.VMEM((fp, width), BF16)),
        ("wr", pltpu.VMEM((fp, width), BF16)),
        ("wd", pltpu.VMEM((fp, width), BF16)),
        ("qkv", pltpu.VMEM((rows, 3 * wc), BF16)),
        ("gate", pltpu.VMEM((rows, wc), BF16)),
        ("gate_now", pltpu.VMEM((CHUNK, wc), F32)),
        ("attended", pltpu.VMEM((rows, wc), BF16)),
        ("gated", pltpu.VMEM((rows, wc), BF16)),
        ("n2", pltpu.VMEM((rows, width), BF16)),
        ("mixed", pltpu.VMEM((rows, fp), BF16)),
        ("d_left", pltpu.VMEM((rows, fp), BF16)),
        ("d_right", pltpu.VMEM((2, rows // 2, fp), BF16)),
        ("do", pltpu.VMEM((rows, width), BF16)),
        ("turned", pltpu.VMEM((256, rows // 2), BF16)),
        ("part", pltpu.VMEM((2, CHUNK, width), BF16)),
        ("part_g", pltpu.VMEM((2, CHUNK, width), BF16)),
        ("pair", pltpu.VMEM((RING, CHUNK // 2, width), BF16)),
        ("pair_g", pltpu.VMEM((RING, CHUNK // 2, width), BF16)),
        ("sent", pltpu.VMEM((own, width), BF16)),
        ("sent_g", pltpu.VMEM((own, width), BF16)),
        ("got", pltpu.VMEM((own, width), BF16)),
        ("got_g", pltpu.VMEM((own, width), BF16)),
        ("own", pltpu.VMEM((2, quarter, width), F32)),
        ("branch", pltpu.VMEM((CHUNK // 2, width), F32)),
        ("own_g", pltpu.VMEM((own, width), BF16)),
        ("hidden", pltpu.VMEM((own, width), F32)),
        ("d_hidden", pltpu.VMEM((own, width), F32)),
        ("grad_g", pltpu.VMEM((3, width, fp), BF16)),
        ("probs", pltpu.VMEM((2,) + probs_shape, BF16)),
        ("sem_po", dma((2,))),
        ("sem_pi", dma((2,))),
        ("sem_tok", dma((chunks,))),
        ("sem_w", dma((9,))),
        ("sem_stage", dma((3 * pairs,))),
    ]
    for name in ("as", "ar", "bs", "br", "cs", "cr", "ps", "pr", "ds", "dr"):
        scratch.append(("sem_" + name, dma((4 * chunks,))))
    scratch.append(("sem_wos", dma((11,))))
    scratch.append(("sem_wor", dma((11,))))
    scratch.append(("sem_o", dma((2 * chunks,))))
    for name in ("xgs", "xgr", "zgs", "zgr", "xas", "xar", "zas", "zar"):
        scratch.append(("sem_" + name, dma((pairs,))))
    names = [n for n, *_ in ins] + [n for n, *_ in outs] + [n for n, _ in scratch]

    def call(*refs):
        named = dict(zip(names, refs))
        named["d_all"] = named["n2"]
        kernel(list(named), ndp, *named.values())

    flops = 6 * rows * width * (5 * wc + 3 * ff)
    result = pl.pallas_call(
        call,
        out_shape=[jax.ShapeDtypeStruct(s, d) for _, s, d, _ in outs],
        in_specs=[s for *_, s in ins],
        out_specs=[s for *_, s in outs],
        scratch_shapes=[s for _, s in scratch],
        compiler_params=pltpu.CompilerParams(
            collective_id=0, has_side_effects=True, vmem_limit_bytes=67043328
        ),
        cost_estimate=pl.CostEstimate(flops=flops, bytes_accessed=1 << 25, transcendentals=1 << 22),
        name="fused_layer",
    )(*[a for _, a, _ in ins])
    return result[0], result[1], result[4], result[5]


def collect(br, wc, ff, refs):
    out_h, gt_h, zg_h, za_h = refs[:4]
    out_o, gt_o, *grads_o = refs[4:14]
    held, zg, za, sem_in, sem_out, sem_z, *grads = refs[14:]
    pairs = zg.shape[0]
    pieces = held.shape[1]
    rows = held.shape[2]
    loads = [
        pltpu.make_async_copy(zg_h, zg, sem_z.at[0]),
        pltpu.make_async_copy(za_h, za, sem_z.at[1]),
    ]
    moves = []
    for i in range(pieces):
        for k, (src, dst) in enumerate(((out_h, out_o), (gt_h, gt_o))):
            span = pl.ds(i * rows, rows)
            get = pltpu.make_async_copy(src.at[span], held.at[k, i], sem_in.at[k * pieces + i])
            put = pltpu.make_async_copy(held.at[k, i], dst.at[span], sem_out.at[k * pieces + i])
            moves.append((get, put))
    for copy in loads:
        copy.start()
    for get, _ in moves:
        get.start()
    for copy in loads:
        copy.wait()

    def total(ref, t, cols):
        value = ref[0, t, :, cols].astype(F32)
        for j in range(1, pairs):
            value = value + ref[j, t, :, cols].astype(F32)
        return value

    stores = [pltpu.make_async_copy(v, h, sem_z.at[2 + i]) for i, (v, h) in enumerate(zip(grads, grads_o))]
    wide = za.shape[3]
    todo = list(moves)

    def pump():
        if todo:
            get, put = todo.pop(0)
            get.wait()
            put.start()

    for kind in range(5):
        for u in range(wc // 128):
            at_col = kind * (wc // 128) + u
            col = (at_col % (wide // 128)) * 128
            value = total(za, at_col // (wide // 128), pl.ds(col, 128))
            if kind < 4:
                grads[kind][:, pl.ds(u * 128, 128)] = value
            else:
                grads[kind][pl.ds(u * 128, 128), :] = value.T
        stores[kind].start()
        pump()
    for t in range(3):
        for start in range(0, ff, 128):
            size = min(128, ff - start)
            value = total(zg, t, pl.ds(start, 128)).T
            grads[5 + t][pl.ds(start, size), :] = value[:size]
        stores[5 + t].start()
        pump()
    while todo:
        pump()
    for _, put in moves:
        put.wait()
    for copy in stores:
        copy.wait()


def collected(arrays, br, wc, ff):
    rows, width = arrays[0].shape
    pieces = 8
    hbm = pl.BlockSpec(memory_space=pl.ANY)
    dma = pltpu.SemaphoreType.DMA
    shapes = [(br, wc)] * 4 + [(wc, br)] + [(ff, br)] * 3
    outs = [((rows, width), BF16)] * 2 + [(s, F32) for s in shapes]
    return pl.pallas_call(
        lambda *refs: collect(br, wc, ff, refs),
        out_shape=[jax.ShapeDtypeStruct(s, d) for s, d in outs],
        in_specs=[hbm] * 4,
        out_specs=[hbm] * 10,
        scratch_shapes=[
            pltpu.VMEM((2, pieces, rows // pieces, width), BF16),
            pltpu.VMEM(arrays[2].shape, BF16),
            pltpu.VMEM(arrays[3].shape, BF16),
            dma((2 * pieces,)),
            dma((2 * pieces,)),
            dma((10,)),
        ]
        + [pltpu.VMEM(s, F32) for s in shapes],
        compiler_params=pltpu.CompilerParams(vmem_limit_bytes=67043328),
        name="collect",
    )(*arrays)


def body(ndp, *args):
    arrays = fused(ndp, args)
    ff, wc, width = args[7].shape[1], args[2].shape[1], args[0].shape[1]
    out, grad_tokens, query, key, value, gate, proj, left, right, down = collected(
        arrays, width // ndp, wc, ff
    )
    return out, grad_tokens, query, key, value, gate, proj, left.T, right.T, down


def solution(mesh):
    rows, cols, down = P("dp", None), P(None, "mp"), P("mp", None)
    grad = P("dp", "mp")
    return jax.shard_map(
        functools.partial(body, mesh.shape["dp"]),
        mesh=mesh,
        in_specs=(rows, rows, cols, cols, cols, cols, down, cols, cols, down, rows),
        out_specs=(rows, rows, grad, grad, grad, grad, P("mp", "dp"), grad, grad, P("mp", "dp")),
        check_vma=False,
    )
```
